32 devices in a mesh: ens: 2 (over x), slab: 4 (over z), feat: 4 (over y, core).
Axes of the slice: x: 2, y: 2, z: 4, core: 2. Of those that a mesh axis runs over, the one named last changes fastest.
Arguments:
- particles: float32 [3072, 14336], P('ens', ('slab', 'feat')), parts along dimension 0
- prec_diag: float32 [28672], P(('ens', 'slab', 'feat')), parts along dimension 0
- mean_vec: float32 [28672], P(('ens', 'slab', 'feat')), parts along dimension 0
- low_rank: bfloat16 [28672, 16], P(('ens', 'slab', 'feat')), parts along dimension 0
Outputs:
- output: float32 [3072, 14336], P('ens', ('slab', 'feat')), parts along dimension 0
There are 2 independent parts. The reference program is written for one: setup_inputs(seed, part) draws one part's arguments, and reference() takes and returns one part's arrays. A program takes and returns all parts, laid end to end along the dimension named above; each array names one.
All inputs are finite; a program needn't handle non-finite values.
Results may differ from the reference program's by a relative error of at most 0.001.
Values are sent between devices in bfloat16 or wider.
A program may use at most 1 GiB of HBM per device.

```python
import jax
import jax.numpy as jnp
from jax import lax

N = 1536
D = 14336
R = 16
NUM_STEPS = 3
BANDWIDTH = 4.0 * D
STEP_SIZE = 0.4 * D


def setup_inputs(seed: int = 0, part: int = 0) -> dict:
    base_key = jax.random.fold_in(jax.random.key(seed), part)
    key_mean, key_shift, key_noise, key_prec, key_fac, key_coef, key_cmean = jax.random.split(base_key, 7)
    mean_vec = jax.random.normal(key_mean, (D,), jnp.float32)
    mean_shift = jax.random.normal(key_shift, (D,), jnp.float32)
    spread_noise = jax.random.normal(key_noise, (N, D), jnp.float32)
    prec_diag = jax.random.uniform(key_prec, (D,), jnp.float32, 0.2, 1.8) / D
    fac_scale = 1.3 / D
    low_rank = (jax.random.normal(key_fac, (D, R), jnp.float32) * fac_scale).astype(jnp.bfloat16)
    coef_rows = jax.random.normal(key_cmean, (1, R), jnp.float32) + jax.random.normal(key_coef, (N, R), jnp.float32)
    span_part = jnp.dot(coef_rows, low_rank.astype(jnp.float32).T) / (fac_scale * R ** 0.5)
    particles = mean_vec[None, :] + mean_shift[None, :] + spread_noise + span_part
    return {"particles": particles, "prec_diag": prec_diag, "mean_vec": mean_vec, "low_rank": low_rank}


def svgd_step(particles, prec_diag, mean_vec, low_rank):
    centered = particles - mean_vec[None, :]
    proj_full = jnp.dot(centered.astype(jnp.bfloat16), low_rank, preferred_element_type=jnp.float32)
    low_term = jnp.dot(proj_full.astype(jnp.bfloat16), low_rank.T, preferred_element_type=jnp.float32)
    grad_log = -(centered * prec_diag[None, :] + low_term)
    part_bf = particles.astype(jnp.bfloat16)
    gram_full = jnp.dot(part_bf, part_bf.T, preferred_element_type=jnp.float32)
    gram_diag = jnp.diagonal(gram_full)
    sq_dist = jnp.maximum(gram_diag[:, None] + gram_diag[None, :] - 2.0 * gram_full, 0.0)
    kernel = jnp.exp(-sq_dist / BANDWIDTH)
    drive_term = grad_log - (2.0 / BANDWIDTH) * particles
    applied = jnp.dot(kernel.astype(jnp.bfloat16), drive_term.astype(jnp.bfloat16), preferred_element_type=jnp.float32)
    phi_dir = (applied + (2.0 / BANDWIDTH) * jnp.sum(kernel, axis=1)[:, None] * particles) / N
    return particles + STEP_SIZE * phi_dir


def reference(particles, prec_diag, mean_vec, low_rank):
    def scan_body(carry, unused):
        return svgd_step(carry, prec_diag, mean_vec, low_rank), None
    result_particles, unused_out = lax.scan(scan_body, particles, None, length=NUM_STEPS)
    return result_particles
```

```python
import functools

import jax
import jax.numpy as jnp
from jax import lax
from jax.experimental import pallas as pl
from jax.experimental.pallas import tpu as pltpu
from jax.sharding import PartitionSpec as P

NUM_STEPS = 3
BAND_SCALE = 4.0
STEP_SCALE = 0.4
FEAT_AXES = ("slab", "feat")
LEAD_AXES = ("ens", "slab", "feat")
MESH = pl.DeviceIdType.MESH

B = 128
NP = 12
NB = 78
ROW = 256
UP = 6
LAG = 2
END = 2
OUT1 = 2
LAG2 = 2
OUT2 = 2
DIE = 2
FIN0 = 3 * LAG + END
AG0 = FIN0 + OUT1
CH = 15
ITERS = AG0 + 3 * LAG2 + CH + OUT2 + DIE


def _block(n):
    e = lax.div(n, NB)
    i = lax.rem(n, NP)
    j = lax.rem(i + lax.div(n, NP), NP)
    return (1 - e) * i + e * NP, (1 - e) * j + e * (n - NB)


def _at(k_ref, n):
    i, j = _block(n)
    return k_ref.at[pl.ds(pl.multiple_of(i * B, B), B), pl.ds(pl.multiple_of(j * B, B), B)]


def kernel(width, x_hbm, lam_ref, mu_ref, ut_ref, o_hbm, theta, th, a_ref, kf, gsrc, gy, zrecv, yrecv, yend, pmb, pmrecv,
           dsrc, dgather, dsum, sacc, sgather, ssum, ld, od, thd_s, thd_r, pm_s, pm_r, dg_s, dg_r, sg_s, sg_r, zs, zr, ys, yr,
           ye_s, ye_r, kz_s, kz_r, kyz_s, kyz_r, ky_s, ky_r, kd_s, kd_r, ke_s, ke_r):
    nf = theta.shape[1]
    n_part = theta.shape[0]
    bandwidth = BAND_SCALE * width
    step_size = STEP_SCALE * width
    rep = 2.0 / bandwidth
    ens = lax.axis_index("ens")
    z = lax.axis_index("slab")
    feat = lax.axis_index("feat")
    y = lax.div(feat, 2)
    c = lax.rem(feat, 2)
    me = z * 4 + feat
    ypart = (ens, z, (1 - y) * 2 + c)
    dpart = (ens, z, y * 2 + 1 - c)
    dc = lax.div(z, 3)
    corner = lax.rem(z, 3) == 0
    own8 = (dc * 2 + y) * 2 + c

    def rcopy(src, dst, s, r, dev):
        return pltpu.make_async_remote_copy(src_ref=src, dst_ref=dst, send_sem=s, recv_sem=r, device_id=dev, device_id_type=MESH)

    def zdev(dz):
        return (ens, z + dz, feat)

    def slot_chain(i, d, yy, cc):
        w = lax.div(i, 10)
        zf = lax.div(i, 2) * 16 + d * 4 + lax.rem(i, 2) * 2
        yf = (i - 10) * 16 + 8 + d * 4 + yy * 2
        return lax.rem((1 - w) * zf + w * yf + cc + NB, 80)

    def slot_yf(k, d, yy, cc):
        return lax.rem(k * 16 + 8 + d * 4 + yy * 2 + cc + NB, 80)

    def load_copy(p):
        rows = pl.ds(pl.multiple_of(p * ROW, ROW), ROW)
        return pltpu.make_async_copy(x_hbm.at[rows], theta.at[rows], ld.at[p])

    def out_copy(p):
        rows = pl.ds(pl.multiple_of(p * ROW, ROW), ROW)
        return pltpu.make_async_copy(theta.at[rows], o_hbm.at[rows], od.at[p])

    def th_copy(p):
        rows = pl.ds(pl.multiple_of(p * ROW, ROW), ROW)
        return rcopy(th.at[rows, pl.ds(0, nf)], th.at[rows, pl.ds(nf, nf)], thd_s.at[p], thd_r.at[p], dpart)

    def pm_copy():
        return rcopy(pmb.at[1 - c], pmrecv, pm_s, pm_r, dpart)

    def dg_copy(e):
        dev = (ens, (e // 4) * 3, e % 4)
        return rcopy(dsrc, dgather.at[me], dg_s.at[e], dg_r.at[me], dev)

    def dg_local():
        return pltpu.make_async_copy(dsrc, dgather.at[me], dg_r.at[me])

    def sg_copy(e):
        dev = (ens, e // 4, e % 4)
        return rcopy(sacc, sgather.at[own8], sg_s.at[e], sg_r.at[own8], dev)

    def sg_local():
        return pltpu.make_async_copy(sacc, sgather.at[own8], sg_r.at[own8])

    def z_copy(d, i):
        return rcopy(gsrc.at[d, i], zrecv.at[d, i], zs.at[d, i], zr.at[d, i], zdev(2 * d - 1))

    def y_copy(d, k):
        return rcopy(gy.at[d, k], yrecv.at[d, k], ys.at[d, k], yr.at[d, k], ypart)

    def ye_copy(k, i):
        return rcopy(gsrc.at[dc, i], yend.at[k], ye_s.at[k], ye_r.at[k], ypart)

    def kz_copy(d, i):
        blk = _at(kf, slot_chain(i, d, y, c))
        return rcopy(blk, blk, kz_s.at[d, i], kz_r.at[d, i], zdev(1 - 2 * d))

    def kyz_copy(k, ey):
        blk = _at(kf, lax.rem(k * 16 + dc * 4 + ey * 2 + c + NB, 80))
        return rcopy(blk, blk, kyz_s.at[k], kyz_r.at[k], ypart)

    def ky_copy(d, k, yy):
        blk = _at(kf, slot_yf(k, d, yy, c))
        return rcopy(blk, blk, ky_s.at[d, k], ky_r.at[d, k], ypart)

    def kd_copy(d, i, cc):
        blk = _at(kf, slot_chain(i, d, y, cc))
        return rcopy(blk, blk, kd_s.at[d, i], kd_r.at[d, i], dpart)

    def ke_copy(d, k, cc):
        blk = _at(kf, slot_yf(k, d, 1 - y, cc))
        return rcopy(blk, blk, ke_s.at[d, k], ke_r.at[d, k], dpart)

    def flip(n):
        i, j = _block(n)

        @pl.when((n >= NP) & (n < NB))
        def _():
            src = kf[pl.ds(pl.multiple_of(i * B, B), B), pl.ds(pl.multiple_of(j * B, B), B)]
            kf[pl.ds(pl.multiple_of(j * B, B), B), pl.ds(pl.multiple_of(i * B, B), B)] = (
                src.astype(jnp.float32).T.astype(jnp.bfloat16)
            )

    def gram(n):
        i, j = _block(n)
        return lax.dot_general(
            th[pl.ds(pl.multiple_of(i * B, B), B), :],
            th[pl.ds(pl.multiple_of(j * B, B), B), :],
            (((1,), (1,)), ((), ())),
            preferred_element_type=jnp.float32,
        )

    def post(p, new):
        rows = pl.ds(pl.multiple_of(p * ROW, ROW), ROW)
        tb = new.astype(jnp.bfloat16)
        th[rows, pl.ds(0, nf)] = tb
        th_copy(p).start()
        xb = (new - mu_ref[...]).astype(jnp.bfloat16)
        pm = lax.dot_general(ut_ref[...], xb, (((1,), (1,)), ((), ())), preferred_element_type=jnp.float32)
        half = lax.div(p, 3)
        for h in range(2):
            q = lax.rem(p, 3) * 2 + h
            pmb[half, pl.ds(pl.multiple_of(q * 16, 16), 16), :] = pm[:, h * B:(h + 1) * B]
            t = tb[h * B:(h + 1) * B, :].astype(jnp.float32)
            sq = t * t
            tot = sq[:, 0:B]
            for m in range(1, nf // B):
                tot = tot + sq[:, m * B:(m + 1) * B]
            dsrc[pl.ds(p * 2 + h, 1), :] = jnp.sum(tot.T, axis=0, keepdims=True)

    barrier = pltpu.get_barrier_semaphore()
    for o in range(1, 16):
        e = lax.rem(me + o, 16)
        pl.semaphore_signal(barrier, inc=1, device_id=(ens, lax.div(e, 4), lax.rem(e, 4)), device_id_type=MESH)
    for p in range(UP):
        load_copy(p).start()
    pmb[...] = jnp.zeros_like(pmb)
    dsrc[...] = jnp.zeros_like(dsrc)
    pl.semaphore_wait(barrier, 15)

    @pl.loop(0, UP)
    def _(p):
        load_copy(p).wait()
        rows = pl.ds(pl.multiple_of(p * ROW, ROW), ROW)
        post(p, theta[rows, :])

    @pl.loop(0, NUM_STEPS)
    def _(step):
        for e in range(8):
            mine = me == (e // 4) * 12 + e % 4

            @pl.when(mine)
            def _():
                dg_local().start()

            @pl.when(jnp.logical_not(mine))
            def _():
                dg_copy(e).start()

        pm_copy().start()
        sacc[...] = jnp.zeros_like(sacc)

        @pl.loop(0, UP)
        def _(p):
            th_copy(p).wait()

        pm_copy().wait()

        @pl.loop(0, 5)
        def _(k):
            for d in range(2):
                gy[d, k] = gram(slot_yf(k, d, 1 - y, c))
            for d in range(2):
                y_copy(d, k).start()

        @pl.loop(0, ITERS)
        def _(g):
            for d in range(2):
                pos = z if d else 3 - z
                i = g - LAG * pos

                @pl.when((i >= 0) & (i < CH))
                def _():
                    n = slot_chain(i, d, y, c)

                    @pl.when(n < NB)
                    def _():
                        gsrc[d, i] = gram(n)

                    if d == 0:
                        @pl.when(n >= NB)
                        def _():
                            gsrc[d, i] = pmb[c] + pmrecv[...]

                    @pl.when(i >= 10)
                    def _():
                        y_copy(d, i - 10).wait_recv()
                        gsrc[d, i] = gsrc[d, i] + yrecv[d, i - 10]

                    @pl.when(pos > 0)
                    def _():
                        z_copy(d, i).wait_recv()
                        gsrc[d, i] = gsrc[d, i] + zrecv[d, i]

            for d in range(2):
                pos = z if d else 3 - z
                i = g - LAG * pos

                @pl.when((i >= 0) & (i < CH))
                def _():
                    @pl.when(pos < 3)
                    def _():
                        z_copy(d, i).start()

                    @pl.when((pos == 3) & (i < 10) & (lax.rem(i, 2) != y))
                    def _():
                        ye_copy(lax.div(i, 2), i).start()

            i = g - FIN0

            @pl.when(corner & (i >= 0) & (i < CH))
            def _():
                @pl.when(i == 0)
                def _():
                    tot = jnp.zeros((16, B), jnp.float32)
                    for e in range(16):
                        pltpu.make_async_copy(dsrc, dgather.at[e], dg_r.at[e]).wait()
                        tot = tot + dgather[e]
                    dsum[...] = tot

                @pl.when((i >= 10) | (lax.rem(i, 2) == y))
                def _():
                    @pl.when(i < 10)
                    def _():
                        k = lax.div(i, 2)
                        ye_copy(k, i).wait_recv()
                        gsrc[dc, i] = gsrc[dc, i] + yend[k]

                    n = slot_chain(i, dc, y, c)
                    bi, bj = _block(n)
                    dst_r = pl.ds(pl.multiple_of(bi * B, B), B)
                    dst_c = pl.ds(pl.multiple_of(bj * B, B), B)

                    @pl.when(n < NB)
                    def _():
                        gi = jnp.broadcast_to(dsum[pl.ds(bi, 1), :], (B, B)).T
                        gj = dsum[pl.ds(bj, 1), :]
                        sq = jnp.maximum(gi + gj - 2.0 * gsrc[dc, i], 0.0)
                        kk = jnp.exp(sq * (-1.0 / bandwidth))
                        kf[dst_r, dst_c] = kk.astype(jnp.bfloat16)
                        sacc[pl.ds(bj, 1), :] = sacc[pl.ds(bj, 1), :] + jnp.sum(kk, axis=0, keepdims=True)

                        @pl.when(n >= NP)
                        def _():
                            sacc[pl.ds(bi, 1), :] = sacc[pl.ds(bi, 1), :] + jnp.sum(kk.T, axis=0, keepdims=True)

                    @pl.when(n >= NB)
                    def _():
                        kf[dst_r, dst_c] = gsrc[dc, i].astype(jnp.bfloat16)

                    @pl.when(i < 10)
                    def _():
                        kyz_copy(lax.div(i, 2), y).start()

                    @pl.when(i >= 10)
                    def _():
                        ky_copy(dc, i - 10, y).start()

                @pl.when(i == CH - 1)
                def _():
                    for e in range(16):
                        @pl.when(me == e)
                        def _():
                            sg_local().start()

                        @pl.when(me != e)
                        def _():
                            sg_copy(e).start()

            for d in range(2):
                dist = 3 - z if d else z
                i = g - AG0 - LAG2 * dist

                @pl.when((i >= 0) & (i < CH))
                def _():
                    @pl.when((dist == 0) & (i < 10) & (lax.rem(i, 2) != y))
                    def _():
                        kyz_copy(lax.div(i, 2), 1 - y).wait_recv()

                    @pl.when(dist > 0)
                    def _():
                        kz_copy(d, i).wait_recv()

                    @pl.when(dist < 3)
                    def _():
                        kz_copy(d, i).start()

                    @pl.when((dist > 0) & (i >= 10))
                    def _():
                        ky_copy(d, i - 10, y).start()

                    kd_copy(d, i, c).start()
                    flip(slot_chain(i, d, y, c))

                k = i - OUT2 - 10

                @pl.when((k >= 0) & (k < 5))
                def _():
                    ky_copy(d, k, 1 - y).wait_recv()
                    ke_copy(d, k, c).start()
                    flip(slot_yf(k, d, 1 - y, c))

                j = i - DIE

                @pl.when((j >= 0) & (j < CH))
                def _():
                    kd_copy(d, j, 1 - c).wait_recv()
                    flip(slot_chain(j, d, y, 1 - c))

                m = k - DIE

                @pl.when((m >= 0) & (m < 5))
                def _():
                    ke_copy(d, m, 1 - c).wait_recv()
                    flip(slot_yf(m, d, 1 - y, 1 - c))

            p = g - (AG0 + 3 * LAG2 + DIE + 2)

            @pl.when((p >= 0) & (p < UP))
            def _():
                rows = pl.ds(pl.multiple_of(p * ROW, ROW), ROW)
                q = lax.rem(p, 3)
                half = lax.div(p, 3)
                hcol = pl.ds(pl.multiple_of(half * B, B), B)
                pmt = jnp.concatenate(
                    [kf[pl.ds(pl.multiple_of(NP * B + (q * 2 + h) * 16, 16), 16), hcol] for h in range(2)], axis=1
                )
                low = lax.dot_general(
                    pmt.astype(jnp.float32).T.astype(jnp.bfloat16),
                    ut_ref[...],
                    (((1,), (0,)), ((), ())),
                    preferred_element_type=jnp.float32,
                )
                cur = theta[rows, :]
                grad = -((cur - mu_ref[...]) * lam_ref[...] + low)
                a_ref[rows, :] = (grad - rep * cur).astype(jnp.bfloat16)

        for e in range(8):
            @pl.when(me != (e // 4) * 12 + e % 4)
            def _():
                dg_copy(e).wait_send()

        @pl.loop(0, 5)
        def _(k):
            for d in range(2):
                y_copy(d, k).wait_send()
                ke_copy(d, k, c).wait_send()
                ky_copy(d, k, y).wait_send()

            @pl.when(corner)
            def _():
                ye_copy(k, 2 * k + 1 - y).wait_send()
                kyz_copy(k, y).wait_send()

        @pl.loop(0, CH)
        def _(i):
            for d in range(2):
                pos = z if d else 3 - z

                @pl.when(pos < 3)
                def _():
                    z_copy(d, i).wait_send()

                @pl.when(pos > 0)
                def _():
                    kz_copy(d, i).wait_send()

                kd_copy(d, i, c).wait_send()

        @pl.when(corner)
        def _():
            for e in range(16):
                @pl.when(me != e)
                def _():
                    sg_copy(e).wait_send()

        tot = jnp.zeros((16, B), jnp.float32)
        for e in range(8):
            pltpu.make_async_copy(sacc, sgather.at[e], sg_r.at[e]).wait()
            tot = tot + sgather[e]
        ssum[...] = tot

        @pl.loop(0, UP)
        def _(p):
            rows = pl.ds(pl.multiple_of(p * ROW, ROW), ROW)
            acc = jnp.dot(kf[rows, :], a_ref[...], preferred_element_type=jnp.float32)
            cur = theta[rows, :]
            col = jnp.concatenate(
                [jnp.broadcast_to(ssum[pl.ds(p * 2 + h, 1), :], (B, B)).T[:, 0:1] for h in range(2)], axis=0
            )
            phi = (acc + (rep * col) * cur) * (1.0 / n_part)
            new = cur + step_size * phi
            theta[rows, :] = new

            @pl.when(step < NUM_STEPS - 1)
            def _():
                post(p, new)

            @pl.when(step == NUM_STEPS - 1)
            def _():
                out_copy(p).start()

    @pl.loop(0, UP)
    def _(p):
        out_copy(p).wait()


def solution(mesh):
    def run_steps(particles, prec_diag, mean_vec, low_rank):
        width = particles.shape[1]

        def local_steps(current, prec_loc, mean_loc, fac_loc):
            n_part, nf = current.shape
            dma = pltpu.SemaphoreType.DMA
            f32, bf16 = jnp.float32, jnp.bfloat16
            vmem = pltpu.VMEM
            return pl.pallas_call(
                functools.partial(kernel, width),
                out_shape=jax.ShapeDtypeStruct((n_part, nf), f32),
                in_specs=[pl.BlockSpec(memory_space=pl.ANY)] + [pl.BlockSpec(memory_space=pltpu.VMEM)] * 3,
                out_specs=pl.BlockSpec(memory_space=pl.ANY),
                scratch_shapes=[
                    vmem((n_part, nf), f32),
                    vmem((n_part, 2 * nf), bf16),
                    vmem((n_part, nf), bf16),
                    vmem((n_part + B, n_part), bf16),
                    vmem((2, CH, B, B), f32),
                    vmem((2, 5, B, B), f32),
                    vmem((2, CH, B, B), f32),
                    vmem((2, 5, B, B), f32),
                    vmem((5, B, B), f32),
                    vmem((2, B, B), f32),
                    vmem((B, B), f32),
                    vmem((16, B), f32),
                    vmem((16, 16, B), f32),
                    vmem((16, B), f32),
                    vmem((16, B), f32),
                    vmem((8, 16, B), f32),
                    vmem((16, B), f32),
                    dma((UP,)), dma((UP,)), dma((UP,)), dma((UP,)), dma, dma, dma((8,)), dma((16,)), dma((16,)), dma((8,)),
                    dma((2, CH)), dma((2, CH)), dma((2, 5)), dma((2, 5)), dma((5,)), dma((5,)),
                    dma((2, CH)), dma((2, CH)), dma((5,)), dma((5,)), dma((2, 5)), dma((2, 5)),
                    dma((2, CH)), dma((2, CH)), dma((2, 5)), dma((2, 5)),
                ],
                compiler_params=pltpu.CompilerParams(
                    collective_id=0, has_side_effects=True, vmem_limit_bytes=56 * 1024 * 1024
                ),
                name="svgd",
            )(current, prec_loc.reshape(1, nf), mean_loc.reshape(1, nf), fac_loc.T)

        sharded = jax.shard_map(
            local_steps,
            mesh=mesh,
            in_specs=(P("ens", FEAT_AXES), P(LEAD_AXES), P(LEAD_AXES), P(LEAD_AXES, None)),
            out_specs=P("ens", FEAT_AXES),
            check_vma=False,
        )
        return sharded(particles, prec_diag, mean_vec, low_rank)

    return run_steps
```

```python
import functools

import jax
import jax.numpy as jnp
from jax import lax
from jax.experimental import pallas as pl
from jax.experimental.pallas import tpu as pltpu
from jax.sharding import PartitionSpec as P

NUM_STEPS = 3
BAND_SCALE = 4.0
STEP_SCALE = 0.4
FEAT_AXES = ("slab", "feat")
LEAD_AXES = ("ens", "slab", "feat")
MESH = pl.DeviceIdType.MESH

B = 128
NP = 12
NB = 78
ROW = 256
UP = 6
LAG = 3
END = 3
OUT1 = 3
LAG2 = 3
OUT2 = 3
DIE = 2
FIN0 = 3 * LAG + END
AG0 = FIN0 + OUT1
CH = 15
ITERS = AG0 + 3 * LAG2 + CH + OUT2 + DIE


def _block(n):
    e = lax.div(n, NB)
    i = lax.rem(n, NP)
    j = lax.rem(i + lax.div(n, NP), NP)
    return (1 - e) * i + e * NP, (1 - e) * j + e * (n - NB)


def _at(k_ref, n):
    i, j = _block(n)
    return k_ref.at[pl.ds(pl.multiple_of(i * B, B), B), pl.ds(pl.multiple_of(j * B, B), B)]


def kernel(width, x_hbm, lam_ref, mu_ref, ut_ref, o_hbm, theta, th, a_ref, kf, gsrc, gy, zrecv, yrecv, yend, pmb, pmrecv,
           dsrc, dgather, dsum, sacc, sgather, ssum, ld, od, thd_s, thd_r, pm_s, pm_r, dg_s, dg_r, sg_s, sg_r, zs, zr, ys, yr,
           ye_s, ye_r, kz_s, kz_r, kyz_s, kyz_r, ky_s, ky_r, kd_s, kd_r, ke_s, ke_r):
    nf = theta.shape[1]
    n_part = theta.shape[0]
    bandwidth = BAND_SCALE * width
    step_size = STEP_SCALE * width
    rep = 2.0 / bandwidth
    ens = lax.axis_index("ens")
    z = lax.axis_index("slab")
    feat = lax.axis_index("feat")
    y = lax.div(feat, 2)
    c = lax.rem(feat, 2)
    me = z * 4 + feat
    ypart = (ens, z, (1 - y) * 2 + c)
    dpart = (ens, z, y * 2 + 1 - c)
    dc = lax.div(z, 3)
    corner = lax.rem(z, 3) == 0
    own8 = (dc * 2 + y) * 2 + c

    def rcopy(src, dst, s, r, dev):
        return pltpu.make_async_remote_copy(src_ref=src, dst_ref=dst, send_sem=s, recv_sem=r, device_id=dev, device_id_type=MESH)

    def zdev(dz):
        return (ens, z + dz, feat)

    def slot_chain(i, d, yy, cc):
        w = lax.div(i, 10)
        zf = lax.div(i, 2) * 16 + d * 4 + lax.rem(i, 2) * 2
        yf = (i - 10) * 16 + 8 + d * 4 + yy * 2
        return lax.rem((1 - w) * zf + w * yf + cc + NB, 80)

    def slot_yf(k, d, yy, cc):
        return lax.rem(k * 16 + 8 + d * 4 + yy * 2 + cc + NB, 80)

    def load_copy(p):
        rows = pl.ds(pl.multiple_of(p * ROW, ROW), ROW)
        return pltpu.make_async_copy(x_hbm.at[rows], theta.at[rows], ld.at[p])

    def out_copy(p):
        rows = pl.ds(pl.multiple_of(p * ROW, ROW), ROW)
        return pltpu.make_async_copy(theta.at[rows], o_hbm.at[rows], od.at[p])

    def th_copy(p):
        rows = pl.ds(pl.multiple_of(p * ROW, ROW), ROW)
        return rcopy(th.at[rows, pl.ds(0, nf)], th.at[rows, pl.ds(nf, nf)], thd_s.at[p], thd_r.at[p], dpart)

    def pm_copy():
        return rcopy(pmb.at[1 - c], pmrecv, pm_s, pm_r, dpart)

    def dg_copy(e):
        dev = (ens, (e // 4) * 3, e % 4)
        return rcopy(dsrc, dgather.at[me], dg_s.at[e], dg_r.at[me], dev)

    def dg_local():
        return pltpu.make_async_copy(dsrc, dgather.at[me], dg_r.at[me])

    def sg_copy(e):
        dev = (ens, e // 4, e % 4)
        return rcopy(sacc, sgather.at[own8], sg_s.at[e], sg_r.at[own8], dev)

    def sg_local():
        return pltpu.make_async_copy(sacc, sgather.at[own8], sg_r.at[own8])

    def z_copy(d, i):
        return rcopy(gsrc.at[d, i], zrecv.at[d, i], zs.at[d, i], zr.at[d, i], zdev(2 * d - 1))

    def y_copy(d, k):
        return rcopy(gy.at[d, k], yrecv.at[d, k], ys.at[d, k], yr.at[d, k], ypart)

    def ye_copy(k, i):
        return rcopy(gsrc.at[dc, i], yend.at[k], ye_s.at[k], ye_r.at[k], ypart)

    def kz_copy(d, i):
        blk = _at(kf, slot_chain(i, d, y, c))
        return rcopy(blk, blk, kz_s.at[d, i], kz_r.at[d, i], zdev(1 - 2 * d))

    def kyz_copy(k, ey):
        blk = _at(kf, lax.rem(k * 16 + dc * 4 + ey * 2 + c + NB, 80))
        return rcopy(blk, blk, kyz_s.at[k], kyz_r.at[k], ypart)

    def ky_copy(d, k, yy):
        blk = _at(kf, slot_yf(k, d, yy, c))
        return rcopy(blk, blk, ky_s.at[d, k], ky_r.at[d, k], ypart)

    def kd_copy(d, i, cc):
        blk = _at(kf, slot_chain(i, d, y, cc))
        return rcopy(blk, blk, kd_s.at[d, i], kd_r.at[d, i], dpart)

    def ke_copy(d, k, cc):
        blk = _at(kf, slot_yf(k, d, 1 - y, cc))
        return rcopy(blk, blk, ke_s.at[d, k], ke_r.at[d, k], dpart)

    def flip(n):
        i, j = _block(n)

        @pl.when((n >= NP) & (n < NB))
        def _():
            src = kf[pl.ds(pl.multiple_of(i * B, B), B), pl.ds(pl.multiple_of(j * B, B), B)]
            kf[pl.ds(pl.multiple_of(j * B, B), B), pl.ds(pl.multiple_of(i * B, B), B)] = (
                src.astype(jnp.float32).T.astype(jnp.bfloat16)
            )

    def gram(n):
        i, j = _block(n)
        return lax.dot_general(
            th[pl.ds(pl.multiple_of(i * B, B), B), :],
            th[pl.ds(pl.multiple_of(j * B, B), B), :],
            (((1,), (1,)), ((), ())),
            preferred_element_type=jnp.float32,
        )

    def post(p, new):
        rows = pl.ds(pl.multiple_of(p * ROW, ROW), ROW)
        tb = new.astype(jnp.bfloat16)
        th[rows, pl.ds(0, nf)] = tb
        th_copy(p).start()
        xb = (new - mu_ref[...]).astype(jnp.bfloat16)
        pm = lax.dot_general(ut_ref[...], xb, (((1,), (1,)), ((), ())), preferred_element_type=jnp.float32)
        half = lax.div(p, 3)
        for h in range(2):
            q = lax.rem(p, 3) * 2 + h
            pmb[half, pl.ds(pl.multiple_of(q * 16, 16), 16), :] = pm[:, h * B:(h + 1) * B]
            t = tb[h * B:(h + 1) * B, :].astype(jnp.float32)
            sq = t * t
            tot = sq[:, 0:B]
            for m in range(1, nf // B):
                tot = tot + sq[:, m * B:(m + 1) * B]
            dsrc[pl.ds(p * 2 + h, 1), :] = jnp.sum(tot.T, axis=0, keepdims=True)

    barrier = pltpu.get_barrier_semaphore()
    for o in range(1, 16):
        e = lax.rem(me + o, 16)
        pl.semaphore_signal(barrier, inc=1, device_id=(ens, lax.div(e, 4), lax.rem(e, 4)), device_id_type=MESH)
    for p in range(UP):
        load_copy(p).start()
    pmb[...] = jnp.zeros_like(pmb)
    dsrc[...] = jnp.zeros_like(dsrc)
    pl.semaphore_wait(barrier, 15)

    @pl.loop(0, UP)
    def _(p):
        load_copy(p).wait()
        rows = pl.ds(pl.multiple_of(p * ROW, ROW), ROW)
        post(p, theta[rows, :])

    @pl.loop(0, NUM_STEPS)
    def _(step):
        for e in range(8):
            mine = me == (e // 4) * 12 + e % 4

            @pl.when(mine)
            def _():
                dg_local().start()

            @pl.when(jnp.logical_not(mine))
            def _():
                dg_copy(e).start()

        pm_copy().start()
        sacc[...] = jnp.zeros_like(sacc)

        @pl.loop(0, UP)
        def _(p):
            th_copy(p).wait()

        pm_copy().wait()

        @pl.loop(0, 5)
        def _(k):
            for d in range(2):
                gy[d, k] = gram(slot_yf(k, d, 1 - y, c))
            for d in range(2):
                y_copy(d, k).start()

        @pl.loop(0, ITERS)
        def _(g):
            for d in range(2):
                pos = z if d else 3 - z
                i = g - LAG * pos

                @pl.when((i >= 0) & (i < CH))
                def _():
                    n = slot_chain(i, d, y, c)

                    @pl.when(n < NB)
                    def _():
                        gsrc[d, i] = gram(n)

                    if d == 0:
                        @pl.when(n >= NB)
                        def _():
                            gsrc[d, i] = pmb[c] + pmrecv[...]

                    @pl.when(i >= 10)
                    def _():
                        y_copy(d, i - 10).wait_recv()
                        gsrc[d, i] = gsrc[d, i] + yrecv[d, i - 10]

                    @pl.when(pos > 0)
                    def _():
                        z_copy(d, i).wait_recv()
                        gsrc[d, i] = gsrc[d, i] + zrecv[d, i]

            for d in range(2):
                pos = z if d else 3 - z
                i = g - LAG * pos

                @pl.when((i >= 0) & (i < CH))
                def _():
                    @pl.when(pos < 3)
                    def _():
                        z_copy(d, i).start()

                    @pl.when((pos == 3) & (i < 10) & (lax.rem(i, 2) != y))
                    def _():
                        ye_copy(lax.div(i, 2), i).start()

            i = g - FIN0

            @pl.when(corner & (i >= 0) & (i < CH))
            def _():
                @pl.when(i == 0)
                def _():
                    tot = jnp.zeros((16, B), jnp.float32)
                    for e in range(16):
                        pltpu.make_async_copy(dsrc, dgather.at[e], dg_r.at[e]).wait()
                        tot = tot + dgather[e]
                    dsum[...] = tot

                @pl.when((i >= 10) | (lax.rem(i, 2) == y))
                def _():
                    @pl.when(i < 10)
                    def _():
                        k = lax.div(i, 2)
                        ye_copy(k, i).wait_recv()
                        gsrc[dc, i] = gsrc[dc, i] + yend[k]

                    n = slot_chain(i, dc, y, c)
                    bi, bj = _block(n)
                    dst_r = pl.ds(pl.multiple_of(bi * B, B), B)
                    dst_c = pl.ds(pl.multiple_of(bj * B, B), B)

                    @pl.when(n < NB)
                    def _():
                        gi = jnp.broadcast_to(dsum[pl.ds(bi, 1), :], (B, B)).T
                        gj = dsum[pl.ds(bj, 1), :]
                        sq = jnp.maximum(gi + gj - 2.0 * gsrc[dc, i], 0.0)
                        kk = jnp.exp(sq * (-1.0 / bandwidth))
                        kf[dst_r, dst_c] = kk.astype(jnp.bfloat16)
                        sacc[pl.ds(bj, 1), :] = sacc[pl.ds(bj, 1), :] + jnp.sum(kk, axis=0, keepdims=True)

                        @pl.when(n >= NP)
                        def _():
                            sacc[pl.ds(bi, 1), :] = sacc[pl.ds(bi, 1), :] + jnp.sum(kk.T, axis=0, keepdims=True)

                    @pl.when(n >= NB)
                    def _():
                        kf[dst_r, dst_c] = gsrc[dc, i].astype(jnp.bfloat16)

                    @pl.when(i < 10)
                    def _():
                        kyz_copy(lax.div(i, 2), y).start()

                    @pl.when(i >= 10)
                    def _():
                        ky_copy(dc, i - 10, y).start()

                @pl.when(i == CH - 1)
                def _():
                    for e in range(16):
                        @pl.when(me == e)
                        def _():
                            sg_local().start()

                        @pl.when(me != e)
                        def _():
                            sg_copy(e).start()

            for d in range(2):
                dist = 3 - z if d else z
                i = g - AG0 - LAG2 * dist

                @pl.when((i >= 0) & (i < CH))
                def _():
                    @pl.when((dist == 0) & (i < 10) & (lax.rem(i, 2) != y))
                    def _():
                        kyz_copy(lax.div(i, 2), 1 - y).wait_recv()

                    @pl.when(dist > 0)
                    def _():
                        kz_copy(d, i).wait_recv()

                    @pl.when(dist < 3)
                    def _():
                        kz_copy(d, i).start()

                    @pl.when((dist > 0) & (i >= 10))
                    def _():
                        ky_copy(d, i - 10, y).start()

                    kd_copy(d, i, c).start()
                    flip(slot_chain(i, d, y, c))

                k = i - OUT2 - 10

                @pl.when((k >= 0) & (k < 5))
                def _():
                    ky_copy(d, k, 1 - y).wait_recv()
                    ke_copy(d, k, c).start()
                    flip(slot_yf(k, d, 1 - y, c))

                j = i - DIE

                @pl.when((j >= 0) & (j < CH))
                def _():
                    kd_copy(d, j, 1 - c).wait_recv()
                    flip(slot_chain(j, d, y, 1 - c))

                m = k - DIE

                @pl.when((m >= 0) & (m < 5))
                def _():
                    ke_copy(d, m, 1 - c).wait_recv()
                    flip(slot_yf(m, d, 1 - y, 1 - c))

            p = g - (AG0 + 3 * LAG2 + DIE + 2)

            @pl.when((p >= 0) & (p < UP))
            def _():
                rows = pl.ds(pl.multiple_of(p * ROW, ROW), ROW)
                q = lax.rem(p, 3)
                half = lax.div(p, 3)
                hcol = pl.ds(pl.multiple_of(half * B, B), B)
                pmt = jnp.concatenate(
                    [kf[pl.ds(pl.multiple_of(NP * B + (q * 2 + h) * 16, 16), 16), hcol] for h in range(2)], axis=1
                )
                low = lax.dot_general(
                    pmt.astype(jnp.float32).T.astype(jnp.bfloat16),
                    ut_ref[...],
                    (((1,), (0,)), ((), ())),
                    preferred_element_type=jnp.float32,
                )
                cur = theta[rows, :]
                grad = -((cur - mu_ref[...]) * lam_ref[...] + low)
                a_ref[rows, :] = (grad - rep * cur).astype(jnp.bfloat16)

        for e in range(8):
            @pl.when(me != (e // 4) * 12 + e % 4)
            def _():
                dg_copy(e).wait_send()

        @pl.loop(0, 5)
        def _(k):
            for d in range(2):
                y_copy(d, k).wait_send()
                ke_copy(d, k, c).wait_send()
                ky_copy(d, k, y).wait_send()

            @pl.when(corner)
            def _():
                ye_copy(k, 2 * k + 1 - y).wait_send()
                kyz_copy(k, y).wait_send()

        @pl.loop(0, CH)
        def _(i):
            for d in range(2):
                pos = z if d else 3 - z

                @pl.when(pos < 3)
                def _():
                    z_copy(d, i).wait_send()

                @pl.when(pos > 0)
                def _():
                    kz_copy(d, i).wait_send()

                kd_copy(d, i, c).wait_send()

        @pl.when(corner)
        def _():
            for e in range(16):
                @pl.when(me != e)
                def _():
                    sg_copy(e).wait_send()

        tot = jnp.zeros((16, B), jnp.float32)
        for e in range(8):
            pltpu.make_async_copy(sacc, sgather.at[e], sg_r.at[e]).wait()
            tot = tot + sgather[e]
        ssum[...] = tot

        @pl.loop(0, UP)
        def _(p):
            rows = pl.ds(pl.multiple_of(p * ROW, ROW), ROW)
            acc = jnp.dot(kf[rows, :], a_ref[...], preferred_element_type=jnp.float32)
            cur = theta[rows, :]
            col = jnp.concatenate(
                [jnp.broadcast_to(ssum[pl.ds(p * 2 + h, 1), :], (B, B)).T[:, 0:1] for h in range(2)], axis=0
            )
            phi = (acc + (rep * col) * cur) * (1.0 / n_part)
            new = cur + step_size * phi
            theta[rows, :] = new

            @pl.when(step < NUM_STEPS - 1)
            def _():
                post(p, new)

            @pl.when(step == NUM_STEPS - 1)
            def _():
                out_copy(p).start()

    @pl.loop(0, UP)
    def _(p):
        out_copy(p).wait()


def solution(mesh):
    def run_steps(particles, prec_diag, mean_vec, low_rank):
        width = particles.shape[1]

        def local_steps(current, prec_loc, mean_loc, fac_loc):
            n_part, nf = current.shape
            dma = pltpu.SemaphoreType.DMA
            f32, bf16 = jnp.float32, jnp.bfloat16
            vmem = pltpu.VMEM
            return pl.pallas_call(
                functools.partial(kernel, width),
                out_shape=jax.ShapeDtypeStruct((n_part, nf), f32),
                in_specs=[pl.BlockSpec(memory_space=pl.ANY)] + [pl.BlockSpec(memory_space=pltpu.VMEM)] * 3,
                out_specs=pl.BlockSpec(memory_space=pl.ANY),
                scratch_shapes=[
                    vmem((n_part, nf), f32),
                    vmem((n_part, 2 * nf), bf16),
                    vmem((n_part, nf), bf16),
                    vmem((n_part + B, n_part), bf16),
                    vmem((2, CH, B, B), f32),
                    vmem((2, 5, B, B), f32),
                    vmem((2, CH, B, B), f32),
                    vmem((2, 5, B, B), f32),
                    vmem((5, B, B), f32),
                    vmem((2, B, B), f32),
                    vmem((B, B), f32),
                    vmem((16, B), f32),
                    vmem((16, 16, B), f32),
                    vmem((16, B), f32),
                    vmem((16, B), f32),
                    vmem((8, 16, B), f32),
                    vmem((16, B), f32),
                    dma((UP,)), dma((UP,)), dma((UP,)), dma((UP,)), dma, dma, dma((8,)), dma((16,)), dma((16,)), dma((8,)),
                    dma((2, CH)), dma((2, CH)), dma((2, 5)), dma((2, 5)), dma((5,)), dma((5,)),
                    dma((2, CH)), dma((2, CH)), dma((5,)), dma((5,)), dma((2, 5)), dma((2, 5)),
                    dma((2, CH)), dma((2, CH)), dma((2, 5)), dma((2, 5)),
                ],
                compiler_params=pltpu.CompilerParams(
                    collective_id=0, has_side_effects=True, vmem_limit_bytes=56 * 1024 * 1024
                ),
                name="svgd",
            )(current, prec_loc.reshape(1, nf), mean_loc.reshape(1, nf), fac_loc.T)

        sharded = jax.shard_map(
            local_steps,
            mesh=mesh,
            in_specs=(P("ens", FEAT_AXES), P(LEAD_AXES), P(LEAD_AXES), P(LEAD_AXES, None)),
            out_specs=P("ens", FEAT_AXES),
            check_vma=False,
        )
        return sharded(particles, prec_diag, mean_vec, low_rank)

    return run_steps
```

```python
import functools

import jax
import jax.numpy as jnp
from jax import lax
from jax.experimental import pallas as pl
from jax.experimental.pallas import tpu as pltpu
from jax.sharding import PartitionSpec as P

NUM_STEPS = 3
BAND_SCALE = 4.0
STEP_SCALE = 0.4
FEAT_AXES = ("slab", "feat")
LEAD_AXES = ("ens", "slab", "feat")
MESH = pl.DeviceIdType.MESH

B = 128
NP = 12
NB = 78
ROW = 256
UP = 6
LAG = 4
END = 4
OUT1 = 4
LAG2 = 4
OUT2 = 4
DIE = 3
FIN0 = 3 * LAG + END
AG0 = FIN0 + OUT1
CH = 15
ITERS = AG0 + 3 * LAG2 + CH + OUT2 + DIE


def _block(n):
    e = lax.div(n, NB)
    i = lax.rem(n, NP)
    j = lax.rem(i + lax.div(n, NP), NP)
    return (1 - e) * i + e * NP, (1 - e) * j + e * (n - NB)


def _at(k_ref, n):
    i, j = _block(n)
    return k_ref.at[pl.ds(pl.multiple_of(i * B, B), B), pl.ds(pl.multiple_of(j * B, B), B)]


def kernel(width, x_hbm, lam_ref, mu_ref, ut_ref, o_hbm, theta, th, a_ref, kf, gsrc, gy, zrecv, yrecv, yend, pmb, pmrecv,
           dsrc, dgather, dsum, sacc, sgather, ssum, ld, od, thd_s, thd_r, pm_s, pm_r, dg_s, dg_r, sg_s, sg_r, zs, zr, ys, yr,
           ye_s, ye_r, kz_s, kz_r, kyz_s, kyz_r, ky_s, ky_r, kd_s, kd_r, ke_s, ke_r):
    nf = theta.shape[1]
    n_part = theta.shape[0]
    bandwidth = BAND_SCALE * width
    step_size = STEP_SCALE * width
    rep = 2.0 / bandwidth
    ens = lax.axis_index("ens")
    z = lax.axis_index("slab")
    feat = lax.axis_index("feat")
    y = lax.div(feat, 2)
    c = lax.rem(feat, 2)
    me = z * 4 + feat
    ypart = (ens, z, (1 - y) * 2 + c)
    dpart = (ens, z, y * 2 + 1 - c)
    dc = lax.div(z, 3)
    corner = lax.rem(z, 3) == 0
    own8 = (dc * 2 + y) * 2 + c

    def rcopy(src, dst, s, r, dev):
        return pltpu.make_async_remote_copy(src_ref=src, dst_ref=dst, send_sem=s, recv_sem=r, device_id=dev, device_id_type=MESH)

    def zdev(dz):
        return (ens, z + dz, feat)

    def slot_chain(i, d, yy, cc):
        w = lax.div(i, 10)
        zf = lax.div(i, 2) * 16 + d * 4 + lax.rem(i, 2) * 2
        yf = (i - 10) * 16 + 8 + d * 4 + yy * 2
        return lax.rem((1 - w) * zf + w * yf + cc + NB, 80)

    def slot_yf(k, d, yy, cc):
        return lax.rem(k * 16 + 8 + d * 4 + yy * 2 + cc + NB, 80)

    def load_copy(p):
        rows = pl.ds(pl.multiple_of(p * ROW, ROW), ROW)
        return pltpu.make_async_copy(x_hbm.at[rows], theta.at[rows], ld.at[p])

    def out_copy(p):
        rows = pl.ds(pl.multiple_of(p * ROW, ROW), ROW)
        return pltpu.make_async_copy(theta.at[rows], o_hbm.at[rows], od.at[p])

    def th_copy(p):
        rows = pl.ds(pl.multiple_of(p * ROW, ROW), ROW)
        return rcopy(th.at[rows, pl.ds(0, nf)], th.at[rows, pl.ds(nf, nf)], thd_s.at[p], thd_r.at[p], dpart)

    def pm_copy():
        return rcopy(pmb.at[1 - c], pmrecv, pm_s, pm_r, dpart)

    def dg_copy(e):
        dev = (ens, (e // 4) * 3, e % 4)
        return rcopy(dsrc, dgather.at[me], dg_s.at[e], dg_r.at[me], dev)

    def dg_local():
        return pltpu.make_async_copy(dsrc, dgather.at[me], dg_r.at[me])

    def sg_copy(e):
        dev = (ens, e // 4, e % 4)
        return rcopy(sacc, sgather.at[own8], sg_s.at[e], sg_r.at[own8], dev)

    def sg_local():
        return pltpu.make_async_copy(sacc, sgather.at[own8], sg_r.at[own8])

    def z_copy(d, i):
        return rcopy(gsrc.at[d, i], zrecv.at[d, i], zs.at[d, i], zr.at[d, i], zdev(2 * d - 1))

    def y_copy(d, k):
        return rcopy(gy.at[d, k], yrecv.at[d, k], ys.at[d, k], yr.at[d, k], ypart)

    def ye_copy(k, i):
        return rcopy(gsrc.at[dc, i], yend.at[k], ye_s.at[k], ye_r.at[k], ypart)

    def kz_copy(d, i):
        blk = _at(kf, slot_chain(i, d, y, c))
        return rcopy(blk, blk, kz_s.at[d, i], kz_r.at[d, i], zdev(1 - 2 * d))

    def kyz_copy(k, ey):
        blk = _at(kf, lax.rem(k * 16 + dc * 4 + ey * 2 + c + NB, 80))
        return rcopy(blk, blk, kyz_s.at[k], kyz_r.at[k], ypart)

    def ky_copy(d, k, yy):
        blk = _at(kf, slot_yf(k, d, yy, c))
        return rcopy(blk, blk, ky_s.at[d, k], ky_r.at[d, k], ypart)

    def kd_copy(d, i, cc):
        blk = _at(kf, slot_chain(i, d, y, cc))
        return rcopy(blk, blk, kd_s.at[d, i], kd_r.at[d, i], dpart)

    def ke_copy(d, k, cc):
        blk = _at(kf, slot_yf(k, d, 1 - y, cc))
        return rcopy(blk, blk, ke_s.at[d, k], ke_r.at[d, k], dpart)

    def flip(n):
        i, j = _block(n)

        @pl.when((n >= NP) & (n < NB))
        def _():
            src = kf[pl.ds(pl.multiple_of(i * B, B), B), pl.ds(pl.multiple_of(j * B, B), B)]
            kf[pl.ds(pl.multiple_of(j * B, B), B), pl.ds(pl.multiple_of(i * B, B), B)] = (
                src.astype(jnp.float32).T.astype(jnp.bfloat16)
            )

    def gram(n):
        i, j = _block(n)
        return lax.dot_general(
            th[pl.ds(pl.multiple_of(i * B, B), B), :],
            th[pl.ds(pl.multiple_of(j * B, B), B), :],
            (((1,), (1,)), ((), ())),
            preferred_element_type=jnp.float32,
        )

    def post(p, new):
        rows = pl.ds(pl.multiple_of(p * ROW, ROW), ROW)
        tb = new.astype(jnp.bfloat16)
        th[rows, pl.ds(0, nf)] = tb
        th_copy(p).start()
        xb = (new - mu_ref[...]).astype(jnp.bfloat16)
        pm = lax.dot_general(ut_ref[...], xb, (((1,), (1,)), ((), ())), preferred_element_type=jnp.float32)
        half = lax.div(p, 3)
        for h in range(2):
            q = lax.rem(p, 3) * 2 + h
            pmb[half, pl.ds(pl.multiple_of(q * 16, 16), 16), :] = pm[:, h * B:(h + 1) * B]
            t = tb[h * B:(h + 1) * B, :].astype(jnp.float32)
            sq = t * t
            tot = sq[:, 0:B]
            for m in range(1, nf // B):
                tot = tot + sq[:, m * B:(m + 1) * B]
            dsrc[pl.ds(p * 2 + h, 1), :] = jnp.sum(tot.T, axis=0, keepdims=True)

    barrier = pltpu.get_barrier_semaphore()
    for o in range(1, 16):
        e = lax.rem(me + o, 16)
        pl.semaphore_signal(barrier, inc=1, device_id=(ens, lax.div(e, 4), lax.rem(e, 4)), device_id_type=MESH)
    for p in range(UP):
        load_copy(p).start()
    pmb[...] = jnp.zeros_like(pmb)
    dsrc[...] = jnp.zeros_like(dsrc)
    pl.semaphore_wait(barrier, 15)

    @pl.loop(0, UP)
    def _(p):
        load_copy(p).wait()
        rows = pl.ds(pl.multiple_of(p * ROW, ROW), ROW)
        post(p, theta[rows, :])

    @pl.loop(0, NUM_STEPS)
    def _(step):
        for e in range(8):
            mine = me == (e // 4) * 12 + e % 4

            @pl.when(mine)
            def _():
                dg_local().start()

            @pl.when(jnp.logical_not(mine))
            def _():
                dg_copy(e).start()

        pm_copy().start()
        sacc[...] = jnp.zeros_like(sacc)

        @pl.loop(0, UP)
        def _(p):
            th_copy(p).wait()

        pm_copy().wait()

        @pl.loop(0, 5)
        def _(k):
            for d in range(2):
                gy[d, k] = gram(slot_yf(k, d, 1 - y, c))
            for d in range(2):
                y_copy(d, k).start()

        @pl.loop(0, ITERS)
        def _(g):
            for d in range(2):
                pos = z if d else 3 - z
                i = g - LAG * pos

                @pl.when((i >= 0) & (i < CH))
                def _():
                    n = slot_chain(i, d, y, c)

                    @pl.when(n < NB)
                    def _():
                        gsrc[d, i] = gram(n)

                    if d == 0:
                        @pl.when(n >= NB)
                        def _():
                            gsrc[d, i] = pmb[c] + pmrecv[...]

                    @pl.when(i >= 10)
                    def _():
                        y_copy(d, i - 10).wait_recv()
                        gsrc[d, i] = gsrc[d, i] + yrecv[d, i - 10]

                    @pl.when(pos > 0)
                    def _():
                        z_copy(d, i).wait_recv()
                        gsrc[d, i] = gsrc[d, i] + zrecv[d, i]

            for d in range(2):
                pos = z if d else 3 - z
                i = g - LAG * pos

                @pl.when((i >= 0) & (i < CH))
                def _():
                    @pl.when(pos < 3)
                    def _():
                        z_copy(d, i).start()

                    @pl.when((pos == 3) & (i < 10) & (lax.rem(i, 2) != y))
                    def _():
                        ye_copy(lax.div(i, 2), i).start()

            i = g - FIN0

            @pl.when(corner & (i >= 0) & (i < CH))
            def _():
                @pl.when(i == 0)
                def _():
                    tot = jnp.zeros((16, B), jnp.float32)
                    for e in range(16):
                        pltpu.make_async_copy(dsrc, dgather.at[e], dg_r.at[e]).wait()
                        tot = tot + dgather[e]
                    dsum[...] = tot

                @pl.when((i >= 10) | (lax.rem(i, 2) == y))
                def _():
                    @pl.when(i < 10)
                    def _():
                        k = lax.div(i, 2)
                        ye_copy(k, i).wait_recv()
                        gsrc[dc, i] = gsrc[dc, i] + yend[k]

                    n = slot_chain(i, dc, y, c)
                    bi, bj = _block(n)
                    dst_r = pl.ds(pl.multiple_of(bi * B, B), B)
                    dst_c = pl.ds(pl.multiple_of(bj * B, B), B)

                    @pl.when(n < NB)
                    def _():
                        gi = jnp.broadcast_to(dsum[pl.ds(bi, 1), :], (B, B)).T
                        gj = dsum[pl.ds(bj, 1), :]
                        sq = jnp.maximum(gi + gj - 2.0 * gsrc[dc, i], 0.0)
                        kk = jnp.exp(sq * (-1.0 / bandwidth))
                        kf[dst_r, dst_c] = kk.astype(jnp.bfloat16)
                        sacc[pl.ds(bj, 1), :] = sacc[pl.ds(bj, 1), :] + jnp.sum(kk, axis=0, keepdims=True)

                        @pl.when(n >= NP)
                        def _():
                            sacc[pl.ds(bi, 1), :] = sacc[pl.ds(bi, 1), :] + jnp.sum(kk.T, axis=0, keepdims=True)

                    @pl.when(n >= NB)
                    def _():
                        kf[dst_r, dst_c] = gsrc[dc, i].astype(jnp.bfloat16)

                    @pl.when(i < 10)
                    def _():
                        kyz_copy(lax.div(i, 2), y).start()

                    @pl.when(i >= 10)
                    def _():
                        ky_copy(dc, i - 10, y).start()

                @pl.when(i == CH - 1)
                def _():
                    for e in range(16):
                        @pl.when(me == e)
                        def _():
                            sg_local().start()

                        @pl.when(me != e)
                        def _():
                            sg_copy(e).start()

            for d in range(2):
                dist = 3 - z if d else z
                i = g - AG0 - LAG2 * dist

                @pl.when((i >= 0) & (i < CH))
                def _():
                    @pl.when((dist == 0) & (i < 10) & (lax.rem(i, 2) != y))
                    def _():
                        kyz_copy(lax.div(i, 2), 1 - y).wait_recv()

                    @pl.when(dist > 0)
                    def _():
                        kz_copy(d, i).wait_recv()

                    @pl.when(dist < 3)
                    def _():
                        kz_copy(d, i).start()

                    @pl.when((dist > 0) & (i >= 10))
                    def _():
                        ky_copy(d, i - 10, y).start()

                    kd_copy(d, i, c).start()
                    flip(slot_chain(i, d, y, c))

                k = i - OUT2 - 10

                @pl.when((k >= 0) & (k < 5))
                def _():
                    ky_copy(d, k, 1 - y).wait_recv()
                    ke_copy(d, k, c).start()
                    flip(slot_yf(k, d, 1 - y, c))

                j = i - DIE

                @pl.when((j >= 0) & (j < CH))
                def _():
                    kd_copy(d, j, 1 - c).wait_recv()
                    flip(slot_chain(j, d, y, 1 - c))

                m = k - DIE

                @pl.when((m >= 0) & (m < 5))
                def _():
                    ke_copy(d, m, 1 - c).wait_recv()
                    flip(slot_yf(m, d, 1 - y, 1 - c))

            p = g - (AG0 + 3 * LAG2 + DIE + 2)

            @pl.when((p >= 0) & (p < UP))
            def _():
                rows = pl.ds(pl.multiple_of(p * ROW, ROW), ROW)
                q = lax.rem(p, 3)
                half = lax.div(p, 3)
                hcol = pl.ds(pl.multiple_of(half * B, B), B)
                pmt = jnp.concatenate(
                    [kf[pl.ds(pl.multiple_of(NP * B + (q * 2 + h) * 16, 16), 16), hcol] for h in range(2)], axis=1
                )
                low = lax.dot_general(
                    pmt.astype(jnp.float32).T.astype(jnp.bfloat16),
                    ut_ref[...],
                    (((1,), (0,)), ((), ())),
                    preferred_element_type=jnp.float32,
                )
                cur = theta[rows, :]
                grad = -((cur - mu_ref[...]) * lam_ref[...] + low)
                a_ref[rows, :] = (grad - rep * cur).astype(jnp.bfloat16)

        for e in range(8):
            @pl.when(me != (e // 4) * 12 + e % 4)
            def _():
                dg_copy(e).wait_send()

        @pl.loop(0, 5)
        def _(k):
            for d in range(2):
                y_copy(d, k).wait_send()
                ke_copy(d, k, c).wait_send()
                ky_copy(d, k, y).wait_send()

            @pl.when(corner)
            def _():
                ye_copy(k, 2 * k + 1 - y).wait_send()
                kyz_copy(k, y).wait_send()

        @pl.loop(0, CH)
        def _(i):
            for d in range(2):
                pos = z if d else 3 - z

                @pl.when(pos < 3)
                def _():
                    z_copy(d, i).wait_send()

                @pl.when(pos > 0)
                def _():
                    kz_copy(d, i).wait_send()

                kd_copy(d, i, c).wait_send()

        @pl.when(corner)
        def _():
            for e in range(16):
                @pl.when(me != e)
                def _():
                    sg_copy(e).wait_send()

        tot = jnp.zeros((16, B), jnp.float32)
        for e in range(8):
            pltpu.make_async_copy(sacc, sgather.at[e], sg_r.at[e]).wait()
            tot = tot + sgather[e]
        ssum[...] = tot

        @pl.loop(0, UP)
        def _(p):
            rows = pl.ds(pl.multiple_of(p * ROW, ROW), ROW)
            acc = jnp.dot(kf[rows, :], a_ref[...], preferred_element_type=jnp.float32)
            cur = theta[rows, :]
            col = jnp.concatenate(
                [jnp.broadcast_to(ssum[pl.ds(p * 2 + h, 1), :], (B, B)).T[:, 0:1] for h in range(2)], axis=0
            )
            phi = (acc + (rep * col) * cur) * (1.0 / n_part)
            new = cur + step_size * phi
            theta[rows, :] = new

            @pl.when(step < NUM_STEPS - 1)
            def _():
                post(p, new)

            @pl.when(step == NUM_STEPS - 1)
            def _():
                out_copy(p).start()

    @pl.loop(0, UP)
    def _(p):
        out_copy(p).wait()


def solution(mesh):
    def run_steps(particles, prec_diag, mean_vec, low_rank):
        width = particles.shape[1]

        def local_steps(current, prec_loc, mean_loc, fac_loc):
            n_part, nf = current.shape
            dma = pltpu.SemaphoreType.DMA
            f32, bf16 = jnp.float32, jnp.bfloat16
            vmem = pltpu.VMEM
            return pl.pallas_call(
                functools.partial(kernel, width),
                out_shape=jax.ShapeDtypeStruct((n_part, nf), f32),
                in_specs=[pl.BlockSpec(memory_space=pl.ANY)] + [pl.BlockSpec(memory_space=pltpu.VMEM)] * 3,
                out_specs=pl.BlockSpec(memory_space=pl.ANY),
                scratch_shapes=[
                    vmem((n_part, nf), f32),
                    vmem((n_part, 2 * nf), bf16),
                    vmem((n_part, nf), bf16),
                    vmem((n_part + B, n_part), bf16),
                    vmem((2, CH, B, B), f32),
                    vmem((2, 5, B, B), f32),
                    vmem((2, CH, B, B), f32),
                    vmem((2, 5, B, B), f32),
                    vmem((5, B, B), f32),
                    vmem((2, B, B), f32),
                    vmem((B, B), f32),
                    vmem((16, B), f32),
                    vmem((16, 16, B), f32),
                    vmem((16, B), f32),
                    vmem((16, B), f32),
                    vmem((8, 16, B), f32),
                    vmem((16, B), f32),
                    dma((UP,)), dma((UP,)), dma((UP,)), dma((UP,)), dma, dma, dma((8,)), dma((16,)), dma((16,)), dma((8,)),
                    dma((2, CH)), dma((2, CH)), dma((2, 5)), dma((2, 5)), dma((5,)), dma((5,)),
                    dma((2, CH)), dma((2, CH)), dma((5,)), dma((5,)), dma((2, 5)), dma((2, 5)),
                    dma((2, CH)), dma((2, CH)), dma((2, 5)), dma((2, 5)),
                ],
                compiler_params=pltpu.CompilerParams(
                    collective_id=0, has_side_effects=True, vmem_limit_bytes=56 * 1024 * 1024
                ),
                name="svgd",
            )(current, prec_loc.reshape(1, nf), mean_loc.reshape(1, nf), fac_loc.T)

        sharded = jax.shard_map(
            local_steps,
            mesh=mesh,
            in_specs=(P("ens", FEAT_AXES), P(LEAD_AXES), P(LEAD_AXES), P(LEAD_AXES, None)),
            out_specs=P("ens", FEAT_AXES),
            check_vma=False,
        )
        return sharded(particles, prec_diag, mean_vec, low_rank)

    return run_steps
```

```python
import functools

import jax
import jax.numpy as jnp
from jax import lax
from jax.experimental import pallas as pl
from jax.experimental.pallas import tpu as pltpu
from jax.sharding import PartitionSpec as P

NUM_STEPS = 3
BAND_SCALE = 4.0
STEP_SCALE = 0.4
FEAT_AXES = ("slab", "feat")
LEAD_AXES = ("ens", "slab", "feat")
MESH = pl.DeviceIdType.MESH

B = 128
ROW = 256
UP = 6
START = 2
LAG = 3
END = 2
OUT1 = 2
LAG2 = 4
OUT2 = 4
DIE = 3
YF0 = 3
FIN0 = START + 3 * LAG + END
AG0 = FIN0 + OUT1
CH = 15
PM = 6
DRV0 = AG0 + 3 * LAG2 + PM + 1 + DIE + 1
ITERS = AG0 + 3 * LAG2 + CH + OUT2 + DIE


def _ref(k, t, d, ey, c):
    f = lax.div(k, 4)
    return k * 16 + (1 - f) * (t * 8 + d * 4 + ey * 2 + c) + f * (t * 4 + d * 2 + ey)


def _block(n):
    p = lax.div(n + 126, B) + lax.div(n + 120, B) + lax.div(n + 110, B) + lax.div(n + 96, B) + lax.div(n + 78, B)
    r = n - 2 * p * p
    i = lax.div(r, 2)
    j = 2 * p + lax.rem(r, 2)
    return i, j, p, 1 - jnp.minimum(j - i, 1)


def _clip(i, n):
    return jnp.minimum(jnp.maximum(i, 0), n - 1)


def _span(i):
    return pl.ds(pl.multiple_of(i * B, B), B)


def _home(n):
    i, j, p, e = _block(n)
    return _span(i + e * (2 * UP - i)), _span(j + e * (p - j))


def kernel(width, x_hbm, lam_ref, mu_ref, ut_ref, o_hbm, theta, th, a_ref, kf, gsrc, gy, zrecv, yrecv, yend, pmb, pmrecv,
           ps, pzr, pye, pmf,
           dsrc, dgather, dsum, sacc, sgather, ssum, ld, od, thd_s, thd_r, pm_s, pm_r, dg_s, dg_r, sg_s, sg_r,
           zs, zr, ys, yr, ye_s, ye_r, kz_s, kz_r, kyz_s, kyz_r, ky_s, ky_r, kd_s, kd_r, ke_s, ke_r,
           pz_s, pz_r, pye_s, pye_r, pky_s, pky_r, pkz_s, pkz_r, pkd_s, pkd_r):
    nf = theta.shape[1]
    n_part = theta.shape[0]
    bandwidth = BAND_SCALE * width
    step_size = STEP_SCALE * width
    rep = 2.0 / bandwidth
    f32, bf16 = jnp.float32, jnp.bfloat16
    ens = lax.axis_index("ens")
    z = lax.axis_index("slab")
    feat = lax.axis_index("feat")
    y = lax.div(feat, 2)
    c = lax.rem(feat, 2)
    me = z * 4 + feat
    ypart = (ens, z, (1 - y) * 2 + c)
    dpart = (ens, z, y * 2 + 1 - c)
    dc = lax.div(z, 3)
    corner = lax.rem(z, 3) == 0
    own8 = (dc * 2 + y) * 2 + c
    rounds = 4 + c
    chain = 3 * rounds
    other_chain = 27 - chain

    def rcopy(src, dst, s, r, dev):
        return pltpu.make_async_remote_copy(src_ref=src, dst_ref=dst, send_sem=s, recv_sem=r, device_id=dev, device_id_type=MESH)

    def zdev(dz):
        return (ens, z + dz, feat)

    def place(i, cc):
        zf = 8 + 2 * cc
        w = lax.div(i, zf)
        return w, (1 - w) * lax.div(i, 2) + w * (i - zf), lax.rem(i, 2)

    def num_chain(i, d, cc):
        w, k, e = place(i, cc)
        return _ref(k, w, d, (1 - w) * e + w * y, cc)

    def panel(p):
        return pl.ds(pl.multiple_of(p * ROW, ROW), ROW)

    def load_copy(p):
        return pltpu.make_async_copy(x_hbm.at[panel(p)], theta.at[panel(p)], ld.at[p])

    def out_copy(p):
        return pltpu.make_async_copy(theta.at[panel(p)], o_hbm.at[panel(p)], od.at[p])

    def th_copy(p):
        return rcopy(th.at[panel(p), pl.ds(0, nf)], th.at[panel(p), pl.ds(nf, nf)], thd_s.at[p], thd_r.at[p], dpart)

    def pm_copy():
        return rcopy(pmb.at[1 - c], pmrecv, pm_s, pm_r, dpart)

    def dg_copy(e):
        return rcopy(dsrc, dgather.at[me], dg_s.at[e], dg_r.at[me], (ens, (e // 4) * 3, e % 4))

    def dg_local():
        return pltpu.make_async_copy(dsrc, dgather.at[me], dg_r.at[me])

    def sg_copy(e):
        return rcopy(sacc, sgather.at[own8], sg_s.at[e], sg_r.at[own8], (ens, e // 4, e % 4))

    def sg_local():
        return pltpu.make_async_copy(sacc, sgather.at[own8], sg_r.at[own8])

    def z_copy(d, i):
        return rcopy(gsrc.at[d, i], zrecv.at[d, i], zs.at[d, i], zr.at[d, i], zdev(2 * d - 1))

    def y_copy(d, k):
        return rcopy(gy.at[d, k], yrecv.at[d, k], ys.at[d, k], yr.at[d, k], ypart)

    def ye_copy(k, i):
        return rcopy(gsrc.at[dc, i], yend.at[k], ye_s.at[k], ye_r.at[k], ypart)

    def kf_copy(n, s, r, dev):
        rows, cols = _home(n)
        return rcopy(kf.at[rows, cols], kf.at[rows, cols], s, r, dev)

    def kz_copy(d, i):
        return kf_copy(num_chain(i, d, c), kz_s.at[d, i], kz_r.at[d, i], zdev(1 - 2 * d))

    def kyz_copy(k, ey):
        return kf_copy(_ref(k, 0, dc, ey, c), kyz_s.at[k], kyz_r.at[k], ypart)

    def ky_copy(d, k, yy):
        return kf_copy(_ref(k, 1, d, yy, c), ky_s.at[d, k], ky_r.at[d, k], ypart)

    def kd_copy(d, i, cc):
        return kf_copy(num_chain(i, d, cc), kd_s.at[d, i], kd_r.at[d, i], dpart)

    def ke_copy(d, k, cc):
        return kf_copy(_ref(k, 1, d, 1 - y, cc), ke_s.at[d, k], ke_r.at[d, k], dpart)

    def pz_copy(d, e):
        return rcopy(ps.at[d, e], pzr.at[d, e], pz_s.at[d, e], pz_r.at[d, e], zdev(2 * d - 1))

    def pye_copy(e):
        return rcopy(ps.at[dc, e], pye, pye_s, pye_r, ypart)

    def pf_copy(d, e, cc, s, r, dev):
        return rcopy(pmf.at[cc, 2 * d + e], pmf.at[cc, 2 * d + e], s, r, dev)

    def pky_copy(e):
        return pf_copy(dc, e, c, pky_s, pky_r, ypart)

    def pkz_copy(d, e):
        return pf_copy(d, e, c, pkz_s.at[d, e], pkz_r.at[d, e], zdev(1 - 2 * d))

    def pkd_copy(d, e, cc):
        return pf_copy(d, e, cc, pkd_s.at[d, e], pkd_r.at[d, e], dpart)

    def low_tri():
        return lax.broadcasted_iota(jnp.int32, (B, B), 0) - lax.broadcasted_iota(jnp.int32, (B, B), 1)

    def unpack(kk):
        kt = kk.T
        tri = low_tri()
        return jnp.where(tri >= 0, kk, kt), jnp.where(tri < 0, kk, jnp.where(tri == 0, 1.0, kt))

    def mirror(n):
        i, j, p, e = _block(n)

        @pl.when(e == 0)
        def _():
            kf[_span(j), _span(i)] = kf[_span(i), _span(j)].astype(f32).T.astype(bf16)

        @pl.when(e == 1)
        def _():
            first, second = unpack(kf[pl.ds(2 * UP * B, B), _span(p)].astype(f32))
            kf[_span(2 * p), _span(2 * p)] = first.astype(bf16)
            kf[_span(2 * p + 1), _span(2 * p + 1)] = second.astype(bf16)

    def dot_t(i, j):
        return lax.dot_general(th[_span(i), :], th[_span(j), :], (((1,), (1,)), ((), ())), preferred_element_type=f32)

    def gram(dst, n):
        i, j, p, e = _block(n)
        dst[...] = dot_t(i, j)

        @pl.when(e == 1)
        def _():
            dst[...] = jnp.where(low_tri() >= 0, dst[...], dot_t(2 * p + 1, 2 * p + 1))

    def post(p):
        new = theta[panel(p), :]
        tb = new.astype(bf16)
        th[panel(p), pl.ds(0, nf)] = tb
        xb = (new - mu_ref[...]).astype(bf16)
        pm = lax.dot_general(ut_ref[...], xb, (((1,), (1,)), ((), ())), preferred_element_type=f32)
        th_copy(p).start()
        half = lax.div(p, 3)
        for h in range(2):
            q = lax.rem(p, 3) * 2 + h
            pmb[half, pl.ds(pl.multiple_of(q * 16, 16), 16), :] = pm[:, h * B:(h + 1) * B]
            t = tb[h * B:(h + 1) * B, :].astype(f32)
            sq = t * t
            tot = sq[:, 0:B]
            for m in range(1, nf // B):
                tot = tot + sq[:, m * B:(m + 1) * B]
            dsrc[pl.ds(p * 2 + h, 1), :] = jnp.sum(tot.T, axis=0, keepdims=True)

    def row_sums():
        tot = jnp.zeros((16, B), f32)
        for e in range(8):
            pltpu.make_async_copy(sacc, sgather.at[e], sg_r.at[e]).wait()
            tot = tot + sgather[e]
        ssum[...] = tot

    def update(p):
        acc = jnp.dot(kf[panel(p), :], a_ref[...], preferred_element_type=f32)
        cur = theta[panel(p), :]
        col = jnp.concatenate(
            [jnp.broadcast_to(ssum[pl.ds(p * 2 + h, 1), :], (B, B)).T[:, 0:1] for h in range(2)], axis=0
        )
        phi = (acc + (rep * col) * cur) * (1.0 / n_part)
        theta[panel(p), :] = cur + step_size * phi

    barrier = pltpu.get_barrier_semaphore()
    for o in range(1, 16):
        e = lax.rem(me + o, 16)
        pl.semaphore_signal(barrier, inc=1, device_id=(ens, lax.div(e, 4), lax.rem(e, 4)), device_id_type=MESH)
    for p in range(UP):
        load_copy(p).start()
    pmb[...] = jnp.zeros_like(pmb)
    dsrc[...] = jnp.zeros_like(dsrc)
    pl.semaphore_wait(barrier, 15)

    @pl.loop(0, NUM_STEPS)
    def _(step):
        @pl.when(step > 0)
        def _():
            row_sums()

        sacc[...] = jnp.zeros_like(sacc)

        @pl.loop(0, ITERS)
        def _(g):
            gp = jnp.minimum(g, UP - 1)

            @pl.when(g < UP)
            def _():
                @pl.when(step == 0)
                def _():
                    load_copy(gp).wait()

                @pl.when(step > 0)
                def _():
                    update(gp)

                post(gp)

            @pl.when(g == UP - 1)
            def _():
                for e in range(8):
                    mine = me == (e // 4) * 12 + e % 4

                    @pl.when(mine)
                    def _():
                        dg_local().start()

                    @pl.when(jnp.logical_not(mine))
                    def _():
                        dg_copy(e).start()

                pm_copy().start()

            @pl.when((g >= 1) & (g <= UP))
            def _():
                th_copy(_clip(g - 1, UP)).wait()

            @pl.when(g == START + PM)
            def _():
                pm_copy().wait()

            v = g - YF0
            v_on = (v >= 0) & (v < 2 * rounds)
            v = _clip(v, 2 * rounds)

            @pl.when(v_on)
            def _():
                d, k = lax.rem(v, 2), lax.div(v, 2)
                gram(gy.at[d, k], _ref(k, 1, d, 1 - y, c))

            for d in range(2):
                pos = z if d else 3 - z
                i = g - START - LAG * pos
                on = (i >= 0) & (i < chain)
                i = _clip(i, chain)

                @pl.when(on)
                def _():
                    w, k, e = place(i, c)
                    gram(gsrc.at[d, i], _ref(k, w, d, (1 - w) * e + w * y, c))

                    @pl.when(w == 1)
                    def _():
                        y_copy(d, k).wait_recv()
                        gsrc[d, i] = gsrc[d, i] + yrecv[d, k]

                    @pl.when(pos > 0)
                    def _():
                        z_copy(d, i).wait_recv()
                        gsrc[d, i] = gsrc[d, i] + zrecv[d, i]

                    @pl.when((i >= PM) & (i < PM + 2))
                    def _():
                        rows = pl.ds(pl.multiple_of((2 * d + e) * 32, 32), 32)
                        ps[d, e] = pmb[c, rows, :] + pmrecv[rows, :]

                        @pl.when(pos > 0)
                        def _():
                            pz_copy(d, e).wait_recv()
                            ps[d, e] = ps[d, e] + pzr[d, e]

            @pl.when(v_on)
            def _():
                y_copy(lax.rem(v, 2), lax.div(v, 2)).start()

            for d in range(2):
                pos = z if d else 3 - z
                i = g - START - LAG * pos
                on = (i >= 0) & (i < chain)
                i = _clip(i, chain)

                @pl.when(on)
                def _():
                    w, k, e = place(i, c)
                    cross = (pos == 3) & (w == 0) & (e != y)
                    rides = (i >= PM) & (i < PM + 2)

                    @pl.when((pos < 3) & rides)
                    def _():
                        pz_copy(d, e).start()

                    @pl.when(pos < 3)
                    def _():
                        z_copy(d, i).start()

                    @pl.when(cross & rides)
                    def _():
                        pye_copy(e).start()

                    @pl.when(cross)
                    def _():
                        ye_copy(k, i).start()

            i = g - FIN0
            on = corner & (i >= 0) & (i < chain)
            i = _clip(i, chain)

            @pl.when(on)
            def _():
                @pl.when(i == 0)
                def _():
                    tot = jnp.zeros((16, B), f32)
                    for e in range(16):
                        pltpu.make_async_copy(dsrc, dgather.at[e], dg_r.at[e]).wait()
                        tot = tot + dgather[e]
                    dsum[...] = tot

                w, k, e = place(i, c)

                @pl.when((w == 1) | (e == y))
                def _():
                    @pl.when(w == 0)
                    def _():
                        ye_copy(k, i).wait_recv()
                        gsrc[dc, i] = gsrc[dc, i] + yend[k]

                    n = num_chain(i, dc, c)
                    bi, bj, bp, be = _block(n)

                    def kern(gi, gj):
                        sq = jnp.maximum(gi + gj - 2.0 * gsrc[dc, i], 0.0)
                        return jnp.exp(sq * (-1.0 / bandwidth))

                    def add_sums(q, blk):
                        sacc[pl.ds(q, 1), :] = sacc[pl.ds(q, 1), :] + jnp.sum(blk, axis=0, keepdims=True)

                    @pl.when(be == 0)
                    def _():
                        kk = kern(jnp.broadcast_to(dsum[pl.ds(bi, 1), :], (B, B)).T, dsum[pl.ds(bj, 1), :])
                        kf[_span(bi), _span(bj)] = kk.astype(bf16)
                        add_sums(bj, kk)
                        add_sums(bi, kk.T)

                    @pl.when(be == 1)
                    def _():
                        tri = low_tri() >= 0
                        ga = jnp.broadcast_to(dsum[pl.ds(2 * bp, 1), :], (B, B))
                        gb = jnp.broadcast_to(dsum[pl.ds(2 * bp + 1, 1), :], (B, B))
                        kk = kern(jnp.where(tri, ga.T, gb.T), jnp.where(tri, ga, gb))
                        kk = jnp.where(low_tri() == 0, 1.0, kk)
                        kf[pl.ds(2 * UP * B, B), _span(bp)] = kk.astype(bf16)
                        first, second = unpack(kk)
                        add_sums(2 * bp, first)
                        add_sums(2 * bp + 1, second)

                    @pl.when((i >= PM) & (i < PM + 2))
                    def _():
                        pye_copy(e).wait_recv()
                        pmf[c, 2 * dc + e] = (ps[dc, e] + pye[...]).astype(bf16)
                        pky_copy(e).start()

                    @pl.when(w == 0)
                    def _():
                        kyz_copy(k, y).start()

                    @pl.when(w == 1)
                    def _():
                        ky_copy(dc, k, y).start()

                @pl.when(i == chain - 1)
                def _():
                    for o in range(16):
                        @pl.when(me == o)
                        def _():
                            sg_local().start()

                        @pl.when(me != o)
                        def _():
                            sg_copy(o).start()

            for d in range(2):
                dist = 3 - z if d else z
                h = g - AG0 - LAG2 * dist
                on = (h >= 0) & (h < chain)
                i = _clip(h, chain)

                @pl.when(on)
                def _():
                    w, k, e = place(i, c)
                    turn = (dist == 0) & (w == 0) & (e != y)

                    @pl.when((i >= PM) & (i < PM + 2))
                    def _():
                        @pl.when(turn)
                        def _():
                            pky_copy(1 - y).wait_recv()

                        @pl.when(dist > 0)
                        def _():
                            pkz_copy(d, e).wait_recv()

                        @pl.when(dist < 3)
                        def _():
                            pkz_copy(d, e).start()

                        pkd_copy(d, e, c).start()

                    @pl.when(turn)
                    def _():
                        kyz_copy(k, 1 - y).wait_recv()

                    @pl.when(dist > 0)
                    def _():
                        kz_copy(d, i).wait_recv()

                    @pl.when(dist < 3)
                    def _():
                        kz_copy(d, i).start()

                    @pl.when((dist > 0) & (w == 1))
                    def _():
                        ky_copy(d, k, y).start()

                    kd_copy(d, i, c).start()
                    mirror(num_chain(i, d, c))

                k = h - OUT2 - 2 * rounds
                on = (k >= 0) & (k < rounds)
                k = _clip(k, rounds)

                @pl.when(on)
                def _():
                    ky_copy(d, k, 1 - y).wait_recv()
                    ke_copy(d, k, c).start()
                    mirror(_ref(k, 1, d, 1 - y, c))

                j = h - DIE
                on = (j >= 0) & (j < other_chain)
                j = _clip(j, other_chain)

                @pl.when(on)
                def _():
                    @pl.when((j >= PM) & (j < PM + 2))
                    def _():
                        pkd_copy(d, lax.rem(j, 2), 1 - c).wait_recv()

                    kd_copy(d, j, 1 - c).wait_recv()
                    mirror(num_chain(j, d, 1 - c))

                m = h - OUT2 - DIE - 2 * (9 - rounds)
                on = (m >= 0) & (m < 9 - rounds)
                m = _clip(m, 9 - rounds)

                @pl.when(on)
                def _():
                    ke_copy(d, m, 1 - c).wait_recv()
                    mirror(_ref(m, 1, d, 1 - y, 1 - c))

            p = g - DRV0
            on = (p >= 0) & (p < UP)
            p = _clip(p, UP)

            @pl.when(on)
            def _():
                q = lax.rem(p, 3) * 2
                half = lax.div(p, 3)
                pmt = jnp.concatenate(
                    [pmf[half, lax.div(q, 2), pl.ds(16 * h, 16), :] for h in range(2)], axis=1
                )
                low = lax.dot_general(
                    pmt.astype(f32).T.astype(bf16), ut_ref[...], (((1,), (0,)), ((), ())), preferred_element_type=f32
                )
                cur = theta[panel(p), :]
                grad = -((cur - mu_ref[...]) * lam_ref[...] + low)
                a_ref[panel(p), :] = (grad - rep * cur).astype(bf16)

        for e in range(8):
            @pl.when(me != (e // 4) * 12 + e % 4)
            def _():
                dg_copy(e).wait_send()

        for d in range(2):
            pos = z if d else 3 - z
            for e in range(2):
                @pl.when(pos < 3)
                def _():
                    pz_copy(d, e).wait_send()

                @pl.when(pos > 0)
                def _():
                    pkz_copy(d, e).wait_send()

                pkd_copy(d, e, c).wait_send()

        @pl.when(corner)
        def _():
            pye_copy(1 - y).wait_send()
            pky_copy(y).wait_send()

        @pl.loop(0, rounds)
        def _(k):
            for d in range(2):
                y_copy(d, k).wait_send()
                ke_copy(d, k, c).wait_send()
                ky_copy(d, k, y).wait_send()

            @pl.when(corner)
            def _():
                ye_copy(k, 2 * k + 1 - y).wait_send()
                kyz_copy(k, y).wait_send()

        @pl.loop(0, chain)
        def _(i):
            for d in range(2):
                pos = z if d else 3 - z

                @pl.when(pos < 3)
                def _():
                    z_copy(d, i).wait_send()

                @pl.when(pos > 0)
                def _():
                    kz_copy(d, i).wait_send()

                kd_copy(d, i, c).wait_send()

        @pl.when(corner)
        def _():
            for e in range(16):
                @pl.when(me != e)
                def _():
                    sg_copy(e).wait_send()

    row_sums()

    @pl.loop(0, UP)
    def _(p):
        update(p)
        out_copy(p).start()

    @pl.loop(0, UP)
    def _(p):
        out_copy(p).wait()


def solution(mesh):
    def run_steps(particles, prec_diag, mean_vec, low_rank):
        width = particles.shape[1]

        def local_steps(current, prec_loc, mean_loc, fac_loc):
            n_part, nf = current.shape
            dma = pltpu.SemaphoreType.DMA
            f32, bf16 = jnp.float32, jnp.bfloat16
            vmem = pltpu.VMEM
            return pl.pallas_call(
                functools.partial(kernel, width),
                out_shape=jax.ShapeDtypeStruct((n_part, nf), f32),
                in_specs=[pl.BlockSpec(memory_space=pl.ANY)] + [pl.BlockSpec(memory_space=pltpu.VMEM)] * 3,
                out_specs=pl.BlockSpec(memory_space=pl.ANY),
                scratch_shapes=[
                    vmem((n_part, nf), f32),
                    vmem((n_part, 2 * nf), bf16),
                    vmem((n_part, nf), bf16),
                    vmem((n_part + B, n_part), bf16),
                    vmem((2, CH, B, B), f32),
                    vmem((2, 5, B, B), f32),
                    vmem((2, CH, B, B), f32),
                    vmem((2, 5, B, B), f32),
                    vmem((5, B, B), f32),
                    vmem((2, B, B), f32),
                    vmem((B, B), f32),
                    vmem((2, 2, 32, B), f32),
                    vmem((2, 2, 32, B), f32),
                    vmem((32, B), f32),
                    vmem((2, 4, 32, B), bf16),
                    vmem((16, B), f32),
                    vmem((16, 16, B), f32),
                    vmem((16, B), f32),
                    vmem((16, B), f32),
                    vmem((8, 16, B), f32),
                    vmem((16, B), f32),
                    dma((UP,)), dma((UP,)), dma((UP,)), dma((UP,)), dma, dma, dma((8,)), dma((16,)), dma((16,)), dma((8,)),
                    dma((2, CH)), dma((2, CH)), dma((2, 5)), dma((2, 5)), dma((5,)), dma((5,)),
                    dma((2, CH)), dma((2, CH)), dma((5,)), dma((5,)), dma((2, 5)), dma((2, 5)),
                    dma((2, CH)), dma((2, CH)), dma((2, 5)), dma((2, 5)),
                    dma((2, 2)), dma((2, 2)), dma, dma, dma, dma, dma((2, 2)), dma((2, 2)), dma((2, 2)), dma((2, 2)),
                ],
                compiler_params=pltpu.CompilerParams(
                    collective_id=0, has_side_effects=True, vmem_limit_bytes=56 * 1024 * 1024
                ),
                name="svgd",
            )(current, prec_loc.reshape(1, nf), mean_loc.reshape(1, nf), fac_loc.T)

        sharded = jax.shard_map(
            local_steps,
            mesh=mesh,
            in_specs=(P("ens", FEAT_AXES), P(LEAD_AXES), P(LEAD_AXES), P(LEAD_AXES, None)),
            out_specs=P("ens", FEAT_AXES),
            check_vma=False,
        )
        return sharded(particles, prec_diag, mean_vec, low_rank)

    return run_steps
```

```python
import functools

import jax
import jax.numpy as jnp
from jax import lax
from jax.experimental import pallas as pl
from jax.experimental.pallas import tpu as pltpu
from jax.sharding import PartitionSpec as P

NUM_STEPS = 3
BAND_SCALE = 4.0
STEP_SCALE = 0.4
FEAT_AXES = ("slab", "feat")
LEAD_AXES = ("ens", "slab", "feat")
MESH = pl.DeviceIdType.MESH

B = 128
ROW = 256
UP = 6
START = 2
LAG = 3
END = 3
OUT1 = 3
LAG2 = 5
OUT2 = 5
DIE = 3
YF0 = 3
FIN0 = START + 3 * LAG + END
AG0 = FIN0 + OUT1
CH = 15
PM = 6
DRV0 = AG0 + 3 * LAG2 + PM + 1 + DIE + 1
ITERS = AG0 + 3 * LAG2 + CH + OUT2 + DIE


def _ref(k, t, d, ey, c):
    f = lax.div(k, 4)
    return k * 16 + (1 - f) * (t * 8 + d * 4 + ey * 2 + c) + f * (t * 4 + d * 2 + ey)


def _block(n):
    p = lax.div(n + 126, B) + lax.div(n + 120, B) + lax.div(n + 110, B) + lax.div(n + 96, B) + lax.div(n + 78, B)
    r = n - 2 * p * p
    i = lax.div(r, 2)
    j = 2 * p + lax.rem(r, 2)
    return i, j, p, 1 - jnp.minimum(j - i, 1)


def _clip(i, n):
    return jnp.minimum(jnp.maximum(i, 0), n - 1)


def _span(i):
    return pl.ds(pl.multiple_of(i * B, B), B)


def _home(n):
    i, j, p, e = _block(n)
    return _span(i + e * (2 * UP - i)), _span(j + e * (p - j))


def kernel(width, x_hbm, lam_ref, mu_ref, ut_ref, o_hbm, theta, th, a_ref, kf, gsrc, gy, zrecv, yrecv, yend, pmb, pmrecv,
           ps, pzr, pye, pmf,
           dsrc, dgather, dsum, sacc, sgather, ssum, ld, od, thd_s, thd_r, pm_s, pm_r, dg_s, dg_r, sg_s, sg_r,
           zs, zr, ys, yr, ye_s, ye_r, kz_s, kz_r, kyz_s, kyz_r, ky_s, ky_r, kd_s, kd_r, ke_s, ke_r,
           pz_s, pz_r, pye_s, pye_r, pky_s, pky_r, pkz_s, pkz_r, pkd_s, pkd_r):
    nf = theta.shape[1]
    n_part = theta.shape[0]
    bandwidth = BAND_SCALE * width
    step_size = STEP_SCALE * width
    rep = 2.0 / bandwidth
    f32, bf16 = jnp.float32, jnp.bfloat16
    ens = lax.axis_index("ens")
    z = lax.axis_index("slab")
    feat = lax.axis_index("feat")
    y = lax.div(feat, 2)
    c = lax.rem(feat, 2)
    me = z * 4 + feat
    ypart = (ens, z, (1 - y) * 2 + c)
    dpart = (ens, z, y * 2 + 1 - c)
    dc = lax.div(z, 3)
    corner = lax.rem(z, 3) == 0
    own8 = (dc * 2 + y) * 2 + c
    rounds = 4 + c
    chain = 3 * rounds
    other_chain = 27 - chain

    def rcopy(src, dst, s, r, dev):
        return pltpu.make_async_remote_copy(src_ref=src, dst_ref=dst, send_sem=s, recv_sem=r, device_id=dev, device_id_type=MESH)

    def zdev(dz):
        return (ens, z + dz, feat)

    def place(i, cc):
        zf = 8 + 2 * cc
        w = lax.div(i, zf)
        return w, (1 - w) * lax.div(i, 2) + w * (i - zf), lax.rem(i, 2)

    def num_chain(i, d, cc):
        w, k, e = place(i, cc)
        return _ref(k, w, d, (1 - w) * e + w * y, cc)

    def panel(p):
        return pl.ds(pl.multiple_of(p * ROW, ROW), ROW)

    def load_copy(p):
        return pltpu.make_async_copy(x_hbm.at[panel(p)], theta.at[panel(p)], ld.at[p])

    def out_copy(p):
        return pltpu.make_async_copy(theta.at[panel(p)], o_hbm.at[panel(p)], od.at[p])

    def th_copy(p):
        return rcopy(th.at[panel(p), pl.ds(0, nf)], th.at[panel(p), pl.ds(nf, nf)], thd_s.at[p], thd_r.at[p], dpart)

    def pm_copy():
        return rcopy(pmb.at[1 - c], pmrecv, pm_s, pm_r, dpart)

    def dg_copy(e):
        return rcopy(dsrc, dgather.at[me], dg_s.at[e], dg_r.at[me], (ens, (e // 4) * 3, e % 4))

    def dg_local():
        return pltpu.make_async_copy(dsrc, dgather.at[me], dg_r.at[me])

    def sg_copy(e):
        return rcopy(sacc, sgather.at[own8], sg_s.at[e], sg_r.at[own8], (ens, e // 4, e % 4))

    def sg_local():
        return pltpu.make_async_copy(sacc, sgather.at[own8], sg_r.at[own8])

    def z_copy(d, i):
        return rcopy(gsrc.at[d, i], zrecv.at[d, i], zs.at[d, i], zr.at[d, i], zdev(2 * d - 1))

    def y_copy(d, k):
        return rcopy(gy.at[d, k], yrecv.at[d, k], ys.at[d, k], yr.at[d, k], ypart)

    def ye_copy(k, i):
        return rcopy(gsrc.at[dc, i], yend.at[k], ye_s.at[k], ye_r.at[k], ypart)

    def kf_copy(n, s, r, dev):
        rows, cols = _home(n)
        return rcopy(kf.at[rows, cols], kf.at[rows, cols], s, r, dev)

    def kz_copy(d, i):
        return kf_copy(num_chain(i, d, c), kz_s.at[d, i], kz_r.at[d, i], zdev(1 - 2 * d))

    def kyz_copy(k, ey):
        return kf_copy(_ref(k, 0, dc, ey, c), kyz_s.at[k], kyz_r.at[k], ypart)

    def ky_copy(d, k, yy):
        return kf_copy(_ref(k, 1, d, yy, c), ky_s.at[d, k], ky_r.at[d, k], ypart)

    def kd_copy(d, i, cc):
        return kf_copy(num_chain(i, d, cc), kd_s.at[d, i], kd_r.at[d, i], dpart)

    def ke_copy(d, k, cc):
        return kf_copy(_ref(k, 1, d, 1 - y, cc), ke_s.at[d, k], ke_r.at[d, k], dpart)

    def pz_copy(d, e):
        return rcopy(ps.at[d, e], pzr.at[d, e], pz_s.at[d, e], pz_r.at[d, e], zdev(2 * d - 1))

    def pye_copy(e):
        return rcopy(ps.at[dc, e], pye, pye_s, pye_r, ypart)

    def pf_copy(d, e, cc, s, r, dev):
        return rcopy(pmf.at[cc, 2 * d + e], pmf.at[cc, 2 * d + e], s, r, dev)

    def pky_copy(e):
        return pf_copy(dc, e, c, pky_s, pky_r, ypart)

    def pkz_copy(d, e):
        return pf_copy(d, e, c, pkz_s.at[d, e], pkz_r.at[d, e], zdev(1 - 2 * d))

    def pkd_copy(d, e, cc):
        return pf_copy(d, e, cc, pkd_s.at[d, e], pkd_r.at[d, e], dpart)

    def low_tri():
        return lax.broadcasted_iota(jnp.int32, (B, B), 0) - lax.broadcasted_iota(jnp.int32, (B, B), 1)

    def unpack(kk):
        kt = kk.T
        tri = low_tri()
        return jnp.where(tri >= 0, kk, kt), jnp.where(tri < 0, kk, jnp.where(tri == 0, 1.0, kt))

    def mirror(n):
        i, j, p, e = _block(n)

        @pl.when(e == 0)
        def _():
            kf[_span(j), _span(i)] = kf[_span(i), _span(j)].astype(f32).T.astype(bf16)

        @pl.when(e == 1)
        def _():
            first, second = unpack(kf[pl.ds(2 * UP * B, B), _span(p)].astype(f32))
            kf[_span(2 * p), _span(2 * p)] = first.astype(bf16)
            kf[_span(2 * p + 1), _span(2 * p + 1)] = second.astype(bf16)

    def dot_t(i, j):
        return lax.dot_general(th[_span(i), :], th[_span(j), :], (((1,), (1,)), ((), ())), preferred_element_type=f32)

    def gram(dst, n):
        i, j, p, e = _block(n)
        dst[...] = dot_t(i, j)

        @pl.when(e == 1)
        def _():
            dst[...] = jnp.where(low_tri() >= 0, dst[...], dot_t(2 * p + 1, 2 * p + 1))

    def post(p):
        new = theta[panel(p), :]
        tb = new.astype(bf16)
        th[panel(p), pl.ds(0, nf)] = tb
        xb = (new - mu_ref[...]).astype(bf16)
        pm = lax.dot_general(ut_ref[...], xb, (((1,), (1,)), ((), ())), preferred_element_type=f32)
        th_copy(p).start()
        half = lax.div(p, 3)
        for h in range(2):
            q = lax.rem(p, 3) * 2 + h
            pmb[half, pl.ds(pl.multiple_of(q * 16, 16), 16), :] = pm[:, h * B:(h + 1) * B]
            t = tb[h * B:(h + 1) * B, :].astype(f32)
            sq = t * t
            tot = sq[:, 0:B]
            for m in range(1, nf // B):
                tot = tot + sq[:, m * B:(m + 1) * B]
            dsrc[pl.ds(p * 2 + h, 1), :] = jnp.sum(tot.T, axis=0, keepdims=True)

    def row_sums():
        tot = jnp.zeros((16, B), f32)
        for e in range(8):
            pltpu.make_async_copy(sacc, sgather.at[e], sg_r.at[e]).wait()
            tot = tot + sgather[e]
        ssum[...] = tot

    def update(p):
        acc = jnp.dot(kf[panel(p), :], a_ref[...], preferred_element_type=f32)
        cur = theta[panel(p), :]
        col = jnp.concatenate(
            [jnp.broadcast_to(ssum[pl.ds(p * 2 + h, 1), :], (B, B)).T[:, 0:1] for h in range(2)], axis=0
        )
        phi = (acc + (rep * col) * cur) * (1.0 / n_part)
        theta[panel(p), :] = cur + step_size * phi

    barrier = pltpu.get_barrier_semaphore()
    for o in range(1, 16):
        e = lax.rem(me + o, 16)
        pl.semaphore_signal(barrier, inc=1, device_id=(ens, lax.div(e, 4), lax.rem(e, 4)), device_id_type=MESH)
    for p in range(UP):
        load_copy(p).start()
    pmb[...] = jnp.zeros_like(pmb)
    dsrc[...] = jnp.zeros_like(dsrc)
    pl.semaphore_wait(barrier, 15)

    @pl.loop(0, NUM_STEPS)
    def _(step):
        @pl.when(step > 0)
        def _():
            row_sums()

        sacc[...] = jnp.zeros_like(sacc)

        @pl.loop(0, ITERS)
        def _(g):
            gp = jnp.minimum(g, UP - 1)

            @pl.when(g < UP)
            def _():
                @pl.when(step == 0)
                def _():
                    load_copy(gp).wait()

                @pl.when(step > 0)
                def _():
                    update(gp)

                post(gp)

            @pl.when(g == UP - 1)
            def _():
                for e in range(8):
                    mine = me == (e // 4) * 12 + e % 4

                    @pl.when(mine)
                    def _():
                        dg_local().start()

                    @pl.when(jnp.logical_not(mine))
                    def _():
                        dg_copy(e).start()

                pm_copy().start()

            @pl.when((g >= 1) & (g <= UP))
            def _():
                th_copy(_clip(g - 1, UP)).wait()

            @pl.when(g == START + PM)
            def _():
                pm_copy().wait()

            v = g - YF0
            v_on = (v >= 0) & (v < 2 * rounds)
            v = _clip(v, 2 * rounds)

            @pl.when(v_on)
            def _():
                d, k = lax.rem(v, 2), lax.div(v, 2)
                gram(gy.at[d, k], _ref(k, 1, d, 1 - y, c))

            for d in range(2):
                pos = z if d else 3 - z
                i = g - START - LAG * pos
                on = (i >= 0) & (i < chain)
                i = _clip(i, chain)

                @pl.when(on)
                def _():
                    w, k, e = place(i, c)
                    gram(gsrc.at[d, i], _ref(k, w, d, (1 - w) * e + w * y, c))

                    @pl.when(w == 1)
                    def _():
                        y_copy(d, k).wait_recv()
                        gsrc[d, i] = gsrc[d, i] + yrecv[d, k]

                    @pl.when(pos > 0)
                    def _():
                        z_copy(d, i).wait_recv()
                        gsrc[d, i] = gsrc[d, i] + zrecv[d, i]

                    @pl.when((i >= PM) & (i < PM + 2))
                    def _():
                        rows = pl.ds(pl.multiple_of((2 * d + e) * 32, 32), 32)
                        ps[d, e] = pmb[c, rows, :] + pmrecv[rows, :]

                        @pl.when(pos > 0)
                        def _():
                            pz_copy(d, e).wait_recv()
                            ps[d, e] = ps[d, e] + pzr[d, e]

            @pl.when(v_on)
            def _():
                y_copy(lax.rem(v, 2), lax.div(v, 2)).start()

            for d in range(2):
                pos = z if d else 3 - z
                i = g - START - LAG * pos
                on = (i >= 0) & (i < chain)
                i = _clip(i, chain)

                @pl.when(on)
                def _():
                    w, k, e = place(i, c)
                    cross = (pos == 3) & (w == 0) & (e != y)
                    rides = (i >= PM) & (i < PM + 2)

                    @pl.when((pos < 3) & rides)
                    def _():
                        pz_copy(d, e).start()

                    @pl.when(pos < 3)
                    def _():
                        z_copy(d, i).start()

                    @pl.when(cross & rides)
                    def _():
                        pye_copy(e).start()

                    @pl.when(cross)
                    def _():
                        ye_copy(k, i).start()

            i = g - FIN0
            on = corner & (i >= 0) & (i < chain)
            i = _clip(i, chain)

            @pl.when(on)
            def _():
                @pl.when(i == 0)
                def _():
                    tot = jnp.zeros((16, B), f32)
                    for e in range(16):
                        pltpu.make_async_copy(dsrc, dgather.at[e], dg_r.at[e]).wait()
                        tot = tot + dgather[e]
                    dsum[...] = tot

                w, k, e = place(i, c)

                @pl.when((w == 1) | (e == y))
                def _():
                    @pl.when(w == 0)
                    def _():
                        ye_copy(k, i).wait_recv()
                        gsrc[dc, i] = gsrc[dc, i] + yend[k]

                    n = num_chain(i, dc, c)
                    bi, bj, bp, be = _block(n)

                    def kern(gi, gj):
                        sq = jnp.maximum(gi + gj - 2.0 * gsrc[dc, i], 0.0)
                        return jnp.exp(sq * (-1.0 / bandwidth))

                    def add_sums(q, blk):
                        sacc[pl.ds(q, 1), :] = sacc[pl.ds(q, 1), :] + jnp.sum(blk, axis=0, keepdims=True)

                    @pl.when(be == 0)
                    def _():
                        kk = kern(jnp.broadcast_to(dsum[pl.ds(bi, 1), :], (B, B)).T, dsum[pl.ds(bj, 1), :])
                        kf[_span(bi), _span(bj)] = kk.astype(bf16)
                        add_sums(bj, kk)
                        add_sums(bi, kk.T)

                    @pl.when(be == 1)
                    def _():
                        tri = low_tri() >= 0
                        ga = jnp.broadcast_to(dsum[pl.ds(2 * bp, 1), :], (B, B))
                        gb = jnp.broadcast_to(dsum[pl.ds(2 * bp + 1, 1), :], (B, B))
                        kk = kern(jnp.where(tri, ga.T, gb.T), jnp.where(tri, ga, gb))
                        kk = jnp.where(low_tri() == 0, 1.0, kk)
                        kf[pl.ds(2 * UP * B, B), _span(bp)] = kk.astype(bf16)
                        first, second = unpack(kk)
                        add_sums(2 * bp, first)
                        add_sums(2 * bp + 1, second)

                    @pl.when((i >= PM) & (i < PM + 2))
                    def _():
                        pye_copy(e).wait_recv()
                        pmf[c, 2 * dc + e] = (ps[dc, e] + pye[...]).astype(bf16)
                        pky_copy(e).start()

                    @pl.when(w == 0)
                    def _():
                        kyz_copy(k, y).start()

                    @pl.when(w == 1)
                    def _():
                        ky_copy(dc, k, y).start()

                @pl.when(i == chain - 1)
                def _():
                    for o in range(16):
                        @pl.when(me == o)
                        def _():
                            sg_local().start()

                        @pl.when(me != o)
                        def _():
                            sg_copy(o).start()

            for d in range(2):
                dist = 3 - z if d else z
                h = g - AG0 - LAG2 * dist
                on = (h >= 0) & (h < chain)
                i = _clip(h, chain)

                @pl.when(on)
                def _():
                    w, k, e = place(i, c)
                    turn = (dist == 0) & (w == 0) & (e != y)

                    @pl.when((i >= PM) & (i < PM + 2))
                    def _():
                        @pl.when(turn)
                        def _():
                            pky_copy(1 - y).wait_recv()

                        @pl.when(dist > 0)
                        def _():
                            pkz_copy(d, e).wait_recv()

                        @pl.when(dist < 3)
                        def _():
                            pkz_copy(d, e).start()

                        pkd_copy(d, e, c).start()

                    @pl.when(turn)
                    def _():
                        kyz_copy(k, 1 - y).wait_recv()

                    @pl.when(dist > 0)
                    def _():
                        kz_copy(d, i).wait_recv()

                    @pl.when(dist < 3)
                    def _():
                        kz_copy(d, i).start()

                    @pl.when((dist > 0) & (w == 1))
                    def _():
                        ky_copy(d, k, y).start()

                    kd_copy(d, i, c).start()
                    mirror(num_chain(i, d, c))

                k = h - OUT2 - 2 * rounds
                on = (k >= 0) & (k < rounds)
                k = _clip(k, rounds)

                @pl.when(on)
                def _():
                    ky_copy(d, k, 1 - y).wait_recv()
                    ke_copy(d, k, c).start()
                    mirror(_ref(k, 1, d, 1 - y, c))

                j = h - DIE
                on = (j >= 0) & (j < other_chain)
                j = _clip(j, other_chain)

                @pl.when(on)
                def _():
                    @pl.when((j >= PM) & (j < PM + 2))
                    def _():
                        pkd_copy(d, lax.rem(j, 2), 1 - c).wait_recv()

                    kd_copy(d, j, 1 - c).wait_recv()
                    mirror(num_chain(j, d, 1 - c))

                m = h - OUT2 - DIE - 2 * (9 - rounds)
                on = (m >= 0) & (m < 9 - rounds)
                m = _clip(m, 9 - rounds)

                @pl.when(on)
                def _():
                    ke_copy(d, m, 1 - c).wait_recv()
                    mirror(_ref(m, 1, d, 1 - y, 1 - c))

            p = g - DRV0
            on = (p >= 0) & (p < UP)
            p = _clip(p, UP)

            @pl.when(on)
            def _():
                q = lax.rem(p, 3) * 2
                half = lax.div(p, 3)
                pmt = jnp.concatenate(
                    [pmf[half, lax.div(q, 2), pl.ds(16 * h, 16), :] for h in range(2)], axis=1
                )
                low = lax.dot_general(
                    pmt.astype(f32).T.astype(bf16), ut_ref[...], (((1,), (0,)), ((), ())), preferred_element_type=f32
                )
                cur = theta[panel(p), :]
                grad = -((cur - mu_ref[...]) * lam_ref[...] + low)
                a_ref[panel(p), :] = (grad - rep * cur).astype(bf16)

        for e in range(8):
            @pl.when(me != (e // 4) * 12 + e % 4)
            def _():
                dg_copy(e).wait_send()

        for d in range(2):
            pos = z if d else 3 - z
            for e in range(2):
                @pl.when(pos < 3)
                def _():
                    pz_copy(d, e).wait_send()

                @pl.when(pos > 0)
                def _():
                    pkz_copy(d, e).wait_send()

                pkd_copy(d, e, c).wait_send()

        @pl.when(corner)
        def _():
            pye_copy(1 - y).wait_send()
            pky_copy(y).wait_send()

        @pl.loop(0, rounds)
        def _(k):
            for d in range(2):
                y_copy(d, k).wait_send()
                ke_copy(d, k, c).wait_send()
                ky_copy(d, k, y).wait_send()

            @pl.when(corner)
            def _():
                ye_copy(k, 2 * k + 1 - y).wait_send()
                kyz_copy(k, y).wait_send()

        @pl.loop(0, chain)
        def _(i):
            for d in range(2):
                pos = z if d else 3 - z

                @pl.when(pos < 3)
                def _():
                    z_copy(d, i).wait_send()

                @pl.when(pos > 0)
                def _():
                    kz_copy(d, i).wait_send()

                kd_copy(d, i, c).wait_send()

        @pl.when(corner)
        def _():
            for e in range(16):
                @pl.when(me != e)
                def _():
                    sg_copy(e).wait_send()

    row_sums()

    @pl.loop(0, UP)
    def _(p):
        update(p)
        out_copy(p).start()

    @pl.loop(0, UP)
    def _(p):
        out_copy(p).wait()


def solution(mesh):
    def run_steps(particles, prec_diag, mean_vec, low_rank):
        width = particles.shape[1]

        def local_steps(current, prec_loc, mean_loc, fac_loc):
            n_part, nf = current.shape
            dma = pltpu.SemaphoreType.DMA
            f32, bf16 = jnp.float32, jnp.bfloat16
            vmem = pltpu.VMEM
            return pl.pallas_call(
                functools.partial(kernel, width),
                out_shape=jax.ShapeDtypeStruct((n_part, nf), f32),
                in_specs=[pl.BlockSpec(memory_space=pl.ANY)] + [pl.BlockSpec(memory_space=pltpu.VMEM)] * 3,
                out_specs=pl.BlockSpec(memory_space=pl.ANY),
                scratch_shapes=[
                    vmem((n_part, nf), f32),
                    vmem((n_part, 2 * nf), bf16),
                    vmem((n_part, nf), bf16),
                    vmem((n_part + B, n_part), bf16),
                    vmem((2, CH, B, B), f32),
                    vmem((2, 5, B, B), f32),
                    vmem((2, CH, B, B), f32),
                    vmem((2, 5, B, B), f32),
                    vmem((5, B, B), f32),
                    vmem((2, B, B), f32),
                    vmem((B, B), f32),
                    vmem((2, 2, 32, B), f32),
                    vmem((2, 2, 32, B), f32),
                    vmem((32, B), f32),
                    vmem((2, 4, 32, B), bf16),
                    vmem((16, B), f32),
                    vmem((16, 16, B), f32),
                    vmem((16, B), f32),
                    vmem((16, B), f32),
                    vmem((8, 16, B), f32),
                    vmem((16, B), f32),
                    dma((UP,)), dma((UP,)), dma((UP,)), dma((UP,)), dma, dma, dma((8,)), dma((16,)), dma((16,)), dma((8,)),
                    dma((2, CH)), dma((2, CH)), dma((2, 5)), dma((2, 5)), dma((5,)), dma((5,)),
                    dma((2, CH)), dma((2, CH)), dma((5,)), dma((5,)), dma((2, 5)), dma((2, 5)),
                    dma((2, CH)), dma((2, CH)), dma((2, 5)), dma((2, 5)),
                    dma((2, 2)), dma((2, 2)), dma, dma, dma, dma, dma((2, 2)), dma((2, 2)), dma((2, 2)), dma((2, 2)),
                ],
                compiler_params=pltpu.CompilerParams(
                    collective_id=0, has_side_effects=True, vmem_limit_bytes=56 * 1024 * 1024
                ),
                name="svgd",
            )(current, prec_loc.reshape(1, nf), mean_loc.reshape(1, nf), fac_loc.T)

        sharded = jax.shard_map(
            local_steps,
            mesh=mesh,
            in_specs=(P("ens", FEAT_AXES), P(LEAD_AXES), P(LEAD_AXES), P(LEAD_AXES, None)),
            out_specs=P("ens", FEAT_AXES),
            check_vma=False,
        )
        return sharded(particles, prec_diag, mean_vec, low_rank)

    return run_steps
```

```python
import functools

import jax
import jax.numpy as jnp
from jax import lax
from jax.experimental import pallas as pl
from jax.experimental.pallas import tpu as pltpu
from jax.sharding import PartitionSpec as P

NUM_STEPS = 3
BAND_SCALE = 4.0
STEP_SCALE = 0.4
FEAT_AXES = ("slab", "feat")
LEAD_AXES = ("ens", "slab", "feat")
MESH = pl.DeviceIdType.MESH

B = 128
ROW = 256
UP = 6
START = 2
LAG = 3
END = 3
OUT1 = 3
LAG2 = 5
OUT2 = 5
DIE = 3
YF0 = 3
FIN0 = START + 3 * LAG + END
AG0 = FIN0 + OUT1
CH = 15
PM = 6
DRV0 = AG0 + 3 * LAG2 + PM + 1 + DIE + 1
ITERS = AG0 + 3 * LAG2 + CH + OUT2 + DIE


def _ref(k, t, d, ey, c):
    f = lax.div(k, 4)
    return k * 16 + (1 - f) * (t * 8 + d * 4 + ey * 2 + c) + f * (t * 4 + d * 2 + ey)


def _block(n):
    p = lax.div(n + 126, B) + lax.div(n + 120, B) + lax.div(n + 110, B) + lax.div(n + 96, B) + lax.div(n + 78, B)
    r = n - 2 * p * p
    i = lax.div(r, 2)
    j = 2 * p + lax.rem(r, 2)
    return i, j, p, 1 - jnp.minimum(j - i, 1)


def _clip(i, n):
    return jnp.minimum(jnp.maximum(i, 0), n - 1)


def _span(i):
    return pl.ds(pl.multiple_of(i * B, B), B)


def _home(n):
    i, j, p, e = _block(n)
    return _span(i + e * (2 * UP - i)), _span(j + e * (p - j))


def kernel(width, x_hbm, lam_ref, mu_ref, ut_ref, o_hbm, theta, th, a_ref, kf, gsrc, gy, zrecv, yrecv, yend, pmb, pmrecv,
           ps, pzr, pye, pmf,
           dsrc, dgather, dsum, sacc, sgather, ssum, ld, od, thd_s, thd_r, pm_s, pm_r, dg_s, dg_r, sg_s, sg_r,
           zs, zr, ys, yr, ye_s, ye_r, kz_s, kz_r, kyz_s, kyz_r, ky_s, ky_r, kd_s, kd_r, ke_s, ke_r,
           pz_s, pz_r, pye_s, pye_r, pky_s, pky_r, pkz_s, pkz_r, pkd_s, pkd_r):
    nf = theta.shape[1]
    n_part = theta.shape[0]
    bandwidth = BAND_SCALE * width
    step_size = STEP_SCALE * width
    rep = 2.0 / bandwidth
    f32, bf16 = jnp.float32, jnp.bfloat16
    ens = lax.axis_index("ens")
    z = lax.axis_index("slab")
    feat = lax.axis_index("feat")
    y = lax.div(feat, 2)
    c = lax.rem(feat, 2)
    me = z * 4 + feat
    ypart = (ens, z, (1 - y) * 2 + c)
    dpart = (ens, z, y * 2 + 1 - c)
    dc = lax.div(z, 3)
    corner = lax.rem(z, 3) == 0
    own8 = (dc * 2 + y) * 2 + c
    rounds = 5 - c
    chain = 3 * rounds
    other_chain = 27 - chain

    def rcopy(src, dst, s, r, dev):
        return pltpu.make_async_remote_copy(src_ref=src, dst_ref=dst, send_sem=s, recv_sem=r, device_id=dev, device_id_type=MESH)

    def zdev(dz):
        return (ens, z + dz, feat)

    def place(i, cc):
        zf = 10 - 2 * cc
        w = lax.div(i, zf)
        return w, (1 - w) * lax.div(i, 2) + w * (i - zf), lax.rem(i, 2)

    def num_chain(i, d, cc):
        w, k, e = place(i, cc)
        return _ref(k, w, d, (1 - w) * e + w * y, cc)

    def panel(p):
        return pl.ds(pl.multiple_of(p * ROW, ROW), ROW)

    def load_copy(p):
        return pltpu.make_async_copy(x_hbm.at[panel(p)], theta.at[panel(p)], ld.at[p])

    def out_copy(p):
        return pltpu.make_async_copy(theta.at[panel(p)], o_hbm.at[panel(p)], od.at[p])

    def th_copy(p):
        return rcopy(th.at[panel(p), pl.ds(0, nf)], th.at[panel(p), pl.ds(nf, nf)], thd_s.at[p], thd_r.at[p], dpart)

    def pm_copy():
        return rcopy(pmb.at[1 - c], pmrecv, pm_s, pm_r, dpart)

    def dg_copy(e):
        return rcopy(dsrc, dgather.at[me], dg_s.at[e], dg_r.at[me], (ens, (e // 4) * 3, e % 4))

    def dg_local():
        return pltpu.make_async_copy(dsrc, dgather.at[me], dg_r.at[me])

    def sg_copy(e):
        return rcopy(sacc, sgather.at[own8], sg_s.at[e], sg_r.at[own8], (ens, e // 4, e % 4))

    def sg_local():
        return pltpu.make_async_copy(sacc, sgather.at[own8], sg_r.at[own8])

    def z_copy(d, i):
        return rcopy(gsrc.at[d, i], zrecv.at[d, i], zs.at[d, i], zr.at[d, i], zdev(2 * d - 1))

    def y_copy(d, k):
        return rcopy(gy.at[d, k], yrecv.at[d, k], ys.at[d, k], yr.at[d, k], ypart)

    def ye_copy(k, i):
        return rcopy(gsrc.at[dc, i], yend.at[k], ye_s.at[k], ye_r.at[k], ypart)

    def kf_copy(n, s, r, dev):
        rows, cols = _home(n)
        return rcopy(kf.at[rows, cols], kf.at[rows, cols], s, r, dev)

    def kz_copy(d, i):
        return kf_copy(num_chain(i, d, c), kz_s.at[d, i], kz_r.at[d, i], zdev(1 - 2 * d))

    def kyz_copy(k, ey):
        return kf_copy(_ref(k, 0, dc, ey, c), kyz_s.at[k], kyz_r.at[k], ypart)

    def ky_copy(d, k, yy):
        return kf_copy(_ref(k, 1, d, yy, c), ky_s.at[d, k], ky_r.at[d, k], ypart)

    def kd_copy(d, i, cc):
        return kf_copy(num_chain(i, d, cc), kd_s.at[d, i], kd_r.at[d, i], dpart)

    def ke_copy(d, k, cc):
        return kf_copy(_ref(k, 1, d, 1 - y, cc), ke_s.at[d, k], ke_r.at[d, k], dpart)

    def pz_copy(d, e):
        return rcopy(ps.at[d, e], pzr.at[d, e], pz_s.at[d, e], pz_r.at[d, e], zdev(2 * d - 1))

    def pye_copy(e):
        return rcopy(ps.at[dc, e], pye, pye_s, pye_r, ypart)

    def pf_copy(d, e, cc, s, r, dev):
        return rcopy(pmf.at[cc, 2 * d + e], pmf.at[cc, 2 * d + e], s, r, dev)

    def pky_copy(e):
        return pf_copy(dc, e, c, pky_s, pky_r, ypart)

    def pkz_copy(d, e):
        return pf_copy(d, e, c, pkz_s.at[d, e], pkz_r.at[d, e], zdev(1 - 2 * d))

    def pkd_copy(d, e, cc):
        return pf_copy(d, e, cc, pkd_s.at[d, e], pkd_r.at[d, e], dpart)

    def low_tri():
        return lax.broadcasted_iota(jnp.int32, (B, B), 0) - lax.broadcasted_iota(jnp.int32, (B, B), 1)

    def unpack(kk):
        kt = kk.T
        tri = low_tri()
        return jnp.where(tri >= 0, kk, kt), jnp.where(tri < 0, kk, jnp.where(tri == 0, 1.0, kt))

    def mirror(n):
        i, j, p, e = _block(n)

        @pl.when(e == 0)
        def _():
            kf[_span(j), _span(i)] = kf[_span(i), _span(j)].astype(f32).T.astype(bf16)

        @pl.when(e == 1)
        def _():
            first, second = unpack(kf[pl.ds(2 * UP * B, B), _span(p)].astype(f32))
            kf[_span(2 * p), _span(2 * p)] = first.astype(bf16)
            kf[_span(2 * p + 1), _span(2 * p + 1)] = second.astype(bf16)

    def dot_t(i, j):
        return lax.dot_general(th[_span(i), :], th[_span(j), :], (((1,), (1,)), ((), ())), preferred_element_type=f32)

    def gram(dst, n):
        i, j, p, e = _block(n)
        dst[...] = dot_t(i, j)

        @pl.when(e == 1)
        def _():
            dst[...] = jnp.where(low_tri() >= 0, dst[...], dot_t(2 * p + 1, 2 * p + 1))

    def post(p):
        new = theta[panel(p), :]
        tb = new.astype(bf16)
        th[panel(p), pl.ds(0, nf)] = tb
        xb = (new - mu_ref[...]).astype(bf16)
        pm = lax.dot_general(ut_ref[...], xb, (((1,), (1,)), ((), ())), preferred_element_type=f32)
        th_copy(p).start()
        half = lax.div(p, 3)
        for h in range(2):
            q = lax.rem(p, 3) * 2 + h
            pmb[half, pl.ds(pl.multiple_of(q * 16, 16), 16), :] = pm[:, h * B:(h + 1) * B]
            t = tb[h * B:(h + 1) * B, :].astype(f32)
            sq = t * t
            tot = sq[:, 0:B]
            for m in range(1, nf // B):
                tot = tot + sq[:, m * B:(m + 1) * B]
            dsrc[pl.ds(p * 2 + h, 1), :] = jnp.sum(tot.T, axis=0, keepdims=True)

    def row_sums():
        tot = jnp.zeros((16, B), f32)
        for e in range(8):
            pltpu.make_async_copy(sacc, sgather.at[e], sg_r.at[e]).wait()
            tot = tot + sgather[e]
        ssum[...] = tot

    def update(p):
        acc = jnp.dot(kf[panel(p), :], a_ref[...], preferred_element_type=f32)
        cur = theta[panel(p), :]
        col = jnp.concatenate(
            [jnp.broadcast_to(ssum[pl.ds(p * 2 + h, 1), :], (B, B)).T[:, 0:1] for h in range(2)], axis=0
        )
        phi = (acc + (rep * col) * cur) * (1.0 / n_part)
        theta[panel(p), :] = cur + step_size * phi

    barrier = pltpu.get_barrier_semaphore()
    for o in range(1, 16):
        e = lax.rem(me + o, 16)
        pl.semaphore_signal(barrier, inc=1, device_id=(ens, lax.div(e, 4), lax.rem(e, 4)), device_id_type=MESH)
    for p in range(UP):
        load_copy(p).start()
    pmb[...] = jnp.zeros_like(pmb)
    dsrc[...] = jnp.zeros_like(dsrc)
    pl.semaphore_wait(barrier, 15)

    @pl.loop(0, NUM_STEPS)
    def _(step):
        @pl.when(step > 0)
        def _():
            row_sums()

        sacc[...] = jnp.zeros_like(sacc)

        @pl.loop(0, ITERS)
        def _(g):
            gp = jnp.minimum(g, UP - 1)

            @pl.when(g < UP)
            def _():
                @pl.when(step == 0)
                def _():
                    load_copy(gp).wait()

                @pl.when(step > 0)
                def _():
                    update(gp)

                post(gp)

            @pl.when(g == UP - 1)
            def _():
                for e in range(8):
                    mine = me == (e // 4) * 12 + e % 4

                    @pl.when(mine)
                    def _():
                        dg_local().start()

                    @pl.when(jnp.logical_not(mine))
                    def _():
                        dg_copy(e).start()

                pm_copy().start()

            @pl.when((g >= 1) & (g <= UP))
            def _():
                th_copy(_clip(g - 1, UP)).wait()

            @pl.when(g == START + PM)
            def _():
                pm_copy().wait()

            v = g - YF0
            v_on = (v >= 0) & (v < 2 * rounds)
            v = _clip(v, 2 * rounds)

            @pl.when(v_on)
            def _():
                d, k = lax.rem(v, 2), lax.div(v, 2)
                gram(gy.at[d, k], _ref(k, 1, d, 1 - y, c))

            for d in range(2):
                pos = z if d else 3 - z
                i = g - START - LAG * pos
                on = (i >= 0) & (i < chain)
                i = _clip(i, chain)

                @pl.when(on)
                def _():
                    w, k, e = place(i, c)
                    gram(gsrc.at[d, i], _ref(k, w, d, (1 - w) * e + w * y, c))

                    @pl.when(w == 1)
                    def _():
                        y_copy(d, k).wait_recv()
                        gsrc[d, i] = gsrc[d, i] + yrecv[d, k]

                    @pl.when(pos > 0)
                    def _():
                        z_copy(d, i).wait_recv()
                        gsrc[d, i] = gsrc[d, i] + zrecv[d, i]

                    @pl.when((i >= PM) & (i < PM + 2))
                    def _():
                        rows = pl.ds(pl.multiple_of((2 * d + e) * 32, 32), 32)
                        ps[d, e] = pmb[c, rows, :] + pmrecv[rows, :]

                        @pl.when(pos > 0)
                        def _():
                            pz_copy(d, e).wait_recv()
                            ps[d, e] = ps[d, e] + pzr[d, e]

            @pl.when(v_on)
            def _():
                y_copy(lax.rem(v, 2), lax.div(v, 2)).start()

            for d in range(2):
                pos = z if d else 3 - z
                i = g - START - LAG * pos
                on = (i >= 0) & (i < chain)
                i = _clip(i, chain)

                @pl.when(on)
                def _():
                    w, k, e = place(i, c)
                    cross = (pos == 3) & (w == 0) & (e != y)
                    rides = (i >= PM) & (i < PM + 2)

                    @pl.when((pos < 3) & rides)
                    def _():
                        pz_copy(d, e).start()

                    @pl.when(pos < 3)
                    def _():
                        z_copy(d, i).start()

                    @pl.when(cross & rides)
                    def _():
                        pye_copy(e).start()

                    @pl.when(cross)
                    def _():
                        ye_copy(k, i).start()

            i = g - FIN0
            on = corner & (i >= 0) & (i < chain)
            i = _clip(i, chain)

            @pl.when(on)
            def _():
                @pl.when(i == 0)
                def _():
                    tot = jnp.zeros((16, B), f32)
                    for e in range(16):
                        pltpu.make_async_copy(dsrc, dgather.at[e], dg_r.at[e]).wait()
                        tot = tot + dgather[e]
                    dsum[...] = tot

                w, k, e = place(i, c)

                @pl.when((w == 1) | (e == y))
                def _():
                    @pl.when(w == 0)
                    def _():
                        ye_copy(k, i).wait_recv()
                        gsrc[dc, i] = gsrc[dc, i] + yend[k]

                    n = num_chain(i, dc, c)
                    bi, bj, bp, be = _block(n)

                    def kern(gi, gj):
                        sq = jnp.maximum(gi + gj - 2.0 * gsrc[dc, i], 0.0)
                        return jnp.exp(sq * (-1.0 / bandwidth))

                    def add_sums(q, blk):
                        sacc[pl.ds(q, 1), :] = sacc[pl.ds(q, 1), :] + jnp.sum(blk, axis=0, keepdims=True)

                    @pl.when(be == 0)
                    def _():
                        kk = kern(jnp.broadcast_to(dsum[pl.ds(bi, 1), :], (B, B)).T, dsum[pl.ds(bj, 1), :])
                        kf[_span(bi), _span(bj)] = kk.astype(bf16)
                        add_sums(bj, kk)
                        add_sums(bi, kk.T)

                    @pl.when(be == 1)
                    def _():
                        tri = low_tri() >= 0
                        ga = jnp.broadcast_to(dsum[pl.ds(2 * bp, 1), :], (B, B))
                        gb = jnp.broadcast_to(dsum[pl.ds(2 * bp + 1, 1), :], (B, B))
                        kk = kern(jnp.where(tri, ga.T, gb.T), jnp.where(tri, ga, gb))
                        kk = jnp.where(low_tri() == 0, 1.0, kk)
                        kf[pl.ds(2 * UP * B, B), _span(bp)] = kk.astype(bf16)
                        first, second = unpack(kk)
                        add_sums(2 * bp, first)
                        add_sums(2 * bp + 1, second)

                    @pl.when((i >= PM) & (i < PM + 2))
                    def _():
                        pye_copy(e).wait_recv()
                        pmf[c, 2 * dc + e] = (ps[dc, e] + pye[...]).astype(bf16)
                        pky_copy(e).start()

                    @pl.when(w == 0)
                    def _():
                        kyz_copy(k, y).start()

                    @pl.when(w == 1)
                    def _():
                        ky_copy(dc, k, y).start()

                @pl.when(i == chain - 1)
                def _():
                    for o in range(16):
                        @pl.when(me == o)
                        def _():
                            sg_local().start()

                        @pl.when(me != o)
                        def _():
                            sg_copy(o).start()

            for d in range(2):
                dist = 3 - z if d else z
                h = g - AG0 - LAG2 * dist
                on = (h >= 0) & (h < chain)
                i = _clip(h, chain)

                @pl.when(on)
                def _():
                    w, k, e = place(i, c)
                    turn = (dist == 0) & (w == 0) & (e != y)

                    @pl.when((i >= PM) & (i < PM + 2))
                    def _():
                        @pl.when(turn)
                        def _():
                            pky_copy(1 - y).wait_recv()

                        @pl.when(dist > 0)
                        def _():
                            pkz_copy(d, e).wait_recv()

                        @pl.when(dist < 3)
                        def _():
                            pkz_copy(d, e).start()

                        pkd_copy(d, e, c).start()

                    @pl.when(turn)
                    def _():
                        kyz_copy(k, 1 - y).wait_recv()

                    @pl.when(dist > 0)
                    def _():
                        kz_copy(d, i).wait_recv()

                    @pl.when(dist < 3)
                    def _():
                        kz_copy(d, i).start()

                    @pl.when((dist > 0) & (w == 1))
                    def _():
                        ky_copy(d, k, y).start()

                    kd_copy(d, i, c).start()
                    mirror(num_chain(i, d, c))

                k = h - OUT2 - 2 * rounds
                on = (k >= 0) & (k < rounds)
                k = _clip(k, rounds)

                @pl.when(on)
                def _():
                    ky_copy(d, k, 1 - y).wait_recv()
                    ke_copy(d, k, c).start()
                    mirror(_ref(k, 1, d, 1 - y, c))

                j = h - DIE
                on = (j >= 0) & (j < other_chain)
                j = _clip(j, other_chain)

                @pl.when(on)
                def _():
                    @pl.when((j >= PM) & (j < PM + 2))
                    def _():
                        pkd_copy(d, lax.rem(j, 2), 1 - c).wait_recv()

                    kd_copy(d, j, 1 - c).wait_recv()
                    mirror(num_chain(j, d, 1 - c))

                m = h - OUT2 - DIE - 2 * (9 - rounds)
                on = (m >= 0) & (m < 9 - rounds)
                m = _clip(m, 9 - rounds)

                @pl.when(on)
                def _():
                    ke_copy(d, m, 1 - c).wait_recv()
                    mirror(_ref(m, 1, d, 1 - y, 1 - c))

            p = g - DRV0
            on = (p >= 0) & (p < UP)
            p = _clip(p, UP)

            @pl.when(on)
            def _():
                q = lax.rem(p, 3) * 2
                half = lax.div(p, 3)
                pmt = jnp.concatenate(
                    [pmf[half, lax.div(q, 2), pl.ds(16 * h, 16), :] for h in range(2)], axis=1
                )
                low = lax.dot_general(
                    pmt.astype(f32).T.astype(bf16), ut_ref[...], (((1,), (0,)), ((), ())), preferred_element_type=f32
                )
                cur = theta[panel(p), :]
                grad = -((cur - mu_ref[...]) * lam_ref[...] + low)
                a_ref[panel(p), :] = (grad - rep * cur).astype(bf16)

        for e in range(8):
            @pl.when(me != (e // 4) * 12 + e % 4)
            def _():
                dg_copy(e).wait_send()

        for d in range(2):
            pos = z if d else 3 - z
            for e in range(2):
                @pl.when(pos < 3)
                def _():
                    pz_copy(d, e).wait_send()

                @pl.when(pos > 0)
                def _():
                    pkz_copy(d, e).wait_send()

                pkd_copy(d, e, c).wait_send()

        @pl.when(corner)
        def _():
            pye_copy(1 - y).wait_send()
            pky_copy(y).wait_send()

        @pl.loop(0, rounds)
        def _(k):
            for d in range(2):
                y_copy(d, k).wait_send()
                ke_copy(d, k, c).wait_send()
                ky_copy(d, k, y).wait_send()

            @pl.when(corner)
            def _():
                ye_copy(k, 2 * k + 1 - y).wait_send()
                kyz_copy(k, y).wait_send()

        @pl.loop(0, chain)
        def _(i):
            for d in range(2):
                pos = z if d else 3 - z

                @pl.when(pos < 3)
                def _():
                    z_copy(d, i).wait_send()

                @pl.when(pos > 0)
                def _():
                    kz_copy(d, i).wait_send()

                kd_copy(d, i, c).wait_send()

        @pl.when(corner)
        def _():
            for e in range(16):
                @pl.when(me != e)
                def _():
                    sg_copy(e).wait_send()

    row_sums()

    @pl.loop(0, UP)
    def _(p):
        update(p)
        out_copy(p).start()

    @pl.loop(0, UP)
    def _(p):
        out_copy(p).wait()


def solution(mesh):
    def run_steps(particles, prec_diag, mean_vec, low_rank):
        width = particles.shape[1]

        def local_steps(current, prec_loc, mean_loc, fac_loc):
            n_part, nf = current.shape
            dma = pltpu.SemaphoreType.DMA
            f32, bf16 = jnp.float32, jnp.bfloat16
            vmem = pltpu.VMEM
            return pl.pallas_call(
                functools.partial(kernel, width),
                out_shape=jax.ShapeDtypeStruct((n_part, nf), f32),
                in_specs=[pl.BlockSpec(memory_space=pl.ANY)] + [pl.BlockSpec(memory_space=pltpu.VMEM)] * 3,
                out_specs=pl.BlockSpec(memory_space=pl.ANY),
                scratch_shapes=[
                    vmem((n_part, nf), f32),
                    vmem((n_part, 2 * nf), bf16),
                    vmem((n_part, nf), bf16),
                    vmem((n_part + B, n_part), bf16),
                    vmem((2, CH, B, B), f32),
                    vmem((2, 5, B, B), f32),
                    vmem((2, CH, B, B), f32),
                    vmem((2, 5, B, B), f32),
                    vmem((5, B, B), f32),
                    vmem((2, B, B), f32),
                    vmem((B, B), f32),
                    vmem((2, 2, 32, B), f32),
                    vmem((2, 2, 32, B), f32),
                    vmem((32, B), f32),
                    vmem((2, 4, 32, B), bf16),
                    vmem((16, B), f32),
                    vmem((16, 16, B), f32),
                    vmem((16, B), f32),
                    vmem((16, B), f32),
                    vmem((8, 16, B), f32),
                    vmem((16, B), f32),
                    dma((UP,)), dma((UP,)), dma((UP,)), dma((UP,)), dma, dma, dma((8,)), dma((16,)), dma((16,)), dma((8,)),
                    dma((2, CH)), dma((2, CH)), dma((2, 5)), dma((2, 5)), dma((5,)), dma((5,)),
                    dma((2, CH)), dma((2, CH)), dma((5,)), dma((5,)), dma((2, 5)), dma((2, 5)),
                    dma((2, CH)), dma((2, CH)), dma((2, 5)), dma((2, 5)),
                    dma((2, 2)), dma((2, 2)), dma, dma, dma, dma, dma((2, 2)), dma((2, 2)), dma((2, 2)), dma((2, 2)),
                ],
                compiler_params=pltpu.CompilerParams(
                    collective_id=0, has_side_effects=True, vmem_limit_bytes=56 * 1024 * 1024
                ),
                name="svgd",
            )(current, prec_loc.reshape(1, nf), mean_loc.reshape(1, nf), fac_loc.T)

        sharded = jax.shard_map(
            local_steps,
            mesh=mesh,
            in_specs=(P("ens", FEAT_AXES), P(LEAD_AXES), P(LEAD_AXES), P(LEAD_AXES, None)),
            out_specs=P("ens", FEAT_AXES),
            check_vma=False,
        )
        return sharded(particles, prec_diag, mean_vec, low_rank)

    return run_steps
```

```python
import functools

import jax
import jax.numpy as jnp
from jax import lax
from jax.experimental import pallas as pl
from jax.experimental.pallas import tpu as pltpu
from jax.sharding import PartitionSpec as P

NUM_STEPS = 3
BAND_SCALE = 4.0
STEP_SCALE = 0.4
FEAT_AXES = ("slab", "feat")
LEAD_AXES = ("ens", "slab", "feat")
MESH = pl.DeviceIdType.MESH

B = 128
ROW = 256
UP = 6
START = 2
LAG = 3
END = 2
OUT1 = 2
LAG2 = 4
OUT2 = 4
DIE = 3
YF0 = 3
FIN0 = START + 3 * LAG + END
AG0 = FIN0 + OUT1
CH = 15
PM = 6
DRV0 = AG0 + 3 * LAG2 + PM + 1 + DIE + 1
ITERS = AG0 + 3 * LAG2 + CH + OUT2 + DIE


def _ref(k, t, d, ey, c):
    f = lax.div(k, 4)
    return k * 16 + (1 - f) * (t * 8 + d * 4 + ey * 2 + c) + f * (t * 4 + d * 2 + ey)


def _block(n):
    p = lax.div(n + 126, B) + lax.div(n + 120, B) + lax.div(n + 110, B) + lax.div(n + 96, B) + lax.div(n + 78, B)
    r = n - 2 * p * p
    i = lax.div(r, 2)
    j = 2 * p + lax.rem(r, 2)
    return i, j, p, 1 - jnp.minimum(j - i, 1)


def _clip(i, n):
    return jnp.minimum(jnp.maximum(i, 0), n - 1)


def _span(i):
    return pl.ds(pl.multiple_of(i * B, B), B)


def kernel(width, x_hbm, lam_ref, mu_ref, ut_ref, o_hbm, theta, th, a_ref, kf, kc, ko, gsrc, gy, zrecv, yrecv, yend, pmb, pmrecv,
           ps, pzr, pye, pmf,
           dsrc, dgather, dsum, sacc, sgather, ssum, ld, od, thd_s, thd_r, pm_s, pm_r, dg_s, dg_r, sg_s, sg_r,
           zs, zr, ys, yr, ye_s, ye_r, kz_s, kz_r, kyz_s, kyz_r, ky_s, ky_r, kd_s, kd_r, ke_s, ke_r,
           pz_s, pz_r, pye_s, pye_r, pky_s, pky_r, pkz_s, pkz_r, pkd_s, pkd_r):
    nf = theta.shape[1]
    n_part = theta.shape[0]
    bandwidth = BAND_SCALE * width
    step_size = STEP_SCALE * width
    rep = 2.0 / bandwidth
    f32, bf16 = jnp.float32, jnp.bfloat16
    ens = lax.axis_index("ens")
    z = lax.axis_index("slab")
    feat = lax.axis_index("feat")
    y = lax.div(feat, 2)
    c = lax.rem(feat, 2)
    me = z * 4 + feat
    ypart = (ens, z, (1 - y) * 2 + c)
    dpart = (ens, z, y * 2 + 1 - c)
    dc = lax.div(z, 3)
    corner = lax.rem(z, 3) == 0
    own8 = (dc * 2 + y) * 2 + c
    rounds = 4 + c
    chain = 3 * rounds
    other_chain = 27 - chain

    def rcopy(src, dst, s, r, dev):
        return pltpu.make_async_remote_copy(src_ref=src, dst_ref=dst, send_sem=s, recv_sem=r, device_id=dev, device_id_type=MESH)

    def zdev(dz):
        return (ens, z + dz, feat)

    def place(i, cc):
        zf = 8 + 2 * cc
        w = _clip(i - zf + 1, 2)
        h = lax.div(i, 2)
        return w, h + w * (i - zf - h), i - 2 * h

    def num_chain(i, d, cc):
        w, k, e = place(i, cc)
        return _ref(k, w, d, (1 - w) * e + w * y, cc)

    def panel(p):
        return pl.ds(pl.multiple_of(p * ROW, ROW), ROW)

    def load_copy(p):
        return pltpu.make_async_copy(x_hbm.at[panel(p)], theta.at[panel(p)], ld.at[p])

    def out_copy(p):
        return pltpu.make_async_copy(theta.at[panel(p)], o_hbm.at[panel(p)], od.at[p])

    def th_copy(p):
        return rcopy(th.at[panel(p), pl.ds(0, nf)], th.at[panel(p), pl.ds(nf, nf)], thd_s.at[p], thd_r.at[p], dpart)

    def pm_copy():
        return rcopy(pmb.at[1 - c], pmrecv, pm_s, pm_r, dpart)

    def dg_copy(e):
        return rcopy(dsrc, dgather.at[me], dg_s.at[e], dg_r.at[me], (ens, (e // 4) * 3, e % 4))

    def dg_local():
        return pltpu.make_async_copy(dsrc, dgather.at[me], dg_r.at[me])

    def sg_copy(e):
        return rcopy(sacc, sgather.at[own8], sg_s.at[e], sg_r.at[own8], (ens, e // 4, e % 4))

    def sg_local():
        return pltpu.make_async_copy(sacc, sgather.at[own8], sg_r.at[own8])

    def z_copy(d, i):
        return rcopy(gsrc.at[d, i], zrecv.at[d, i], zs.at[d, i], zr.at[d, i], zdev(2 * d - 1))

    def y_copy(d, k):
        return rcopy(gy.at[d, k], yrecv.at[d, k], ys.at[d, k], yr.at[d, k], ypart)

    def ye_copy(k, i):
        return rcopy(gsrc.at[dc, i], yend.at[k], ye_s.at[k], ye_r.at[k], ypart)

    def kc_copy(d, i, cc, s, r, dev):
        return rcopy(kc.at[cc, d, i], kc.at[cc, d, i], s, r, dev)

    def ko_copy(d, k, cc, s, r, dev):
        return rcopy(ko.at[cc, d, k], ko.at[cc, d, k], s, r, dev)

    def kz_copy(d, i):
        return kc_copy(d, i, c, kz_s.at[d, i], kz_r.at[d, i], zdev(1 - 2 * d))

    def kyz_copy(k, i):
        return kc_copy(dc, i, c, kyz_s.at[k], kyz_r.at[k], ypart)

    def ky_copy(d, k, i):
        return rcopy(kc.at[c, d, i], ko.at[c, d, k], ky_s.at[d, k], ky_r.at[d, k], ypart)

    def kd_copy(d, i, cc):
        return kc_copy(d, i, cc, kd_s.at[d, i], kd_r.at[d, i], dpart)

    def ke_copy(d, k, cc):
        return ko_copy(d, k, cc, ke_s.at[d, k], ke_r.at[d, k], dpart)

    def pz_copy(d, e):
        return rcopy(ps.at[d, e], pzr.at[d, e], pz_s.at[d, e], pz_r.at[d, e], zdev(2 * d - 1))

    def pye_copy(e):
        return rcopy(ps.at[dc, e], pye, pye_s, pye_r, ypart)

    def pf_copy(d, e, cc, s, r, dev):
        return rcopy(pmf.at[cc, 2 * d + e], pmf.at[cc, 2 * d + e], s, r, dev)

    def pky_copy(e):
        return pf_copy(dc, e, c, pky_s, pky_r, ypart)

    def pkz_copy(d, e):
        return pf_copy(d, e, c, pkz_s.at[d, e], pkz_r.at[d, e], zdev(1 - 2 * d))

    def pkd_copy(d, e, cc):
        return pf_copy(d, e, cc, pkd_s.at[d, e], pkd_r.at[d, e], dpart)

    def low_tri():
        return lax.broadcasted_iota(jnp.int32, (B, B), 0) - lax.broadcasted_iota(jnp.int32, (B, B), 1)

    def unpack(kk):
        kt = kk.T
        tri = low_tri()
        return jnp.where(tri >= 0, kk, kt), jnp.where(tri < 0, kk, jnp.where(tri == 0, 1.0, kt))

    def settle(src, n):
        i, j, p, e = _block(n)

        @pl.when(e == 0)
        def _():
            blk = src[...]
            kf[_span(i), _span(j)] = blk
            kf[_span(j), _span(i)] = blk.astype(f32).T.astype(bf16)

        @pl.when(e == 1)
        def _():
            first, second = unpack(src[...].astype(f32))
            kf[_span(2 * p), _span(2 * p)] = first.astype(bf16)
            kf[_span(2 * p + 1), _span(2 * p + 1)] = second.astype(bf16)

    def dot_t(i, j):
        return lax.dot_general(th[_span(i), :], th[_span(j), :], (((1,), (1,)), ((), ())), preferred_element_type=f32)

    def gram(dst, n):
        i, j, p, e = _block(n)
        dst[...] = dot_t(i, j)

        @pl.when(e == 1)
        def _():
            dst[...] = jnp.where(low_tri() >= 0, dst[...], dot_t(2 * p + 1, 2 * p + 1))

    def post(p):
        new = theta[panel(p), :]
        tb = new.astype(bf16)
        th[panel(p), pl.ds(0, nf)] = tb
        xb = (new - mu_ref[...]).astype(bf16)
        pm = lax.dot_general(ut_ref[...], xb, (((1,), (1,)), ((), ())), preferred_element_type=f32)
        th_copy(p).start()
        half = lax.div(p, 3)
        for h in range(2):
            q = lax.rem(p, 3) * 2 + h
            pmb[half, pl.ds(pl.multiple_of(q * 16, 16), 16), :] = pm[:, h * B:(h + 1) * B]
            t = tb[h * B:(h + 1) * B, :].astype(f32)
            sq = t * t
            tot = sq[:, 0:B]
            for m in range(1, nf // B):
                tot = tot + sq[:, m * B:(m + 1) * B]
            dsrc[pl.ds(p * 2 + h, 1), :] = jnp.sum(tot.T, axis=0, keepdims=True)

    def row_sums():
        tot = jnp.zeros((16, B), f32)
        for e in range(8):
            pltpu.make_async_copy(sacc, sgather.at[e], sg_r.at[e]).wait()
            tot = tot + sgather[e]
        ssum[...] = tot

    def update(p):
        acc = jnp.dot(kf[panel(p), :], a_ref[...], preferred_element_type=f32)
        cur = theta[panel(p), :]
        col = jnp.concatenate(
            [jnp.broadcast_to(ssum[pl.ds(p * 2 + h, 1), :], (B, B)).T[:, 0:1] for h in range(2)], axis=0
        )
        phi = (acc + (rep * col) * cur) * (1.0 / n_part)
        theta[panel(p), :] = cur + step_size * phi

    barrier = pltpu.get_barrier_semaphore()
    for o in range(1, 16):
        e = lax.rem(me + o, 16)
        pl.semaphore_signal(barrier, inc=1, device_id=(ens, lax.div(e, 4), lax.rem(e, 4)), device_id_type=MESH)
    for p in range(UP):
        load_copy(p).start()
    pmb[...] = jnp.zeros_like(pmb)
    dsrc[...] = jnp.zeros_like(dsrc)
    pl.semaphore_wait(barrier, 15)

    @pl.loop(0, NUM_STEPS)
    def _(step):
        @pl.when(step > 0)
        def _():
            row_sums()

        sacc[...] = jnp.zeros_like(sacc)

        @pl.loop(0, ITERS)
        def _(g):
            gp = jnp.minimum(g, UP - 1)

            @pl.when(g < UP)
            def _():
                @pl.when(step == 0)
                def _():
                    load_copy(gp).wait()

                @pl.when(step > 0)
                def _():
                    update(gp)

                post(gp)

            @pl.when(g == UP - 1)
            def _():
                for e in range(8):
                    mine = me == (e // 4) * 12 + e % 4

                    @pl.when(mine)
                    def _():
                        dg_local().start()

                    @pl.when(jnp.logical_not(mine))
                    def _():
                        dg_copy(e).start()

                pm_copy().start()

            @pl.when((g >= 1) & (g <= UP))
            def _():
                th_copy(_clip(g - 1, UP)).wait()

            @pl.when(g == START + PM)
            def _():
                pm_copy().wait()

            v = g - YF0
            v_on = (v >= 0) & (v < 2 * rounds)
            v = _clip(v, 2 * rounds)
            vk = lax.div(v, 2)
            vd = v - 2 * vk

            @pl.when(v_on)
            def _():
                gram(gy.at[vd, vk], _ref(vk, 1, vd, 1 - y, c))

            state = []
            for d in range(2):
                pos = z if d else 3 - z
                i = g - START - LAG * pos
                on = (i >= 0) & (i < chain)
                i = _clip(i, chain)
                w, k, e = place(i, c)
                state.append((pos, on, i, w, k, e))

            def send_sum(d):
                pos, on, i, w, k, e = state[d]

                @pl.when(on)
                def _():
                    rides = (i >= PM) & (i < PM + 2)

                    @pl.when(pos < 3)
                    def _():
                        @pl.when(rides)
                        def _():
                            pz_copy(d, e).start()

                        z_copy(d, i).start()

                    @pl.when((pos == 3) & (w == 0) & (e != y))
                    def _():
                        @pl.when(rides)
                        def _():
                            pye_copy(e).start()

                        ye_copy(k, i).start()

            for d in range(2):
                pos, on, i, w, k, e = state[d]

                @pl.when(on)
                def _():
                    gram(gsrc.at[d, i], _ref(k, w, d, e + w * (y - e), c))

                if d == 0:
                    @pl.when(v_on)
                    def _():
                        y_copy(vd, vk).start()
                else:
                    send_sum(0)

                @pl.when(on)
                def _():
                    @pl.when(w == 1)
                    def _():
                        y_copy(d, k).wait_recv()
                        gsrc[d, i] = gsrc[d, i] + yrecv[d, k]

                    @pl.when((i >= PM) & (i < PM + 2))
                    def _():
                        rows = pl.ds(pl.multiple_of((2 * d + e) * 32, 32), 32)
                        ps[d, e] = pmb[c, rows, :] + pmrecv[rows, :]

                        @pl.when(pos > 0)
                        def _():
                            pz_copy(d, e).wait_recv()
                            ps[d, e] = ps[d, e] + pzr[d, e]

                    @pl.when(pos > 0)
                    def _():
                        z_copy(d, i).wait_recv()
                        gsrc[d, i] = gsrc[d, i] + zrecv[d, i]

            i = g - FIN0
            on = corner & (i >= 0) & (i < chain)
            i = _clip(i, chain)
            w, k, e = place(i, c)

            @pl.when(on & (i == 0))
            def _():
                tot = jnp.zeros((16, B), f32)
                for o in range(16):
                    pltpu.make_async_copy(dsrc, dgather.at[o], dg_r.at[o]).wait()
                    tot = tot + dgather[o]
                dsum[...] = tot

            @pl.when(on & ((w == 1) | (e == y)))
            def _():
                @pl.when(w == 0)
                def _():
                    ye_copy(k, i).wait_recv()
                    gsrc[dc, i] = gsrc[dc, i] + yend[k]

                bi, bj, bp, be = _block(_ref(k, w, dc, y, c))

                def kern(gi, gj):
                    sq = jnp.maximum(gi + gj - 2.0 * gsrc[dc, i], 0.0)
                    return jnp.exp(sq * (-1.0 / bandwidth))

                def add_sums(q, blk):
                    sacc[pl.ds(q, 1), :] = sacc[pl.ds(q, 1), :] + jnp.sum(blk, axis=0, keepdims=True)

                @pl.when(be == 0)
                def _():
                    kk = kern(jnp.broadcast_to(dsum[pl.ds(bi, 1), :], (B, B)).T, dsum[pl.ds(bj, 1), :])
                    kc[c, dc, i] = kk.astype(bf16)
                    add_sums(bj, kk)
                    add_sums(bi, kk.T)

                @pl.when(be == 1)
                def _():
                    tri = low_tri() >= 0
                    ga = jnp.broadcast_to(dsum[pl.ds(2 * bp, 1), :], (B, B))
                    gb = jnp.broadcast_to(dsum[pl.ds(2 * bp + 1, 1), :], (B, B))
                    kk = kern(jnp.where(tri, ga.T, gb.T), jnp.where(tri, ga, gb))
                    kk = jnp.where(low_tri() == 0, 1.0, kk)
                    kc[c, dc, i] = kk.astype(bf16)
                    first, second = unpack(kk)
                    add_sums(2 * bp, first)
                    add_sums(2 * bp + 1, second)

                @pl.when((i >= PM) & (i < PM + 2))
                def _():
                    pye_copy(e).wait_recv()
                    pmf[c, 2 * dc + e] = (ps[dc, e] + pye[...]).astype(bf16)

            send_sum(1)

            @pl.when(on & ((w == 1) | (e == y)))
            def _():
                @pl.when((i >= PM) & (i < PM + 2))
                def _():
                    pky_copy(e).start()

                @pl.when(w == 0)
                def _():
                    kyz_copy(k, i).start()

                @pl.when(w == 1)
                def _():
                    ky_copy(dc, k, i).start()

            @pl.when(on & (i == chain - 1))
            def _():
                for o in range(16):
                    @pl.when(me == o)
                    def _():
                        sg_local().start()

                    @pl.when(me != o)
                    def _():
                        sg_copy(o).start()

            heard = []
            for d in range(2):
                dist = 3 - z if d else z
                h = g - AG0 - LAG2 * dist
                on = (h >= 0) & (h < chain)
                i = _clip(h, chain)
                heard.append((h, on, i))

                @pl.when(on)
                def _():
                    w, k, e = place(i, c)
                    turn = (dist == 0) & (w == 0) & (e != y)

                    @pl.when((i >= PM) & (i < PM + 2))
                    def _():
                        @pl.when(turn)
                        def _():
                            pky_copy(1 - y).wait_recv()

                        @pl.when(dist > 0)
                        def _():
                            pkz_copy(d, e).wait_recv()

                        @pl.when(dist < 3)
                        def _():
                            pkz_copy(d, e).start()

                        pkd_copy(d, e, c).start()

                    @pl.when(turn)
                    def _():
                        kyz_copy(k, i).wait_recv()

                    @pl.when(dist > 0)
                    def _():
                        kz_copy(d, i).wait_recv()

                        @pl.when(w == 1)
                        def _():
                            ky_copy(d, k, i).start()

                    @pl.when(dist < 3)
                    def _():
                        kz_copy(d, i).start()

                    kd_copy(d, i, c).start()

                k = h - OUT2 - 2 * rounds

                @pl.when((k >= 0) & (k < rounds))
                def _():
                    kk = _clip(k, rounds)
                    ky_copy(d, kk, 0).wait_recv()
                    ke_copy(d, kk, c).start()

            for d in range(2):
                h, on, i = heard[d]

                @pl.when(on)
                def _():
                    settle(kc.at[c, d, i], num_chain(i, d, c))

                k = h - OUT2 - 2 * rounds

                @pl.when((k >= 0) & (k < rounds))
                def _():
                    kk = _clip(k, rounds)
                    settle(ko.at[c, d, kk], _ref(kk, 1, d, 1 - y, c))

                j = h - DIE

                @pl.when((j >= 0) & (j < other_chain))
                def _():
                    jj = _clip(j, other_chain)

                    @pl.when((jj >= PM) & (jj < PM + 2))
                    def _():
                        pkd_copy(d, jj - 2 * lax.div(jj, 2), 1 - c).wait_recv()

                    kd_copy(d, jj, 1 - c).wait_recv()
                    settle(kc.at[1 - c, d, jj], num_chain(jj, d, 1 - c))

                m = h - OUT2 - DIE - 2 * (9 - rounds)

                @pl.when((m >= 0) & (m < 9 - rounds))
                def _():
                    mm = _clip(m, 9 - rounds)
                    ke_copy(d, mm, 1 - c).wait_recv()
                    settle(ko.at[1 - c, d, mm], _ref(mm, 1, d, 1 - y, 1 - c))

            p = g - DRV0
            on = (p >= 0) & (p < UP)
            p = _clip(p, UP)

            @pl.when(on)
            def _():
                q = lax.rem(p, 3) * 2
                half = lax.div(p, 3)
                pmt = jnp.concatenate(
                    [pmf[half, lax.div(q, 2), pl.ds(16 * h, 16), :] for h in range(2)], axis=1
                )
                low = lax.dot_general(
                    pmt.astype(f32).T.astype(bf16), ut_ref[...], (((1,), (0,)), ((), ())), preferred_element_type=f32
                )
                cur = theta[panel(p), :]
                grad = -((cur - mu_ref[...]) * lam_ref[...] + low)
                a_ref[panel(p), :] = (grad - rep * cur).astype(bf16)

        for e in range(8):
            @pl.when(me != (e // 4) * 12 + e % 4)
            def _():
                dg_copy(e).wait_send()

        for d in range(2):
            pos = z if d else 3 - z
            for e in range(2):
                @pl.when(pos < 3)
                def _():
                    pz_copy(d, e).wait_send()

                @pl.when(pos > 0)
                def _():
                    pkz_copy(d, e).wait_send()

                pkd_copy(d, e, c).wait_send()

        @pl.when(corner)
        def _():
            pye_copy(1 - y).wait_send()
            pky_copy(y).wait_send()

        @pl.loop(0, rounds)
        def _(k):
            for d in range(2):
                y_copy(d, k).wait_send()
                ke_copy(d, k, c).wait_send()
                ky_copy(d, k, 0).wait_send()

            @pl.when(corner)
            def _():
                ye_copy(k, 2 * k + 1 - y).wait_send()
                kyz_copy(k, 0).wait_send()

        @pl.loop(0, chain)
        def _(i):
            for d in range(2):
                pos = z if d else 3 - z

                @pl.when(pos < 3)
                def _():
                    z_copy(d, i).wait_send()

                @pl.when(pos > 0)
                def _():
                    kz_copy(d, i).wait_send()

                kd_copy(d, i, c).wait_send()

        @pl.when(corner)
        def _():
            for e in range(16):
                @pl.when(me != e)
                def _():
                    sg_copy(e).wait_send()

    row_sums()

    @pl.loop(0, UP)
    def _(p):
        update(p)
        out_copy(p).start()

    @pl.loop(0, UP)
    def _(p):
        out_copy(p).wait()


def solution(mesh):
    def run_steps(particles, prec_diag, mean_vec, low_rank):
        width = particles.shape[1]

        def local_steps(current, prec_loc, mean_loc, fac_loc):
            n_part, nf = current.shape
            dma = pltpu.SemaphoreType.DMA
            f32, bf16 = jnp.float32, jnp.bfloat16
            vmem = pltpu.VMEM
            return pl.pallas_call(
                functools.partial(kernel, width),
                out_shape=jax.ShapeDtypeStruct((n_part, nf), f32),
                in_specs=[pl.BlockSpec(memory_space=pl.ANY)] + [pl.BlockSpec(memory_space=pltpu.VMEM)] * 3,
                out_specs=pl.BlockSpec(memory_space=pl.ANY),
                scratch_shapes=[
                    vmem((n_part, nf), f32),
                    vmem((n_part, 2 * nf), bf16),
                    vmem((n_part, nf), bf16),
                    vmem((n_part, n_part), bf16),
                    vmem((2, 2, CH, B, B), bf16),
                    vmem((2, 2, 5, B, B), bf16),
                    vmem((2, CH, B, B), f32),
                    vmem((2, 5, B, B), f32),
                    vmem((2, CH, B, B), f32),
                    vmem((2, 5, B, B), f32),
                    vmem((5, B, B), f32),
                    vmem((2, B, B), f32),
                    vmem((B, B), f32),
                    vmem((2, 2, 32, B), f32),
                    vmem((2, 2, 32, B), f32),
                    vmem((32, B), f32),
                    vmem((2, 4, 32, B), bf16),
                    vmem((16, B), f32),
                    vmem((16, 16, B), f32),
                    vmem((16, B), f32),
                    vmem((16, B), f32),
                    vmem((8, 16, B), f32),
                    vmem((16, B), f32),
                    dma((UP,)), dma((UP,)), dma((UP,)), dma((UP,)), dma, dma, dma((8,)), dma((16,)), dma((16,)), dma((8,)),
                    dma((2, CH)), dma((2, CH)), dma((2, 5)), dma((2, 5)), dma((5,)), dma((5,)),
                    dma((2, CH)), dma((2, CH)), dma((5,)), dma((5,)), dma((2, 5)), dma((2, 5)),
                    dma((2, CH)), dma((2, CH)), dma((2, 5)), dma((2, 5)),
                    dma((2, 2)), dma((2, 2)), dma, dma, dma, dma, dma((2, 2)), dma((2, 2)), dma((2, 2)), dma((2, 2)),
                ],
                compiler_params=pltpu.CompilerParams(
                    collective_id=0, has_side_effects=True, vmem_limit_bytes=56 * 1024 * 1024
                ),
                name="svgd",
            )(current, prec_loc.reshape(1, nf), mean_loc.reshape(1, nf), fac_loc.T)

        sharded = jax.shard_map(
            local_steps,
            mesh=mesh,
            in_specs=(P("ens", FEAT_AXES), P(LEAD_AXES), P(LEAD_AXES), P(LEAD_AXES, None)),
            out_specs=P("ens", FEAT_AXES),
            check_vma=False,
        )
        return sharded(particles, prec_diag, mean_vec, low_rank)

    return run_steps
```

```python
import functools

import jax
import jax.numpy as jnp
from jax import lax
from jax.experimental import pallas as pl
from jax.experimental.pallas import tpu as pltpu
from jax.sharding import PartitionSpec as P

NUM_STEPS = 3
BAND_SCALE = 4.0
STEP_SCALE = 0.4
FEAT_AXES = ("slab", "feat")
LEAD_AXES = ("ens", "slab", "feat")
MESH = pl.DeviceIdType.MESH

B = 128
ROW = 256
UP = 6
START = 2
LAG = 3
END = 2
OUT1 = 2
LAG2 = 3
OUT2 = 3
DIE = 3
YF0 = 3
FIN0 = START + 3 * LAG + END
AG0 = FIN0 + OUT1
CH = 15
PM = 6
DRV0 = AG0 + 3 * LAG2 + PM + 1 + DIE + 1
ITERS = AG0 + 3 * LAG2 + CH + OUT2 + DIE


def _ref(k, t, d, ey, c):
    f = lax.div(k, 4)
    return k * 16 + (1 - f) * (t * 8 + d * 4 + ey * 2 + c) + f * (t * 4 + d * 2 + ey)


def _block(n):
    p = lax.div(n + 126, B) + lax.div(n + 120, B) + lax.div(n + 110, B) + lax.div(n + 96, B) + lax.div(n + 78, B)
    r = n - 2 * p * p
    i = lax.div(r, 2)
    j = 2 * p + lax.rem(r, 2)
    return i, j, p, 1 - jnp.minimum(j - i, 1)


def _clip(i, n):
    return jnp.minimum(jnp.maximum(i, 0), n - 1)


def _span(i):
    return pl.ds(pl.multiple_of(i * B, B), B)


def kernel(width, x_hbm, lam_in, mu_in, ut_ref, o_hbm, theta, th, a_ref, kf, kc, ko, gsrc, gy, zrecv, yrecv, yend, pmb, pmrecv,
           ps, pzr, pye, pmf, lam_ref, mu_ref,
           dsrc, dgather, dsum, sacc, sgather, ssum, ld, od, thd_s, thd_r, pm_s, pm_r, dg_s, dg_r, sg_s, sg_r,
           zs, zr, ys, yr, ye_s, ye_r, kz_s, kz_r, kyz_s, kyz_r, ky_s, ky_r, kd_s, kd_r, ke_s, ke_r,
           pz_s, pz_r, pye_s, pye_r, pky_s, pky_r, pkz_s, pkz_r, pkd_s, pkd_r):
    nf = theta.shape[1]
    n_part = theta.shape[0]
    bandwidth = BAND_SCALE * width
    step_size = STEP_SCALE * width
    rep = 2.0 / bandwidth
    f32, bf16 = jnp.float32, jnp.bfloat16
    ens = lax.axis_index("ens")
    z = lax.axis_index("slab")
    feat = lax.axis_index("feat")
    y = lax.div(feat, 2)
    c = lax.rem(feat, 2)
    me = z * 4 + feat
    ypart = (ens, z, (1 - y) * 2 + c)
    dpart = (ens, z, y * 2 + 1 - c)
    dc = lax.div(z, 3)
    corner = lax.rem(z, 3) == 0
    own8 = (dc * 2 + y) * 2 + c
    rounds = 4 + c
    chain = 3 * rounds
    other_chain = 27 - chain

    def rcopy(src, dst, s, r, dev):
        return pltpu.make_async_remote_copy(src_ref=src, dst_ref=dst, send_sem=s, recv_sem=r, device_id=dev, device_id_type=MESH)

    def zdev(dz):
        return (ens, z + dz, feat)

    def place(i, cc):
        zf = 8 + 2 * cc
        w = _clip(i - zf + 1, 2)
        h = lax.div(i, 2)
        return w, h + w * (i - zf - h), i - 2 * h

    def num_chain(i, d, cc):
        w, k, e = place(i, cc)
        return _ref(k, w, d, (1 - w) * e + w * y, cc)

    def panel(p):
        return pl.ds(pl.multiple_of(p * ROW, ROW), ROW)

    def load_copy(p):
        return pltpu.make_async_copy(x_hbm.at[panel(p)], theta.at[panel(p)], ld.at[p])

    def out_copy(p):
        return pltpu.make_async_copy(theta.at[panel(p)], o_hbm.at[panel(p)], od.at[p])

    def th_copy(p):
        return rcopy(th.at[panel(p), pl.ds(0, nf)], th.at[panel(p), pl.ds(nf, nf)], thd_s.at[p], thd_r.at[p], dpart)

    def pm_copy():
        return rcopy(pmb.at[1 - c], pmrecv, pm_s, pm_r, dpart)

    def dg_copy(e):
        return rcopy(dsrc, dgather.at[me], dg_s.at[e], dg_r.at[me], (ens, (e // 4) * 3, e % 4))

    def dg_local():
        return pltpu.make_async_copy(dsrc, dgather.at[me], dg_r.at[me])

    def sg_copy(e):
        return rcopy(sacc, sgather.at[own8], sg_s.at[e], sg_r.at[own8], (ens, e // 4, e % 4))

    def sg_local():
        return pltpu.make_async_copy(sacc, sgather.at[own8], sg_r.at[own8])

    def z_copy(d, i):
        return rcopy(gsrc.at[d, i], zrecv.at[d, i], zs.at[d, i], zr.at[d, i], zdev(2 * d - 1))

    def y_copy(d, k):
        return rcopy(gy.at[d, k], yrecv.at[d, k], ys.at[d, k], yr.at[d, k], ypart)

    def ye_copy(k, i):
        return rcopy(gsrc.at[dc, i], yend.at[k], ye_s.at[k], ye_r.at[k], ypart)

    def kc_copy(d, i, cc, s, r, dev):
        return rcopy(kc.at[cc, d, i], kc.at[cc, d, i], s, r, dev)

    def ko_copy(d, k, cc, s, r, dev):
        return rcopy(ko.at[cc, d, k], ko.at[cc, d, k], s, r, dev)

    def kz_copy(d, i):
        return kc_copy(d, i, c, kz_s.at[d, i], kz_r.at[d, i], zdev(1 - 2 * d))

    def kyz_copy(k, i):
        return kc_copy(dc, i, c, kyz_s.at[k], kyz_r.at[k], ypart)

    def ky_copy(d, k, i):
        return rcopy(kc.at[c, d, i], ko.at[c, d, k], ky_s.at[d, k], ky_r.at[d, k], ypart)

    def kd_copy(d, i, cc):
        return kc_copy(d, i, cc, kd_s.at[d, i], kd_r.at[d, i], dpart)

    def ke_copy(d, k, cc):
        return ko_copy(d, k, cc, ke_s.at[d, k], ke_r.at[d, k], dpart)

    def pz_copy(d, e):
        return rcopy(ps.at[d, e], pzr.at[d, e], pz_s.at[d, e], pz_r.at[d, e], zdev(2 * d - 1))

    def pye_copy(e):
        return rcopy(ps.at[dc, e], pye, pye_s, pye_r, ypart)

    def pf_copy(d, e, cc, s, r, dev):
        return rcopy(pmf.at[cc, 2 * d + e], pmf.at[cc, 2 * d + e], s, r, dev)

    def pky_copy(e):
        return pf_copy(dc, e, c, pky_s, pky_r, ypart)

    def pkz_copy(d, e):
        return pf_copy(d, e, c, pkz_s.at[d, e], pkz_r.at[d, e], zdev(1 - 2 * d))

    def pkd_copy(d, e, cc):
        return pf_copy(d, e, cc, pkd_s.at[d, e], pkd_r.at[d, e], dpart)

    def low_tri():
        return lax.broadcasted_iota(jnp.int32, (B, B), 0) - lax.broadcasted_iota(jnp.int32, (B, B), 1)

    def unpack(kk):
        kt = kk.T
        tri = low_tri()
        return jnp.where(tri >= 0, kk, kt), jnp.where(tri < 0, kk, jnp.where(tri == 0, 1.0, kt))

    def settle(src, n):
        i, j, p, e = _block(n)

        @pl.when(e == 0)
        def _():
            blk = src[...]
            kf[_span(i), _span(j)] = blk
            kf[_span(j), _span(i)] = blk.astype(f32).T.astype(bf16)

        @pl.when(e == 1)
        def _():
            first, second = unpack(src[...].astype(f32))
            kf[_span(2 * p), _span(2 * p)] = first.astype(bf16)
            kf[_span(2 * p + 1), _span(2 * p + 1)] = second.astype(bf16)

    def dot_t(i, j):
        return lax.dot_general(th[_span(i), :], th[_span(j), :], (((1,), (1,)), ((), ())), preferred_element_type=f32)

    def gram(dst, n):
        i, j, p, e = _block(n)
        dst[...] = dot_t(i, j)

        @pl.when(e == 1)
        def _():
            dst[...] = jnp.where(low_tri() >= 0, dst[...], dot_t(2 * p + 1, 2 * p + 1))

    def post(p):
        new = theta[panel(p), :]
        tb = new.astype(bf16)
        th[panel(p), pl.ds(0, nf)] = tb
        xb = (new - mu_ref[0:1, 0:nf]).astype(bf16)
        pm = lax.dot_general(ut_ref[...], xb, (((1,), (1,)), ((), ())), preferred_element_type=f32)
        th_copy(p).start()
        half = lax.div(p, 3)
        for h in range(2):
            q = lax.rem(p, 3) * 2 + h
            pmb[half, pl.ds(pl.multiple_of(q * 16, 16), 16), :] = pm[:, h * B:(h + 1) * B]
            t = tb[h * B:(h + 1) * B, :].astype(f32)
            sq = t * t
            tot = sq[:, 0:B]
            for m in range(1, nf // B):
                tot = tot + sq[:, m * B:(m + 1) * B]
            dsrc[pl.ds(p * 2 + h, 1), :] = jnp.sum(tot.T, axis=0, keepdims=True)

    def row_sums():
        tot = jnp.zeros((16, B), f32)
        for e in range(8):
            pltpu.make_async_copy(sacc, sgather.at[e], sg_r.at[e]).wait()
            tot = tot + sgather[e]
        ssum[...] = tot

    def update(p):
        acc = jnp.dot(kf[panel(p), :], a_ref[...], preferred_element_type=f32)
        cur = theta[panel(p), :]
        col = jnp.concatenate(
            [jnp.broadcast_to(ssum[pl.ds(p * 2 + h, 1), :], (B, B)).T[:, 0:1] for h in range(2)], axis=0
        )
        phi = (acc + (rep * col) * cur) * (1.0 / n_part)
        theta[panel(p), :] = cur + step_size * phi

    barrier = pltpu.get_barrier_semaphore()
    for o in range(1, 16):
        e = lax.rem(me + o, 16)
        pl.semaphore_signal(barrier, inc=1, device_id=(ens, lax.div(e, 4), lax.rem(e, 4)), device_id_type=MESH)
    for p in range(UP):
        load_copy(p).start()
    pmb[...] = jnp.zeros_like(pmb)
    dsrc[...] = jnp.zeros_like(dsrc)
    for m in range(nf // B):
        lam_ref[0:1, m * B:(m + 1) * B] = lam_in[m:m + 1, :]
        mu_ref[0:1, m * B:(m + 1) * B] = mu_in[m:m + 1, :]
    pl.semaphore_wait(barrier, 15)

    @pl.loop(0, NUM_STEPS)
    def _(step):
        @pl.when(step > 0)
        def _():
            row_sums()

        sacc[...] = jnp.zeros_like(sacc)

        @pl.loop(0, ITERS)
        def _(g):
            gp = jnp.minimum(g, UP - 1)

            @pl.when(g < UP)
            def _():
                @pl.when(step == 0)
                def _():
                    load_copy(gp).wait()

                @pl.when(step > 0)
                def _():
                    update(gp)

                post(gp)

            @pl.when(g == UP - 1)
            def _():
                for e in range(8):
                    mine = me == (e // 4) * 12 + e % 4

                    @pl.when(mine)
                    def _():
                        dg_local().start()

                    @pl.when(jnp.logical_not(mine))
                    def _():
                        dg_copy(e).start()

                pm_copy().start()

            @pl.when((g >= 1) & (g <= UP))
            def _():
                th_copy(_clip(g - 1, UP)).wait()

            @pl.when(g == START + PM)
            def _():
                pm_copy().wait()

            v = g - YF0
            v_on = (v >= 0) & (v < 2 * rounds)
            v = _clip(v, 2 * rounds)
            vk = lax.div(v, 2)
            vd = v - 2 * vk

            @pl.when(v_on)
            def _():
                gram(gy.at[vd, vk], _ref(vk, 1, vd, 1 - y, c))

            state = []
            for d in range(2):
                pos = z if d else 3 - z
                i = g - START - LAG * pos
                on = (i >= 0) & (i < chain)
                i = _clip(i, chain)
                w, k, e = place(i, c)
                state.append((pos, on, i, w, k, e))

            def send_sum(d):
                pos, on, i, w, k, e = state[d]

                @pl.when(on)
                def _():
                    rides = (i >= PM) & (i < PM + 2)

                    @pl.when(pos < 3)
                    def _():
                        @pl.when(rides)
                        def _():
                            pz_copy(d, e).start()

                        z_copy(d, i).start()

                    @pl.when((pos == 3) & (w == 0) & (e != y))
                    def _():
                        @pl.when(rides)
                        def _():
                            pye_copy(e).start()

                        ye_copy(k, i).start()

            for d in range(2):
                pos, on, i, w, k, e = state[d]

                @pl.when(on)
                def _():
                    gram(gsrc.at[d, i], _ref(k, w, d, e + w * (y - e), c))

                if d == 0:
                    @pl.when(v_on)
                    def _():
                        y_copy(vd, vk).start()
                else:
                    send_sum(0)

                @pl.when(on)
                def _():
                    @pl.when(w == 1)
                    def _():
                        y_copy(d, k).wait_recv()
                        gsrc[d, i] = gsrc[d, i] + yrecv[d, k]

                    @pl.when((i >= PM) & (i < PM + 2))
                    def _():
                        rows = pl.ds(pl.multiple_of((2 * d + e) * 32, 32), 32)
                        ps[d, e] = pmb[c, rows, :] + pmrecv[rows, :]

                        @pl.when(pos > 0)
                        def _():
                            pz_copy(d, e).wait_recv()
                            ps[d, e] = ps[d, e] + pzr[d, e]

                    @pl.when(pos > 0)
                    def _():
                        z_copy(d, i).wait_recv()
                        gsrc[d, i] = gsrc[d, i] + zrecv[d, i]

            i = g - FIN0
            on = corner & (i >= 0) & (i < chain)
            i = _clip(i, chain)
            w, k, e = place(i, c)

            @pl.when(on & (i == 0))
            def _():
                tot = jnp.zeros((16, B), f32)
                for o in range(16):
                    pltpu.make_async_copy(dsrc, dgather.at[o], dg_r.at[o]).wait()
                    tot = tot + dgather[o]
                dsum[...] = tot

            @pl.when(on & ((w == 1) | (e == y)))
            def _():
                @pl.when(w == 0)
                def _():
                    ye_copy(k, i).wait_recv()
                    gsrc[dc, i] = gsrc[dc, i] + yend[k]

                bi, bj, bp, be = _block(_ref(k, w, dc, y, c))

                def kern(gi, gj):
                    sq = jnp.maximum(gi + gj - 2.0 * gsrc[dc, i], 0.0)
                    return jnp.exp(sq * (-1.0 / bandwidth))

                def add_sums(q, blk):
                    sacc[pl.ds(q, 1), :] = sacc[pl.ds(q, 1), :] + jnp.sum(blk, axis=0, keepdims=True)

                @pl.when(be == 0)
                def _():
                    kk = kern(jnp.broadcast_to(dsum[pl.ds(bi, 1), :], (B, B)).T, dsum[pl.ds(bj, 1), :])
                    kc[c, dc, i] = kk.astype(bf16)
                    add_sums(bj, kk)
                    add_sums(bi, kk.T)

                @pl.when(be == 1)
                def _():
                    tri = low_tri() >= 0
                    ga = jnp.broadcast_to(dsum[pl.ds(2 * bp, 1), :], (B, B))
                    gb = jnp.broadcast_to(dsum[pl.ds(2 * bp + 1, 1), :], (B, B))
                    kk = kern(jnp.where(tri, ga.T, gb.T), jnp.where(tri, ga, gb))
                    kk = jnp.where(low_tri() == 0, 1.0, kk)
                    kc[c, dc, i] = kk.astype(bf16)
                    first, second = unpack(kk)
                    add_sums(2 * bp, first)
                    add_sums(2 * bp + 1, second)

                @pl.when((i >= PM) & (i < PM + 2))
                def _():
                    pye_copy(e).wait_recv()
                    pmf[c, 2 * dc + e] = (ps[dc, e] + pye[...]).astype(bf16)

            send_sum(1)

            @pl.when(on & ((w == 1) | (e == y)))
            def _():
                @pl.when((i >= PM) & (i < PM + 2))
                def _():
                    pky_copy(e).start()

                @pl.when(w == 0)
                def _():
                    kyz_copy(k, i).start()

                @pl.when(w == 1)
                def _():
                    ky_copy(dc, k, i).start()

            @pl.when(on & (i == chain - 1))
            def _():
                for o in range(16):
                    @pl.when(me == o)
                    def _():
                        sg_local().start()

                    @pl.when(me != o)
                    def _():
                        sg_copy(o).start()

            heard = []
            for d in range(2):
                dist = 3 - z if d else z
                h = g - AG0 - LAG2 * dist
                on = (h >= 0) & (h < chain)
                i = _clip(h, chain)
                heard.append((h, on, i))

                @pl.when(on)
                def _():
                    w, k, e = place(i, c)
                    turn = (dist == 0) & (w == 0) & (e != y)

                    @pl.when((i >= PM) & (i < PM + 2))
                    def _():
                        @pl.when(turn)
                        def _():
                            pky_copy(1 - y).wait_recv()

                        @pl.when(dist > 0)
                        def _():
                            pkz_copy(d, e).wait_recv()

                        @pl.when(dist < 3)
                        def _():
                            pkz_copy(d, e).start()

                        pkd_copy(d, e, c).start()

                    @pl.when(turn)
                    def _():
                        kyz_copy(k, i).wait_recv()

                    @pl.when(dist > 0)
                    def _():
                        kz_copy(d, i).wait_recv()

                        @pl.when(w == 1)
                        def _():
                            ky_copy(d, k, i).start()

                    @pl.when(dist < 3)
                    def _():
                        kz_copy(d, i).start()

                    kd_copy(d, i, c).start()

                k = h - OUT2 - 2 * rounds

                @pl.when((k >= 0) & (k < rounds))
                def _():
                    kk = _clip(k, rounds)
                    ky_copy(d, kk, 0).wait_recv()
                    ke_copy(d, kk, c).start()

            for d in range(2):
                h, on, i = heard[d]

                @pl.when(on)
                def _():
                    settle(kc.at[c, d, i], num_chain(i, d, c))

                k = h - OUT2 - 2 * rounds

                @pl.when((k >= 0) & (k < rounds))
                def _():
                    kk = _clip(k, rounds)
                    settle(ko.at[c, d, kk], _ref(kk, 1, d, 1 - y, c))

                j = h - DIE

                @pl.when((j >= 0) & (j < other_chain))
                def _():
                    jj = _clip(j, other_chain)

                    @pl.when((jj >= PM) & (jj < PM + 2))
                    def _():
                        pkd_copy(d, jj - 2 * lax.div(jj, 2), 1 - c).wait_recv()

                    kd_copy(d, jj, 1 - c).wait_recv()
                    settle(kc.at[1 - c, d, jj], num_chain(jj, d, 1 - c))

                m = h - OUT2 - DIE - 2 * (9 - rounds)

                @pl.when((m >= 0) & (m < 9 - rounds))
                def _():
                    mm = _clip(m, 9 - rounds)
                    ke_copy(d, mm, 1 - c).wait_recv()
                    settle(ko.at[1 - c, d, mm], _ref(mm, 1, d, 1 - y, 1 - c))

            p = g - DRV0
            on = (p >= 0) & (p < UP)
            p = _clip(p, UP)

            @pl.when(on)
            def _():
                q = lax.rem(p, 3) * 2
                half = lax.div(p, 3)
                pmt = jnp.concatenate(
                    [pmf[half, lax.div(q, 2), pl.ds(16 * h, 16), :] for h in range(2)], axis=1
                )
                low = lax.dot_general(
                    pmt.astype(f32).T.astype(bf16), ut_ref[...], (((1,), (0,)), ((), ())), preferred_element_type=f32
                )
                cur = theta[panel(p), :]
                grad = -((cur - mu_ref[0:1, 0:nf]) * lam_ref[0:1, 0:nf] + low)
                a_ref[panel(p), :] = (grad - rep * cur).astype(bf16)

        for e in range(8):
            @pl.when(me != (e // 4) * 12 + e % 4)
            def _():
                dg_copy(e).wait_send()

        for d in range(2):
            pos = z if d else 3 - z
            for e in range(2):
                @pl.when(pos < 3)
                def _():
                    pz_copy(d, e).wait_send()

                @pl.when(pos > 0)
                def _():
                    pkz_copy(d, e).wait_send()

                pkd_copy(d, e, c).wait_send()

        @pl.when(corner)
        def _():
            pye_copy(1 - y).wait_send()
            pky_copy(y).wait_send()

        @pl.loop(0, rounds)
        def _(k):
            for d in range(2):
                y_copy(d, k).wait_send()
                ke_copy(d, k, c).wait_send()
                ky_copy(d, k, 0).wait_send()

            @pl.when(corner)
            def _():
                ye_copy(k, 2 * k + 1 - y).wait_send()
                kyz_copy(k, 0).wait_send()

        @pl.loop(0, chain)
        def _(i):
            for d in range(2):
                pos = z if d else 3 - z

                @pl.when(pos < 3)
                def _():
                    z_copy(d, i).wait_send()

                @pl.when(pos > 0)
                def _():
                    kz_copy(d, i).wait_send()

                kd_copy(d, i, c).wait_send()

        @pl.when(corner)
        def _():
            for e in range(16):
                @pl.when(me != e)
                def _():
                    sg_copy(e).wait_send()

    row_sums()

    @pl.loop(0, UP)
    def _(p):
        update(p)
        out_copy(p).start()

    @pl.loop(0, UP)
    def _(p):
        out_copy(p).wait()


def solution(mesh):
    def run_steps(particles, prec_diag, mean_vec, low_rank):
        width = particles.shape[1]

        def local_steps(current, prec_loc, mean_loc, fac_loc):
            n_part, nf = current.shape
            dma = pltpu.SemaphoreType.DMA
            f32, bf16 = jnp.float32, jnp.bfloat16
            vmem = pltpu.VMEM
            return pl.pallas_call(
                functools.partial(kernel, width),
                out_shape=jax.ShapeDtypeStruct((n_part, nf), f32),
                in_specs=[pl.BlockSpec(memory_space=pl.ANY)] + [pl.BlockSpec(memory_space=pltpu.VMEM)] * 3,
                out_specs=pl.BlockSpec(memory_space=pl.ANY),
                scratch_shapes=[
                    vmem((n_part, nf), f32),
                    vmem((n_part, 2 * nf), bf16),
                    vmem((n_part, nf), bf16),
                    vmem((n_part, n_part), bf16),
                    vmem((2, 2, CH, B, B), bf16),
                    vmem((2, 2, 5, B, B), bf16),
                    vmem((2, CH, B, B), f32),
                    vmem((2, 5, B, B), f32),
                    vmem((2, CH, B, B), f32),
                    vmem((2, 5, B, B), f32),
                    vmem((5, B, B), f32),
                    vmem((2, B, B), f32),
                    vmem((B, B), f32),
                    vmem((2, 2, 32, B), f32),
                    vmem((2, 2, 32, B), f32),
                    vmem((32, B), f32),
                    vmem((2, 4, 32, B), bf16),
                    vmem((8, nf + B), f32),
                    vmem((8, nf + B), f32),
                    vmem((16, B), f32),
                    vmem((16, 16, B), f32),
                    vmem((16, B), f32),
                    vmem((16, B), f32),
                    vmem((8, 16, B), f32),
                    vmem((16, B), f32),
                    dma((UP,)), dma((UP,)), dma((UP,)), dma((UP,)), dma, dma, dma((8,)), dma((16,)), dma((16,)), dma((8,)),
                    dma((2, CH)), dma((2, CH)), dma((2, 5)), dma((2, 5)), dma((5,)), dma((5,)),
                    dma((2, CH)), dma((2, CH)), dma((5,)), dma((5,)), dma((2, 5)), dma((2, 5)),
                    dma((2, CH)), dma((2, CH)), dma((2, 5)), dma((2, 5)),
                    dma((2, 2)), dma((2, 2)), dma, dma, dma, dma, dma((2, 2)), dma((2, 2)), dma((2, 2)), dma((2, 2)),
                ],
                compiler_params=pltpu.CompilerParams(
                    collective_id=0, has_side_effects=True, vmem_limit_bytes=56 * 1024 * 1024
                ),
                name="svgd",
            )(current, prec_loc.reshape(nf // B, B), mean_loc.reshape(nf // B, B), fac_loc.T)

        sharded = jax.shard_map(
            local_steps,
            mesh=mesh,
            in_specs=(P("ens", FEAT_AXES), P(LEAD_AXES), P(LEAD_AXES), P(LEAD_AXES, None)),
            out_specs=P("ens", FEAT_AXES),
            check_vma=False,
        )
        return sharded(particles, prec_diag, mean_vec, low_rank)

    return run_steps
```

```python
import functools

import jax
import jax.numpy as jnp
from jax import lax
from jax.experimental import pallas as pl
from jax.experimental.pallas import tpu as pltpu
from jax.sharding import PartitionSpec as P

NUM_STEPS = 3
BAND_SCALE = 4.0
STEP_SCALE = 0.4
FEAT_AXES = ("slab", "feat")
LEAD_AXES = ("ens", "slab", "feat")
MESH = pl.DeviceIdType.MESH

B = 128
ROW = 256
UP = 6
START = 2
LAG = 3
END = 2
OUT1 = 2
LAG2 = 3
OUT2 = 3
DIE = 3
YF0 = 3
FIN0 = START + 3 * LAG + END
AG0 = FIN0 + OUT1
CH = 15
PM = 6
DRV0 = AG0 + 3 * LAG2 + PM + 1 + DIE + 1
ITERS = AG0 + 3 * LAG2 + CH + OUT2 + DIE
assert YF0 + 10 <= FIN0 and FIN0 + CH <= DRV0 and DRV0 + UP <= ITERS


def _ref(k, t, d, ey, c):
    f = lax.div(k, 4)
    return k * 16 + (1 - f) * (t * 8 + d * 4 + ey * 2 + c) + f * (t * 4 + d * 2 + ey)


def _block(n):
    p = lax.div(n + 126, B) + lax.div(n + 120, B) + lax.div(n + 110, B) + lax.div(n + 96, B) + lax.div(n + 78, B)
    r = n - 2 * p * p
    i = lax.div(r, 2)
    j = 2 * p + lax.rem(r, 2)
    return i, j, p, 1 - jnp.minimum(j - i, 1)


def _clip(i, n):
    return jnp.minimum(jnp.maximum(i, 0), n - 1)


def _span(i):
    return pl.ds(pl.multiple_of(i * B, B), B)


def kernel(width, x_hbm, lam_in, mu_in, ut_ref, o_hbm, theta, th, a_ref, kf, kc, ko, gsrc, gy, zrecv, yrecv, yend, pmb, pmrecv,
           ps, pzr, pye, pmf, lam_ref, mu_ref,
           dsrc, dgather, dsum, sacc, sgather, ssum, ld, od, thd_s, thd_r, pm_s, pm_r, dg_s, dg_r, sg_s, sg_r,
           zs, zr, ys, yr, ye_s, ye_r, kz_s, kz_r, kyz_s, kyz_r, ky_s, ky_r, kd_s, kd_r, ke_s, ke_r,
           pz_s, pz_r, pye_s, pye_r, pky_s, pky_r, pkz_s, pkz_r, pkd_s, pkd_r):
    nf = theta.shape[1]
    n_part = theta.shape[0]
    bandwidth = BAND_SCALE * width
    step_size = STEP_SCALE * width
    rep = 2.0 / bandwidth
    f32, bf16 = jnp.float32, jnp.bfloat16
    ens = lax.axis_index("ens")
    z = lax.axis_index("slab")
    feat = lax.axis_index("feat")
    y = lax.div(feat, 2)
    c = lax.rem(feat, 2)
    me = z * 4 + feat
    ypart = (ens, z, (1 - y) * 2 + c)
    dpart = (ens, z, y * 2 + 1 - c)
    dc = lax.div(z, 3)
    corner = lax.rem(z, 3) == 0
    own8 = (dc * 2 + y) * 2 + c
    rounds = 4 + c
    chain = 3 * rounds
    other_chain = 27 - chain

    def rcopy(src, dst, s, r, dev):
        return pltpu.make_async_remote_copy(src_ref=src, dst_ref=dst, send_sem=s, recv_sem=r, device_id=dev, device_id_type=MESH)

    def zdev(dz):
        return (ens, z + dz, feat)

    def place(i, cc):
        zf = 8 + 2 * cc
        w = _clip(i - zf + 1, 2)
        h = lax.div(i, 2)
        return w, h + w * (i - zf - h), i - 2 * h

    def num_chain(i, d, cc):
        w, k, e = place(i, cc)
        return _ref(k, w, d, (1 - w) * e + w * y, cc)

    def panel(p):
        return pl.ds(pl.multiple_of(p * ROW, ROW), ROW)

    def load_copy(p):
        return pltpu.make_async_copy(x_hbm.at[panel(p)], theta.at[panel(p)], ld.at[p])

    def out_copy(p):
        return pltpu.make_async_copy(theta.at[panel(p)], o_hbm.at[panel(p)], od.at[p])

    def th_copy(p):
        return rcopy(th.at[panel(p), pl.ds(0, nf)], th.at[panel(p), pl.ds(nf, nf)], thd_s.at[p], thd_r.at[p], dpart)

    def pm_copy():
        return rcopy(pmb.at[1 - c], pmrecv, pm_s, pm_r, dpart)

    def dg_copy(e):
        return rcopy(dsrc, dgather.at[me], dg_s.at[e], dg_r.at[me], (ens, (e // 4) * 3, e % 4))

    def dg_local():
        return pltpu.make_async_copy(dsrc, dgather.at[me], dg_r.at[me])

    def sg_copy(e):
        return rcopy(sacc, sgather.at[own8], sg_s.at[e], sg_r.at[own8], (ens, e // 4, e % 4))

    def sg_local():
        return pltpu.make_async_copy(sacc, sgather.at[own8], sg_r.at[own8])

    def z_copy(d, i):
        return rcopy(gsrc.at[d, i], zrecv.at[d, i], zs.at[d, i], zr.at[d, i], zdev(2 * d - 1))

    def y_copy(d, k):
        return rcopy(gy.at[d, k], yrecv.at[d, k], ys.at[d, k], yr.at[d, k], ypart)

    def ye_copy(k, i):
        return rcopy(gsrc.at[dc, i], yend.at[k], ye_s.at[k], ye_r.at[k], ypart)

    def kc_copy(d, i, cc, s, r, dev):
        return rcopy(kc.at[cc, d, i], kc.at[cc, d, i], s, r, dev)

    def ko_copy(d, k, cc, s, r, dev):
        return rcopy(ko.at[cc, d, k], ko.at[cc, d, k], s, r, dev)

    def kz_copy(d, i):
        return kc_copy(d, i, c, kz_s.at[d, i], kz_r.at[d, i], zdev(1 - 2 * d))

    def kyz_copy(k, i):
        return kc_copy(dc, i, c, kyz_s.at[k], kyz_r.at[k], ypart)

    def ky_copy(d, k, i):
        return rcopy(kc.at[c, d, i], ko.at[c, d, k], ky_s.at[d, k], ky_r.at[d, k], ypart)

    def kd_copy(d, i, cc):
        return kc_copy(d, i, cc, kd_s.at[d, i], kd_r.at[d, i], dpart)

    def ke_copy(d, k, cc):
        return ko_copy(d, k, cc, ke_s.at[d, k], ke_r.at[d, k], dpart)

    def pz_copy(d, e):
        return rcopy(ps.at[d, e], pzr.at[d, e], pz_s.at[d, e], pz_r.at[d, e], zdev(2 * d - 1))

    def pye_copy(e):
        return rcopy(ps.at[dc, e], pye, pye_s, pye_r, ypart)

    def pf_copy(d, e, cc, s, r, dev):
        return rcopy(pmf.at[cc, 2 * d + e], pmf.at[cc, 2 * d + e], s, r, dev)

    def pky_copy(e):
        return pf_copy(dc, e, c, pky_s, pky_r, ypart)

    def pkz_copy(d, e):
        return pf_copy(d, e, c, pkz_s.at[d, e], pkz_r.at[d, e], zdev(1 - 2 * d))

    def pkd_copy(d, e, cc):
        return pf_copy(d, e, cc, pkd_s.at[d, e], pkd_r.at[d, e], dpart)

    def low_tri():
        return lax.broadcasted_iota(jnp.int32, (B, B), 0) - lax.broadcasted_iota(jnp.int32, (B, B), 1)

    def unpack(kk):
        kt = kk.T
        tri = low_tri()
        return jnp.where(tri >= 0, kk, kt), jnp.where(tri < 0, kk, jnp.where(tri == 0, 1.0, kt))

    def settle(src, n):
        i, j, p, e = _block(n)

        @pl.when(e == 0)
        def _():
            blk = src[...]
            kf[_span(i), _span(j)] = blk
            kf[_span(j), _span(i)] = blk.astype(f32).T.astype(bf16)

        @pl.when(e == 1)
        def _():
            first, second = unpack(src[...].astype(f32))
            kf[_span(2 * p), _span(2 * p)] = first.astype(bf16)
            kf[_span(2 * p + 1), _span(2 * p + 1)] = second.astype(bf16)

    def dot_t(i, j):
        return lax.dot_general(th[_span(i), :], th[_span(j), :], (((1,), (1,)), ((), ())), preferred_element_type=f32)

    def gram(dst, n):
        i, j, p, e = _block(n)
        dst[...] = dot_t(i, j)

        @pl.when(e == 1)
        def _():
            dst[...] = jnp.where(low_tri() >= 0, dst[...], dot_t(2 * p + 1, 2 * p + 1))

    def post(p):
        new = theta[panel(p), :]
        tb = new.astype(bf16)
        th[panel(p), pl.ds(0, nf)] = tb
        xb = (new - mu_ref[0:1, 0:nf]).astype(bf16)
        pm = lax.dot_general(ut_ref[...], xb, (((1,), (1,)), ((), ())), preferred_element_type=f32)
        th_copy(p).start()
        half = lax.div(p, 3)
        for h in range(2):
            q = lax.rem(p, 3) * 2 + h
            pmb[half, pl.ds(pl.multiple_of(q * 16, 16), 16), :] = pm[:, h * B:(h + 1) * B]
            t = tb[h * B:(h + 1) * B, :].astype(f32)
            sq = t * t
            tot = sq[:, 0:B]
            for m in range(1, nf // B):
                tot = tot + sq[:, m * B:(m + 1) * B]
            dsrc[pl.ds(p * 2 + h, 1), :] = jnp.sum(tot.T, axis=0, keepdims=True)

    def row_sums():
        tot = jnp.zeros((16, B), f32)
        for e in range(8):
            pltpu.make_async_copy(sacc, sgather.at[e], sg_r.at[e]).wait()
            tot = tot + sgather[e]
        ssum[...] = tot

    def update(p):
        acc = jnp.dot(kf[panel(p), :], a_ref[...], preferred_element_type=f32)
        cur = theta[panel(p), :]
        col = jnp.concatenate(
            [jnp.broadcast_to(ssum[pl.ds(p * 2 + h, 1), :], (B, B)).T[:, 0:1] for h in range(2)], axis=0
        )
        phi = (acc + (rep * col) * cur) * (1.0 / n_part)
        theta[panel(p), :] = cur + step_size * phi

    barrier = pltpu.get_barrier_semaphore()
    for o in range(1, 16):
        e = lax.rem(me + o, 16)
        pl.semaphore_signal(barrier, inc=1, device_id=(ens, lax.div(e, 4), lax.rem(e, 4)), device_id_type=MESH)
    for p in range(UP):
        load_copy(p).start()
    pmb[...] = jnp.zeros_like(pmb)
    dsrc[...] = jnp.zeros_like(dsrc)
    for m in range(nf // B):
        lam_ref[0:1, m * B:(m + 1) * B] = lam_in[m:m + 1, :]
        mu_ref[0:1, m * B:(m + 1) * B] = mu_in[m:m + 1, :]
    pl.semaphore_wait(barrier, 15)

    @pl.loop(0, NUM_STEPS)
    def _(step):
        @pl.when(step > 0)
        def _():
            row_sums()

        sacc[...] = jnp.zeros_like(sacc)

        def renew(g):
            gp = jnp.minimum(g, UP - 1)

            @pl.when(g < UP)
            def _():
                @pl.when(step == 0)
                def _():
                    load_copy(gp).wait()

                @pl.when(step > 0)
                def _():
                    update(gp)

                post(gp)

            @pl.when(g == UP - 1)
            def _():
                for e in range(8):
                    mine = me == (e // 4) * 12 + e % 4

                    @pl.when(mine)
                    def _():
                        dg_local().start()

                    @pl.when(jnp.logical_not(mine))
                    def _():
                        dg_copy(e).start()

                pm_copy().start()

            @pl.when((g >= 1) & (g <= UP))
            def _():
                th_copy(_clip(g - 1, UP)).wait()

        def sums(g, yf):
            if yf:
                @pl.when(g == START + PM)
                def _():
                    pm_copy().wait()

            v = g - YF0
            v_on = (v >= 0) & (v < 2 * rounds)
            v = _clip(v, 2 * rounds)
            vk = lax.div(v, 2)
            vd = v - 2 * vk

            if yf:
                @pl.when(v_on)
                def _():
                    gram(gy.at[vd, vk], _ref(vk, 1, vd, 1 - y, c))

            state = []
            for d in range(2):
                pos = z if d else 3 - z
                i = g - START - LAG * pos
                on = (i >= 0) & (i < chain)
                i = _clip(i, chain)
                w, k, e = place(i, c)
                state.append((pos, on, i, w, k, e))

            def send_sum(d):
                pos, on, i, w, k, e = state[d]

                @pl.when(on)
                def _():
                    rides = (i >= PM) & (i < PM + 2)

                    @pl.when(pos < 3)
                    def _():
                        @pl.when(rides)
                        def _():
                            pz_copy(d, e).start()

                        z_copy(d, i).start()

                    @pl.when((pos == 3) & (w == 0) & (e != y))
                    def _():
                        @pl.when(rides)
                        def _():
                            pye_copy(e).start()

                        ye_copy(k, i).start()

            for d in range(2):
                pos, on, i, w, k, e = state[d]

                @pl.when(on)
                def _():
                    gram(gsrc.at[d, i], _ref(k, w, d, e + w * (y - e), c))

                if d == 0 and yf:
                    @pl.when(v_on)
                    def _():
                        y_copy(vd, vk).start()

                if d == 1:
                    send_sum(0)

                @pl.when(on)
                def _():
                    @pl.when(w == 1)
                    def _():
                        y_copy(d, k).wait_recv()
                        gsrc[d, i] = gsrc[d, i] + yrecv[d, k]

                    @pl.when((i >= PM) & (i < PM + 2))
                    def _():
                        rows = pl.ds(pl.multiple_of((2 * d + e) * 32, 32), 32)
                        ps[d, e] = pmb[c, rows, :] + pmrecv[rows, :]

                        @pl.when(pos > 0)
                        def _():
                            pz_copy(d, e).wait_recv()
                            ps[d, e] = ps[d, e] + pzr[d, e]

                    @pl.when(pos > 0)
                    def _():
                        z_copy(d, i).wait_recv()
                        gsrc[d, i] = gsrc[d, i] + zrecv[d, i]

            if yf:
                send_sum(1)
                return

            i = g - FIN0
            on = corner & (i >= 0) & (i < chain)
            i = _clip(i, chain)
            w, k, e = place(i, c)

            @pl.when(on & (i == 0))
            def _():
                tot = jnp.zeros((16, B), f32)
                for o in range(16):
                    pltpu.make_async_copy(dsrc, dgather.at[o], dg_r.at[o]).wait()
                    tot = tot + dgather[o]
                dsum[...] = tot

            @pl.when(on & ((w == 1) | (e == y)))
            def _():
                @pl.when(w == 0)
                def _():
                    ye_copy(k, i).wait_recv()
                    gsrc[dc, i] = gsrc[dc, i] + yend[k]

                bi, bj, bp, be = _block(_ref(k, w, dc, y, c))

                def kern(gi, gj):
                    sq = jnp.maximum(gi + gj - 2.0 * gsrc[dc, i], 0.0)
                    return jnp.exp(sq * (-1.0 / bandwidth))

                def add_sums(q, blk):
                    sacc[pl.ds(q, 1), :] = sacc[pl.ds(q, 1), :] + jnp.sum(blk, axis=0, keepdims=True)

                @pl.when(be == 0)
                def _():
                    kk = kern(jnp.broadcast_to(dsum[pl.ds(bi, 1), :], (B, B)).T, dsum[pl.ds(bj, 1), :])
                    kc[c, dc, i] = kk.astype(bf16)
                    add_sums(bj, kk)
                    add_sums(bi, kk.T)

                @pl.when(be == 1)
                def _():
                    tri = low_tri() >= 0
                    ga = jnp.broadcast_to(dsum[pl.ds(2 * bp, 1), :], (B, B))
                    gb = jnp.broadcast_to(dsum[pl.ds(2 * bp + 1, 1), :], (B, B))
                    kk = kern(jnp.where(tri, ga.T, gb.T), jnp.where(tri, ga, gb))
                    kk = jnp.where(low_tri() == 0, 1.0, kk)
                    kc[c, dc, i] = kk.astype(bf16)
                    first, second = unpack(kk)
                    add_sums(2 * bp, first)
                    add_sums(2 * bp + 1, second)

                @pl.when((i >= PM) & (i < PM + 2))
                def _():
                    pye_copy(e).wait_recv()
                    pmf[c, 2 * dc + e] = (ps[dc, e] + pye[...]).astype(bf16)

            send_sum(1)

            @pl.when(on & ((w == 1) | (e == y)))
            def _():
                @pl.when((i >= PM) & (i < PM + 2))
                def _():
                    pky_copy(e).start()

                @pl.when(w == 0)
                def _():
                    kyz_copy(k, i).start()

                @pl.when(w == 1)
                def _():
                    ky_copy(dc, k, i).start()

            @pl.when(on & (i == chain - 1))
            def _():
                for o in range(16):
                    @pl.when(me == o)
                    def _():
                        sg_local().start()

                    @pl.when(me != o)
                    def _():
                        sg_copy(o).start()

        def spread(g):
            heard = []
            for d in range(2):
                dist = 3 - z if d else z
                h = g - AG0 - LAG2 * dist
                on = (h >= 0) & (h < chain)
                i = _clip(h, chain)
                heard.append((h, on, i))

                @pl.when(on)
                def _():
                    w, k, e = place(i, c)
                    turn = (dist == 0) & (w == 0) & (e != y)

                    @pl.when((i >= PM) & (i < PM + 2))
                    def _():
                        @pl.when(turn)
                        def _():
                            pky_copy(1 - y).wait_recv()

                        @pl.when(dist > 0)
                        def _():
                            pkz_copy(d, e).wait_recv()

                        @pl.when(dist < 3)
                        def _():
                            pkz_copy(d, e).start()

                        pkd_copy(d, e, c).start()

                    @pl.when(turn)
                    def _():
                        kyz_copy(k, i).wait_recv()

                    @pl.when(dist > 0)
                    def _():
                        kz_copy(d, i).wait_recv()

                        @pl.when(w == 1)
                        def _():
                            ky_copy(d, k, i).start()

                    @pl.when(dist < 3)
                    def _():
                        kz_copy(d, i).start()

                    kd_copy(d, i, c).start()

                k = h - OUT2 - 2 * rounds

                @pl.when((k >= 0) & (k < rounds))
                def _():
                    kk = _clip(k, rounds)
                    ky_copy(d, kk, 0).wait_recv()
                    ke_copy(d, kk, c).start()

            for d in range(2):
                h, on, i = heard[d]

                @pl.when(on)
                def _():
                    settle(kc.at[c, d, i], num_chain(i, d, c))

                k = h - OUT2 - 2 * rounds

                @pl.when((k >= 0) & (k < rounds))
                def _():
                    kk = _clip(k, rounds)
                    settle(ko.at[c, d, kk], _ref(kk, 1, d, 1 - y, c))

                j = h - DIE

                @pl.when((j >= 0) & (j < other_chain))
                def _():
                    jj = _clip(j, other_chain)

                    @pl.when((jj >= PM) & (jj < PM + 2))
                    def _():
                        pkd_copy(d, jj - 2 * lax.div(jj, 2), 1 - c).wait_recv()

                    kd_copy(d, jj, 1 - c).wait_recv()
                    settle(kc.at[1 - c, d, jj], num_chain(jj, d, 1 - c))

                m = h - OUT2 - DIE - 2 * (9 - rounds)

                @pl.when((m >= 0) & (m < 9 - rounds))
                def _():
                    mm = _clip(m, 9 - rounds)
                    ke_copy(d, mm, 1 - c).wait_recv()
                    settle(ko.at[1 - c, d, mm], _ref(mm, 1, d, 1 - y, 1 - c))

        def drive(g):
            p = g - DRV0
            on = (p >= 0) & (p < UP)
            p = _clip(p, UP)

            @pl.when(on)
            def _():
                q = lax.rem(p, 3) * 2
                half = lax.div(p, 3)
                pmt = jnp.concatenate(
                    [pmf[half, lax.div(q, 2), pl.ds(16 * h, 16), :] for h in range(2)], axis=1
                )
                low = lax.dot_general(
                    pmt.astype(f32).T.astype(bf16), ut_ref[...], (((1,), (0,)), ((), ())), preferred_element_type=f32
                )
                cur = theta[panel(p), :]
                grad = -((cur - mu_ref[0:1, 0:nf]) * lam_ref[0:1, 0:nf] + low)
                a_ref[panel(p), :] = (grad - rep * cur).astype(bf16)

        @pl.loop(0, UP + 1)
        def _(g):
            renew(g)
            sums(g, True)

        @pl.loop(UP + 1, FIN0)
        def _(g):
            sums(g, True)

        @pl.loop(FIN0, FIN0 + CH)
        def _(g):
            sums(g, False)
            spread(g)

        @pl.loop(FIN0 + CH, ITERS)
        def _(g):
            spread(g)
            drive(g)

        for e in range(8):
            @pl.when(me != (e // 4) * 12 + e % 4)
            def _():
                dg_copy(e).wait_send()

        for d in range(2):
            pos = z if d else 3 - z
            for e in range(2):
                @pl.when(pos < 3)
                def _():
                    pz_copy(d, e).wait_send()

                @pl.when(pos > 0)
                def _():
                    pkz_copy(d, e).wait_send()

                pkd_copy(d, e, c).wait_send()

        @pl.when(corner)
        def _():
            pye_copy(1 - y).wait_send()
            pky_copy(y).wait_send()

        @pl.loop(0, rounds)
        def _(k):
            for d in range(2):
                y_copy(d, k).wait_send()
                ke_copy(d, k, c).wait_send()
                ky_copy(d, k, 0).wait_send()

            @pl.when(corner)
            def _():
                ye_copy(k, 2 * k + 1 - y).wait_send()
                kyz_copy(k, 0).wait_send()

        @pl.loop(0, chain)
        def _(i):
            for d in range(2):
                pos = z if d else 3 - z

                @pl.when(pos < 3)
                def _():
                    z_copy(d, i).wait_send()

                @pl.when(pos > 0)
                def _():
                    kz_copy(d, i).wait_send()

                kd_copy(d, i, c).wait_send()

        @pl.when(corner)
        def _():
            for e in range(16):
                @pl.when(me != e)
                def _():
                    sg_copy(e).wait_send()

    row_sums()

    @pl.loop(0, UP)
    def _(p):
        update(p)
        out_copy(p).start()

    @pl.loop(0, UP)
    def _(p):
        out_copy(p).wait()


def solution(mesh):
    def run_steps(particles, prec_diag, mean_vec, low_rank):
        width = particles.shape[1]

        def local_steps(current, prec_loc, mean_loc, fac_loc):
            n_part, nf = current.shape
            dma = pltpu.SemaphoreType.DMA
            f32, bf16 = jnp.float32, jnp.bfloat16
            vmem = pltpu.VMEM
            return pl.pallas_call(
                functools.partial(kernel, width),
                out_shape=jax.ShapeDtypeStruct((n_part, nf), f32),
                in_specs=[pl.BlockSpec(memory_space=pl.ANY)] + [pl.BlockSpec(memory_space=pltpu.VMEM)] * 3,
                out_specs=pl.BlockSpec(memory_space=pl.ANY),
                scratch_shapes=[
                    vmem((n_part, nf), f32),
                    vmem((n_part, 2 * nf), bf16),
                    vmem((n_part, nf), bf16),
                    vmem((n_part, n_part), bf16),
                    vmem((2, 2, CH, B, B), bf16),
                    vmem((2, 2, 5, B, B), bf16),
                    vmem((2, CH, B, B), f32),
                    vmem((2, 5, B, B), f32),
                    vmem((2, CH, B, B), f32),
                    vmem((2, 5, B, B), f32),
                    vmem((5, B, B), f32),
                    vmem((2, B, B), f32),
                    vmem((B, B), f32),
                    vmem((2, 2, 32, B), f32),
                    vmem((2, 2, 32, B), f32),
                    vmem((32, B), f32),
                    vmem((2, 4, 32, B), bf16),
                    vmem((8, nf + B), f32),
                    vmem((8, nf + B), f32),
                    vmem((16, B), f32),
                    vmem((16, 16, B), f32),
                    vmem((16, B), f32),
                    vmem((16, B), f32),
                    vmem((8, 16, B), f32),
                    vmem((16, B), f32),
                    dma((UP,)), dma((UP,)), dma((UP,)), dma((UP,)), dma, dma, dma((8,)), dma((16,)), dma((16,)), dma((8,)),
                    dma((2, CH)), dma((2, CH)), dma((2, 5)), dma((2, 5)), dma((5,)), dma((5,)),
                    dma((2, CH)), dma((2, CH)), dma((5,)), dma((5,)), dma((2, 5)), dma((2, 5)),
                    dma((2, CH)), dma((2, CH)), dma((2, 5)), dma((2, 5)),
                    dma((2, 2)), dma((2, 2)), dma, dma, dma, dma, dma((2, 2)), dma((2, 2)), dma((2, 2)), dma((2, 2)),
                ],
                compiler_params=pltpu.CompilerParams(
                    collective_id=0, has_side_effects=True, vmem_limit_bytes=56 * 1024 * 1024
                ),
                name="svgd",
            )(current, prec_loc.reshape(nf // B, B), mean_loc.reshape(nf // B, B), fac_loc.T)

        sharded = jax.shard_map(
            local_steps,
            mesh=mesh,
            in_specs=(P("ens", FEAT_AXES), P(LEAD_AXES), P(LEAD_AXES), P(LEAD_AXES, None)),
            out_specs=P("ens", FEAT_AXES),
            check_vma=False,
        )
        return sharded(particles, prec_diag, mean_vec, low_rank)

    return run_steps
```

```python
import functools

import jax
import jax.numpy as jnp
from jax import lax
from jax.experimental import pallas as pl
from jax.experimental.pallas import tpu as pltpu
from jax.sharding import PartitionSpec as P

NUM_STEPS = 3
BAND_SCALE = 4.0
STEP_SCALE = 0.4
FEAT_AXES = ("slab", "feat")
LEAD_AXES = ("ens", "slab", "feat")
MESH = pl.DeviceIdType.MESH

B = 128
ROW = 256
UP = 6
START = 2
LAG = 3
END = 2
OUT1 = 2
LAG2 = 3
OUT2 = 3
DIE = 3
YF0 = 3
FIN0 = START + 3 * LAG + END
AG0 = FIN0 + OUT1
CH = 15
PM = 6
DRV0 = AG0 + 3 * LAG2 + PM + 1 + DIE + 1
ITERS = AG0 + 3 * LAG2 + CH + OUT2 + DIE
assert YF0 + 10 <= FIN0 and FIN0 + CH <= DRV0 and DRV0 + UP <= ITERS


def _ref(k, t, d, ey, c):
    f = lax.div(k, 4)
    return k * 16 + (1 - f) * (t * 8 + d * 4 + ey * 2 + c) + f * (t * 4 + d * 2 + ey)


def _block(n):
    p = lax.div(n + 126, B) + lax.div(n + 120, B) + lax.div(n + 110, B) + lax.div(n + 96, B) + lax.div(n + 78, B)
    r = n - 2 * p * p
    i = lax.div(r, 2)
    j = 2 * p + lax.rem(r, 2)
    return i, j, p, 1 - jnp.minimum(j - i, 1)


def _clip(i, n):
    return jnp.minimum(jnp.maximum(i, 0), n - 1)


def _span(i):
    return pl.ds(pl.multiple_of(i * B, B), B)


def kernel(width, x_hbm, lam_in, mu_in, ut_ref, o_hbm, theta, th, a_ref, kf, kc, ko, gsrc, gy, zrecv, yrecv, yend, pmb, pmrecv,
           ps, pzr, pye, pmf, lam_ref, mu_ref,
           dsrc, dgather, dsum, sacc, sgather, ssum, ld, od, thd_s, thd_r, pm_s, pm_r, dg_s, dg_r, sg_s, sg_r,
           zs, zr, ys, yr, ye_s, ye_r, kz_s, kz_r, kyz_s, kyz_r, ky_s, ky_r, kd_s, kd_r, ke_s, ke_r,
           pz_s, pz_r, pye_s, pye_r, pky_s, pky_r, pkz_s, pkz_r, pkd_s, pkd_r):
    nf = theta.shape[1]
    n_part = theta.shape[0]
    bandwidth = BAND_SCALE * width
    step_size = STEP_SCALE * width
    rep = 2.0 / bandwidth
    f32, bf16 = jnp.float32, jnp.bfloat16
    ens = lax.axis_index("ens")
    z = lax.axis_index("slab")
    feat = lax.axis_index("feat")
    y = lax.div(feat, 2)
    c = lax.rem(feat, 2)
    me = z * 4 + feat
    ypart = (ens, z, (1 - y) * 2 + c)
    dpart = (ens, z, y * 2 + 1 - c)
    dc = lax.div(z, 3)
    corner = lax.rem(z, 3) == 0
    own8 = (dc * 2 + y) * 2 + c
    rounds = 4 + c
    chain = 3 * rounds
    other_chain = 27 - chain

    def rcopy(src, dst, s, r, dev):
        return pltpu.make_async_remote_copy(src_ref=src, dst_ref=dst, send_sem=s, recv_sem=r, device_id=dev, device_id_type=MESH)

    def zdev(dz):
        return (ens, z + dz, feat)

    def place(i, cc):
        zf = 8 + 2 * cc
        w = _clip(i - zf + 1, 2)
        h = lax.div(i, 2)
        return w, h + w * (i - zf - h), i - 2 * h

    def num_chain(i, d, cc):
        w, k, e = place(i, cc)
        return _ref(k, w, d, (1 - w) * e + w * y, cc)

    def panel(p):
        return pl.ds(pl.multiple_of(p * ROW, ROW), ROW)

    def load_copy(p):
        return pltpu.make_async_copy(x_hbm.at[panel(p)], theta.at[panel(p)], ld.at[p])

    def out_copy(p):
        return pltpu.make_async_copy(theta.at[panel(p)], o_hbm.at[panel(p)], od.at[p])

    def th_copy(p):
        return rcopy(th.at[panel(p), pl.ds(0, nf)], th.at[panel(p), pl.ds(nf, nf)], thd_s.at[p], thd_r.at[p], dpart)

    def pm_copy():
        return rcopy(pmb.at[1 - c], pmrecv, pm_s, pm_r, dpart)

    def dg_copy(e):
        return rcopy(dsrc, dgather.at[me], dg_s.at[e], dg_r.at[me], (ens, (e // 4) * 3, e % 4))

    def dg_local():
        return pltpu.make_async_copy(dsrc, dgather.at[me], dg_r.at[me])

    def sg_copy(e):
        return rcopy(sacc, sgather.at[own8], sg_s.at[e], sg_r.at[own8], (ens, e // 4, e % 4))

    def sg_local():
        return pltpu.make_async_copy(sacc, sgather.at[own8], sg_r.at[own8])

    def z_copy(d, i):
        return rcopy(gsrc.at[d, i], zrecv.at[d, i], zs.at[d, i], zr.at[d, i], zdev(2 * d - 1))

    def y_copy(d, k):
        return rcopy(gy.at[d, k], yrecv.at[d, k], ys.at[d, k], yr.at[d, k], ypart)

    def ye_copy(k, i):
        return rcopy(gsrc.at[dc, i], yend.at[k], ye_s.at[k], ye_r.at[k], ypart)

    def kc_copy(d, i, cc, s, r, dev):
        return rcopy(kc.at[cc, d, i], kc.at[cc, d, i], s, r, dev)

    def ko_copy(d, k, cc, s, r, dev):
        return rcopy(ko.at[cc, d, k], ko.at[cc, d, k], s, r, dev)

    def kz_copy(d, i):
        return kc_copy(d, i, c, kz_s.at[d, i], kz_r.at[d, i], zdev(1 - 2 * d))

    def kyz_copy(k, i):
        return kc_copy(dc, i, c, kyz_s.at[k], kyz_r.at[k], ypart)

    def ky_copy(d, k, i):
        return rcopy(kc.at[c, d, i], ko.at[c, d, k], ky_s.at[d, k], ky_r.at[d, k], ypart)

    def kd_copy(d, i, cc):
        return kc_copy(d, i, cc, kd_s.at[d, i], kd_r.at[d, i], dpart)

    def ke_copy(d, k, cc):
        return ko_copy(d, k, cc, ke_s.at[d, k], ke_r.at[d, k], dpart)

    def pz_copy(d, e):
        return rcopy(ps.at[d, e], pzr.at[d, e], pz_s.at[d, e], pz_r.at[d, e], zdev(2 * d - 1))

    def pye_copy(e):
        return rcopy(ps.at[dc, e], pye, pye_s, pye_r, ypart)

    def pf_copy(d, e, cc, s, r, dev):
        return rcopy(pmf.at[cc, 2 * d + e], pmf.at[cc, 2 * d + e], s, r, dev)

    def pky_copy(e):
        return pf_copy(dc, e, c, pky_s, pky_r, ypart)

    def pkz_copy(d, e):
        return pf_copy(d, e, c, pkz_s.at[d, e], pkz_r.at[d, e], zdev(1 - 2 * d))

    def pkd_copy(d, e, cc):
        return pf_copy(d, e, cc, pkd_s.at[d, e], pkd_r.at[d, e], dpart)

    def low_tri():
        return lax.broadcasted_iota(jnp.int32, (B, B), 0) - lax.broadcasted_iota(jnp.int32, (B, B), 1)

    def unpack(kk):
        kt = kk.T
        tri = low_tri()
        return jnp.where(tri >= 0, kk, kt), jnp.where(tri < 0, kk, jnp.where(tri == 0, 1.0, kt))

    def settle(src, n):
        i, j, p, e = _block(n)

        @pl.when(e == 0)
        def _():
            blk = src[...]
            kf[_span(i), _span(j)] = blk
            kf[_span(j), _span(i)] = blk.T

        @pl.when(e == 1)
        def _():
            first, second = unpack(src[...].astype(f32))
            kf[_span(2 * p), _span(2 * p)] = first.astype(bf16)
            kf[_span(2 * p + 1), _span(2 * p + 1)] = second.astype(bf16)

    def dot_t(i, j):
        return lax.dot_general(th[_span(i), :], th[_span(j), :], (((1,), (1,)), ((), ())), preferred_element_type=f32)

    def gram(dst, n):
        i, j, p, e = _block(n)
        dst[...] = dot_t(i, j)

        @pl.when(e == 1)
        def _():
            dst[...] = jnp.where(low_tri() >= 0, dst[...], dot_t(2 * p + 1, 2 * p + 1))

    def post(p):
        new = theta[panel(p), :]
        tb = new.astype(bf16)
        th[panel(p), pl.ds(0, nf)] = tb
        xb = (new - mu_ref[0:1, 0:nf]).astype(bf16)
        pm = lax.dot_general(ut_ref[...], xb, (((1,), (1,)), ((), ())), preferred_element_type=f32)
        th_copy(p).start()
        half = lax.div(p, 3)
        for h in range(2):
            q = lax.rem(p, 3) * 2 + h
            pmb[half, pl.ds(pl.multiple_of(q * 16, 16), 16), :] = pm[:, h * B:(h + 1) * B]
            t = tb[h * B:(h + 1) * B, :].astype(f32)
            sq = t * t
            tot = sq[:, 0:B]
            for m in range(1, nf // B):
                tot = tot + sq[:, m * B:(m + 1) * B]
            dsrc[pl.ds(p * 2 + h, 1), :] = jnp.sum(tot.T, axis=0, keepdims=True)

    def row_sums():
        tot = jnp.zeros((16, B), f32)
        for e in range(8):
            pltpu.make_async_copy(sacc, sgather.at[e], sg_r.at[e]).wait()
            tot = tot + sgather[e]
        ssum[...] = tot

    def update(p):
        acc = jnp.dot(kf[panel(p), :], a_ref[...], preferred_element_type=f32)
        cur = theta[panel(p), :]
        col = jnp.concatenate(
            [jnp.broadcast_to(ssum[pl.ds(p * 2 + h, 1), :], (B, B)).T[:, 0:1] for h in range(2)], axis=0
        )
        phi = (acc + (rep * col) * cur) * (1.0 / n_part)
        theta[panel(p), :] = cur + step_size * phi

    barrier = pltpu.get_barrier_semaphore()
    for o in range(1, 16):
        e = lax.rem(me + o, 16)
        pl.semaphore_signal(barrier, inc=1, device_id=(ens, lax.div(e, 4), lax.rem(e, 4)), device_id_type=MESH)
    for p in range(UP):
        load_copy(p).start()
    pmb[...] = jnp.zeros_like(pmb)
    dsrc[...] = jnp.zeros_like(dsrc)
    for m in range(nf // B):
        lam_ref[0:1, m * B:(m + 1) * B] = lam_in[m:m + 1, :]
        mu_ref[0:1, m * B:(m + 1) * B] = mu_in[m:m + 1, :]
    pl.semaphore_wait(barrier, 15)

    @pl.loop(0, NUM_STEPS)
    def _(step):
        @pl.when(step > 0)
        def _():
            row_sums()

        sacc[...] = jnp.zeros_like(sacc)

        def renew(g):
            gp = jnp.minimum(g, UP - 1)

            @pl.when(g < UP)
            def _():
                @pl.when(step == 0)
                def _():
                    load_copy(gp).wait()

                @pl.when(step > 0)
                def _():
                    update(gp)

                post(gp)

            @pl.when(g == UP - 1)
            def _():
                for e in range(8):
                    mine = me == (e // 4) * 12 + e % 4

                    @pl.when(mine)
                    def _():
                        dg_local().start()

                    @pl.when(jnp.logical_not(mine))
                    def _():
                        dg_copy(e).start()

                pm_copy().start()

            @pl.when((g >= 1) & (g <= UP))
            def _():
                th_copy(_clip(g - 1, UP)).wait()

        def sums(g, yf):
            if yf:
                @pl.when(g == START + PM)
                def _():
                    pm_copy().wait()

            v = g - YF0
            v_on = (v >= 0) & (v < 2 * rounds)
            v = _clip(v, 2 * rounds)
            vk = lax.div(v, 2)
            vd = v - 2 * vk

            if yf:
                @pl.when(v_on)
                def _():
                    gram(gy.at[vd, vk], _ref(vk, 1, vd, 1 - y, c))

            state = []
            for d in range(2):
                pos = z if d else 3 - z
                i = g - START - LAG * pos
                on = (i >= 0) & (i < chain)
                i = _clip(i, chain)
                w, k, e = place(i, c)
                state.append((pos, on, i, w, k, e))

            def send_sum(d):
                pos, on, i, w, k, e = state[d]

                @pl.when(on)
                def _():
                    rides = (i >= PM) & (i < PM + 2)

                    @pl.when(pos < 3)
                    def _():
                        @pl.when(rides)
                        def _():
                            pz_copy(d, e).start()

                        z_copy(d, i).start()

                    @pl.when((pos == 3) & (w == 0) & (e != y))
                    def _():
                        @pl.when(rides)
                        def _():
                            pye_copy(e).start()

                        ye_copy(k, i).start()

            for d in range(2):
                pos, on, i, w, k, e = state[d]

                @pl.when(on)
                def _():
                    gram(gsrc.at[d, i], _ref(k, w, d, e + w * (y - e), c))

                if d == 0 and yf:
                    @pl.when(v_on)
                    def _():
                        y_copy(vd, vk).start()

                if d == 1:
                    send_sum(0)

                @pl.when(on)
                def _():
                    @pl.when(w == 1)
                    def _():
                        y_copy(d, k).wait_recv()
                        gsrc[d, i] = gsrc[d, i] + yrecv[d, k]

                    @pl.when((i >= PM) & (i < PM + 2))
                    def _():
                        rows = pl.ds(pl.multiple_of((2 * d + e) * 32, 32), 32)
                        ps[d, e] = pmb[c, rows, :] + pmrecv[rows, :]

                        @pl.when(pos > 0)
                        def _():
                            pz_copy(d, e).wait_recv()
                            ps[d, e] = ps[d, e] + pzr[d, e]

                    @pl.when(pos > 0)
                    def _():
                        z_copy(d, i).wait_recv()
                        gsrc[d, i] = gsrc[d, i] + zrecv[d, i]

            if yf:
                send_sum(1)
                return

            i = g - FIN0
            on = corner & (i >= 0) & (i < chain)
            i = _clip(i, chain)
            w, k, e = place(i, c)

            @pl.when(on & (i == 0))
            def _():
                tot = jnp.zeros((16, B), f32)
                for o in range(16):
                    pltpu.make_async_copy(dsrc, dgather.at[o], dg_r.at[o]).wait()
                    tot = tot + dgather[o]
                dsum[...] = tot

            @pl.when(on & ((w == 1) | (e == y)))
            def _():
                @pl.when(w == 0)
                def _():
                    ye_copy(k, i).wait_recv()
                    gsrc[dc, i] = gsrc[dc, i] + yend[k]

                bi, bj, bp, be = _block(_ref(k, w, dc, y, c))

                def kern(gi, gj):
                    sq = jnp.maximum(gi + gj - 2.0 * gsrc[dc, i], 0.0)
                    return jnp.exp(sq * (-1.0 / bandwidth))

                def add_sums(q, blk):
                    sacc[pl.ds(q, 1), :] = sacc[pl.ds(q, 1), :] + jnp.sum(blk, axis=0, keepdims=True)

                @pl.when(be == 0)
                def _():
                    kk = kern(jnp.broadcast_to(dsum[pl.ds(bi, 1), :], (B, B)).T, dsum[pl.ds(bj, 1), :])
                    kc[c, dc, i] = kk.astype(bf16)
                    add_sums(bj, kk)
                    add_sums(bi, kk.T)

                @pl.when(be == 1)
                def _():
                    tri = low_tri() >= 0
                    ga = jnp.broadcast_to(dsum[pl.ds(2 * bp, 1), :], (B, B))
                    gb = jnp.broadcast_to(dsum[pl.ds(2 * bp + 1, 1), :], (B, B))
                    kk = kern(jnp.where(tri, ga.T, gb.T), jnp.where(tri, ga, gb))
                    kk = jnp.where(low_tri() == 0, 1.0, kk)
                    kc[c, dc, i] = kk.astype(bf16)
                    first, second = unpack(kk)
                    add_sums(2 * bp, first)
                    add_sums(2 * bp + 1, second)

                @pl.when((i >= PM) & (i < PM + 2))
                def _():
                    pye_copy(e).wait_recv()
                    pmf[c, 2 * dc + e] = (ps[dc, e] + pye[...]).astype(bf16)

            send_sum(1)

            @pl.when(on & ((w == 1) | (e == y)))
            def _():
                @pl.when((i >= PM) & (i < PM + 2))
                def _():
                    pky_copy(e).start()

                @pl.when(w == 0)
                def _():
                    kyz_copy(k, i).start()

                @pl.when(w == 1)
                def _():
                    ky_copy(dc, k, i).start()

            @pl.when(on & (i == chain - 1))
            def _():
                for o in range(16):
                    @pl.when(me == o)
                    def _():
                        sg_local().start()

                    @pl.when(me != o)
                    def _():
                        sg_copy(o).start()

        def spread(g):
            heard = []
            for d in range(2):
                dist = 3 - z if d else z
                h = g - AG0 - LAG2 * dist
                on = (h >= 0) & (h < chain)
                i = _clip(h, chain)
                heard.append((h, on, i))

                @pl.when(on)
                def _():
                    w, k, e = place(i, c)
                    turn = (dist == 0) & (w == 0) & (e != y)

                    @pl.when((i >= PM) & (i < PM + 2))
                    def _():
                        @pl.when(turn)
                        def _():
                            pky_copy(1 - y).wait_recv()

                        @pl.when(dist > 0)
                        def _():
                            pkz_copy(d, e).wait_recv()

                        @pl.when(dist < 3)
                        def _():
                            pkz_copy(d, e).start()

                        pkd_copy(d, e, c).start()

                    @pl.when(turn)
                    def _():
                        kyz_copy(k, i).wait_recv()

                    @pl.when(dist > 0)
                    def _():
                        kz_copy(d, i).wait_recv()

                        @pl.when(w == 1)
                        def _():
                            ky_copy(d, k, i).start()

                    @pl.when(dist < 3)
                    def _():
                        kz_copy(d, i).start()

                    kd_copy(d, i, c).start()

                k = h - OUT2 - 2 * rounds

                @pl.when((k >= 0) & (k < rounds))
                def _():
                    kk = _clip(k, rounds)
                    ky_copy(d, kk, 0).wait_recv()
                    ke_copy(d, kk, c).start()

            for d in range(2):
                h, on, i = heard[d]

                @pl.when(on)
                def _():
                    settle(kc.at[c, d, i], num_chain(i, d, c))

                k = h - OUT2 - 2 * rounds

                @pl.when((k >= 0) & (k < rounds))
                def _():
                    kk = _clip(k, rounds)
                    settle(ko.at[c, d, kk], _ref(kk, 1, d, 1 - y, c))

                j = h - DIE

                @pl.when((j >= 0) & (j < other_chain))
                def _():
                    jj = _clip(j, other_chain)

                    @pl.when((jj >= PM) & (jj < PM + 2))
                    def _():
                        pkd_copy(d, jj - 2 * lax.div(jj, 2), 1 - c).wait_recv()

                    kd_copy(d, jj, 1 - c).wait_recv()
                    settle(kc.at[1 - c, d, jj], num_chain(jj, d, 1 - c))

                m = h - OUT2 - DIE - 2 * (9 - rounds)

                @pl.when((m >= 0) & (m < 9 - rounds))
                def _():
                    mm = _clip(m, 9 - rounds)
                    ke_copy(d, mm, 1 - c).wait_recv()
                    settle(ko.at[1 - c, d, mm], _ref(mm, 1, d, 1 - y, 1 - c))

        def drive(g):
            p = g - DRV0
            on = (p >= 0) & (p < UP)
            p = _clip(p, UP)

            @pl.when(on)
            def _():
                q = lax.rem(p, 3) * 2
                half = lax.div(p, 3)
                pmt = jnp.concatenate(
                    [pmf[half, lax.div(q, 2), pl.ds(16 * h, 16), :] for h in range(2)], axis=1
                )
                low = lax.dot_general(
                    pmt.astype(f32).T.astype(bf16), ut_ref[...], (((1,), (0,)), ((), ())), preferred_element_type=f32
                )
                cur = theta[panel(p), :]
                grad = -((cur - mu_ref[0:1, 0:nf]) * lam_ref[0:1, 0:nf] + low)
                a_ref[panel(p), :] = (grad - rep * cur).astype(bf16)

        @pl.loop(0, UP + 1)
        def _(g):
            renew(g)
            sums(g, True)

        @pl.loop(UP + 1, FIN0)
        def _(g):
            sums(g, True)

        @pl.loop(FIN0, FIN0 + CH)
        def _(g):
            sums(g, False)
            spread(g)

        @pl.loop(FIN0 + CH, ITERS)
        def _(g):
            spread(g)
            drive(g)

        for e in range(8):
            @pl.when(me != (e // 4) * 12 + e % 4)
            def _():
                dg_copy(e).wait_send()

        for d in range(2):
            pos = z if d else 3 - z
            for e in range(2):
                @pl.when(pos < 3)
                def _():
                    pz_copy(d, e).wait_send()

                @pl.when(pos > 0)
                def _():
                    pkz_copy(d, e).wait_send()

                pkd_copy(d, e, c).wait_send()

        @pl.when(corner)
        def _():
            pye_copy(1 - y).wait_send()
            pky_copy(y).wait_send()

        @pl.loop(0, rounds)
        def _(k):
            for d in range(2):
                y_copy(d, k).wait_send()
                ke_copy(d, k, c).wait_send()
                ky_copy(d, k, 0).wait_send()

            @pl.when(corner)
            def _():
                ye_copy(k, 2 * k + 1 - y).wait_send()
                kyz_copy(k, 0).wait_send()

        @pl.loop(0, chain)
        def _(i):
            for d in range(2):
                pos = z if d else 3 - z

                @pl.when(pos < 3)
                def _():
                    z_copy(d, i).wait_send()

                @pl.when(pos > 0)
                def _():
                    kz_copy(d, i).wait_send()

                kd_copy(d, i, c).wait_send()

        @pl.when(corner)
        def _():
            for e in range(16):
                @pl.when(me != e)
                def _():
                    sg_copy(e).wait_send()

    row_sums()

    @pl.loop(0, UP)
    def _(p):
        update(p)
        out_copy(p).start()

    @pl.loop(0, UP)
    def _(p):
        out_copy(p).wait()


def solution(mesh):
    def run_steps(particles, prec_diag, mean_vec, low_rank):
        width = particles.shape[1]

        def local_steps(current, prec_loc, mean_loc, fac_loc):
            n_part, nf = current.shape
            dma = pltpu.SemaphoreType.DMA
            f32, bf16 = jnp.float32, jnp.bfloat16
            vmem = pltpu.VMEM
            return pl.pallas_call(
                functools.partial(kernel, width),
                out_shape=jax.ShapeDtypeStruct((n_part, nf), f32),
                in_specs=[pl.BlockSpec(memory_space=pl.ANY)] + [pl.BlockSpec(memory_space=pltpu.VMEM)] * 3,
                out_specs=pl.BlockSpec(memory_space=pl.ANY),
                scratch_shapes=[
                    vmem((n_part, nf), f32),
                    vmem((n_part, 2 * nf), bf16),
                    vmem((n_part, nf), bf16),
                    vmem((n_part, n_part), bf16),
                    vmem((2, 2, CH, B, B), bf16),
                    vmem((2, 2, 5, B, B), bf16),
                    vmem((2, CH, B, B), f32),
                    vmem((2, 5, B, B), f32),
                    vmem((2, CH, B, B), f32),
                    vmem((2, 5, B, B), f32),
                    vmem((5, B, B), f32),
                    vmem((2, B, B), f32),
                    vmem((B, B), f32),
                    vmem((2, 2, 32, B), f32),
                    vmem((2, 2, 32, B), f32),
                    vmem((32, B), f32),
                    vmem((2, 4, 32, B), bf16),
                    vmem((8, nf + B), f32),
                    vmem((8, nf + B), f32),
                    vmem((16, B), f32),
                    vmem((16, 16, B), f32),
                    vmem((16, B), f32),
                    vmem((16, B), f32),
                    vmem((8, 16, B), f32),
                    vmem((16, B), f32),
                    dma((UP,)), dma((UP,)), dma((UP,)), dma((UP,)), dma, dma, dma((8,)), dma((16,)), dma((16,)), dma((8,)),
                    dma((2, CH)), dma((2, CH)), dma((2, 5)), dma((2, 5)), dma((5,)), dma((5,)),
                    dma((2, CH)), dma((2, CH)), dma((5,)), dma((5,)), dma((2, 5)), dma((2, 5)),
                    dma((2, CH)), dma((2, CH)), dma((2, 5)), dma((2, 5)),
                    dma((2, 2)), dma((2, 2)), dma, dma, dma, dma, dma((2, 2)), dma((2, 2)), dma((2, 2)), dma((2, 2)),
                ],
                compiler_params=pltpu.CompilerParams(
                    collective_id=0, has_side_effects=True, vmem_limit_bytes=56 * 1024 * 1024
                ),
                name="svgd",
            )(current, prec_loc.reshape(nf // B, B), mean_loc.reshape(nf // B, B), fac_loc.T)

        sharded = jax.shard_map(
            local_steps,
            mesh=mesh,
            in_specs=(P("ens", FEAT_AXES), P(LEAD_AXES), P(LEAD_AXES), P(LEAD_AXES, None)),
            out_specs=P("ens", FEAT_AXES),
            check_vma=False,
        )
        return sharded(particles, prec_diag, mean_vec, low_rank)

    return run_steps
```

```python
import functools

import jax
import jax.numpy as jnp
from jax import lax
from jax.experimental import pallas as pl
from jax.experimental.pallas import tpu as pltpu
from jax.sharding import PartitionSpec as P

NUM_STEPS = 3
BAND_SCALE = 4.0
STEP_SCALE = 0.4
FEAT_AXES = ("slab", "feat")
LEAD_AXES = ("ens", "slab", "feat")
MESH = pl.DeviceIdType.MESH

B = 128
ROW = 256
UP = 6
START = 2
LAG = 3
END = 3
OUT1 = 2
LAG2 = 4
OUT2 = 5
DIE = 3
YF0 = 3
FIN0 = START + 3 * LAG + END
AG0 = FIN0 + OUT1
CH = 15
PM = 6
DRV0 = AG0 + 3 * LAG2 + PM + 1 + DIE + 1
ITERS = AG0 + 3 * LAG2 + CH + OUT2 + DIE
assert YF0 + 10 <= FIN0 and FIN0 + CH <= DRV0 and DRV0 + UP <= ITERS


def _ref(k, t, d, ey, c):
    f = lax.div(k, 4)
    return k * 16 + (1 - f) * (t * 8 + d * 4 + ey * 2 + c) + f * (t * 4 + d * 2 + ey)


def _block(n):
    p = lax.div(n + 126, B) + lax.div(n + 120, B) + lax.div(n + 110, B) + lax.div(n + 96, B) + lax.div(n + 78, B)
    r = n - 2 * p * p
    i = lax.div(r, 2)
    j = 2 * p + lax.rem(r, 2)
    return i, j, p, 1 - jnp.minimum(j - i, 1)


def _clip(i, n):
    return jnp.minimum(jnp.maximum(i, 0), n - 1)


def _span(i):
    return pl.ds(pl.multiple_of(i * B, B), B)


def kernel(width, x_hbm, lam_in, mu_in, ut_ref, o_hbm, theta, th, a_ref, kf, kc, ko, gsrc, gy, zrecv, yrecv, yend, pmb, pmrecv,
           ps, pzr, pye, pmf, lam_ref, mu_ref,
           dsrc, dgather, dsum, sacc, sgather, ssum, ld, od, thd_s, thd_r, pm_s, pm_r, dg_s, dg_r, sg_s, sg_r,
           zs, zr, ys, yr, ye_s, ye_r, kz_s, kz_r, kyz_s, kyz_r, ky_s, ky_r, kd_s, kd_r, ke_s, ke_r,
           pz_s, pz_r, pye_s, pye_r, pky_s, pky_r, pkz_s, pkz_r, pkd_s, pkd_r):
    nf = theta.shape[1]
    n_part = theta.shape[0]
    bandwidth = BAND_SCALE * width
    step_size = STEP_SCALE * width
    rep = 2.0 / bandwidth
    f32, bf16 = jnp.float32, jnp.bfloat16
    ens = lax.axis_index("ens")
    z = lax.axis_index("slab")
    feat = lax.axis_index("feat")
    y = lax.div(feat, 2)
    c = lax.rem(feat, 2)
    me = z * 4 + feat
    ypart = (ens, z, (1 - y) * 2 + c)
    dpart = (ens, z, y * 2 + 1 - c)
    dc = lax.div(z, 3)
    corner = lax.rem(z, 3) == 0
    own8 = (dc * 2 + y) * 2 + c
    rounds = 4 + c
    chain = 3 * rounds
    other_chain = 27 - chain

    def rcopy(src, dst, s, r, dev):
        return pltpu.make_async_remote_copy(src_ref=src, dst_ref=dst, send_sem=s, recv_sem=r, device_id=dev, device_id_type=MESH)

    def zdev(dz):
        return (ens, z + dz, feat)

    def place(i, cc):
        zf = 8 + 2 * cc
        w = _clip(i - zf + 1, 2)
        h = lax.div(i, 2)
        return w, h + w * (i - zf - h), i - 2 * h

    def num_chain(i, d, cc):
        w, k, e = place(i, cc)
        return _ref(k, w, d, (1 - w) * e + w * y, cc)

    def panel(p):
        return pl.ds(pl.multiple_of(p * ROW, ROW), ROW)

    def load_copy(p):
        return pltpu.make_async_copy(x_hbm.at[panel(p)], theta.at[panel(p)], ld.at[p])

    def out_copy(p):
        return pltpu.make_async_copy(theta.at[panel(p)], o_hbm.at[panel(p)], od.at[p])

    def th_copy(p):
        return rcopy(th.at[panel(p), pl.ds(0, nf)], th.at[panel(p), pl.ds(nf, nf)], thd_s.at[p], thd_r.at[p], dpart)

    def pm_copy():
        return rcopy(pmb.at[1 - c], pmrecv, pm_s, pm_r, dpart)

    def dg_copy(e):
        return rcopy(dsrc, dgather.at[me], dg_s.at[e], dg_r.at[me], (ens, (e // 4) * 3, e % 4))

    def dg_local():
        return pltpu.make_async_copy(dsrc, dgather.at[me], dg_r.at[me])

    def sg_copy(e):
        return rcopy(sacc, sgather.at[own8], sg_s.at[e], sg_r.at[own8], (ens, e // 4, e % 4))

    def sg_local():
        return pltpu.make_async_copy(sacc, sgather.at[own8], sg_r.at[own8])

    def z_copy(d, i):
        return rcopy(gsrc.at[d, i], zrecv.at[d, i], zs.at[d, i], zr.at[d, i], zdev(2 * d - 1))

    def y_copy(d, k):
        return rcopy(gy.at[d, k], yrecv.at[d, k], ys.at[d, k], yr.at[d, k], ypart)

    def ye_copy(k, i):
        return rcopy(gsrc.at[dc, i], yend.at[k], ye_s.at[k], ye_r.at[k], ypart)

    def kc_copy(d, i, cc, s, r, dev):
        return rcopy(kc.at[cc, d, i], kc.at[cc, d, i], s, r, dev)

    def ko_copy(d, k, cc, s, r, dev):
        return rcopy(ko.at[cc, d, k], ko.at[cc, d, k], s, r, dev)

    def kz_copy(d, i):
        return kc_copy(d, i, c, kz_s.at[d, i], kz_r.at[d, i], zdev(1 - 2 * d))

    def kyz_copy(k, i):
        return kc_copy(dc, i, c, kyz_s.at[k], kyz_r.at[k], ypart)

    def ky_copy(d, k, i):
        return rcopy(kc.at[c, d, i], ko.at[c, d, k], ky_s.at[d, k], ky_r.at[d, k], ypart)

    def kd_copy(d, i, cc):
        return kc_copy(d, i, cc, kd_s.at[d, i], kd_r.at[d, i], dpart)

    def ke_copy(d, k, cc):
        return ko_copy(d, k, cc, ke_s.at[d, k], ke_r.at[d, k], dpart)

    def pz_copy(d, e):
        return rcopy(ps.at[d, e], pzr.at[d, e], pz_s.at[d, e], pz_r.at[d, e], zdev(2 * d - 1))

    def pye_copy(e):
        return rcopy(ps.at[dc, e], pye, pye_s, pye_r, ypart)

    def pf_copy(d, e, cc, s, r, dev):
        return rcopy(pmf.at[cc, 2 * d + e], pmf.at[cc, 2 * d + e], s, r, dev)

    def pky_copy(e):
        return pf_copy(dc, e, c, pky_s, pky_r, ypart)

    def pkz_copy(d, e):
        return pf_copy(d, e, c, pkz_s.at[d, e], pkz_r.at[d, e], zdev(1 - 2 * d))

    def pkd_copy(d, e, cc):
        return pf_copy(d, e, cc, pkd_s.at[d, e], pkd_r.at[d, e], dpart)

    def low_tri():
        return lax.broadcasted_iota(jnp.int32, (B, B), 0) - lax.broadcasted_iota(jnp.int32, (B, B), 1)

    def unpack(kk):
        kt = kk.T
        tri = low_tri()
        return jnp.where(tri >= 0, kk, kt), jnp.where(tri < 0, kk, jnp.where(tri == 0, 1.0, kt))

    def settle(src, n):
        i, j, p, e = _block(n)

        @pl.when(e == 0)
        def _():
            blk = src[...]
            kf[_span(i), _span(j)] = blk
            kf[_span(j), _span(i)] = blk.T

        @pl.when(e == 1)
        def _():
            first, second = unpack(src[...].astype(f32))
            kf[_span(2 * p), _span(2 * p)] = first.astype(bf16)
            kf[_span(2 * p + 1), _span(2 * p + 1)] = second.astype(bf16)

    def dot_t(i, j):
        return lax.dot_general(th[_span(i), :], th[_span(j), :], (((1,), (1,)), ((), ())), preferred_element_type=f32)

    def gram(dst, n):
        i, j, p, e = _block(n)
        dst[...] = dot_t(i, j)

        @pl.when(e == 1)
        def _():
            dst[...] = jnp.where(low_tri() >= 0, dst[...], dot_t(2 * p + 1, 2 * p + 1))

    def post(p):
        new = theta[panel(p), :]
        tb = new.astype(bf16)
        th[panel(p), pl.ds(0, nf)] = tb
        xb = (new - mu_ref[0:1, 0:nf]).astype(bf16)
        pm = lax.dot_general(ut_ref[...], xb, (((1,), (1,)), ((), ())), preferred_element_type=f32)
        th_copy(p).start()
        half = lax.div(p, 3)
        for h in range(2):
            q = lax.rem(p, 3) * 2 + h
            pmb[half, pl.ds(pl.multiple_of(q * 16, 16), 16), :] = pm[:, h * B:(h + 1) * B]
            t = tb[h * B:(h + 1) * B, :].astype(f32)
            sq = t * t
            tot = sq[:, 0:B]
            for m in range(1, nf // B):
                tot = tot + sq[:, m * B:(m + 1) * B]
            dsrc[pl.ds(p * 2 + h, 1), :] = jnp.sum(tot.T, axis=0, keepdims=True)

    def row_sums():
        tot = jnp.zeros((16, B), f32)
        for e in range(8):
            pltpu.make_async_copy(sacc, sgather.at[e], sg_r.at[e]).wait()
            tot = tot + sgather[e]
        ssum[...] = tot

    def update(p):
        acc = jnp.dot(kf[panel(p), :], a_ref[...], preferred_element_type=f32)
        cur = theta[panel(p), :]
        col = jnp.concatenate(
            [jnp.broadcast_to(ssum[pl.ds(p * 2 + h, 1), :], (B, B)).T[:, 0:1] for h in range(2)], axis=0
        )
        phi = (acc + (rep * col) * cur) * (1.0 / n_part)
        theta[panel(p), :] = cur + step_size * phi

    barrier = pltpu.get_barrier_semaphore()
    for o in range(1, 16):
        e = lax.rem(me + o, 16)
        pl.semaphore_signal(barrier, inc=1, device_id=(ens, lax.div(e, 4), lax.rem(e, 4)), device_id_type=MESH)
    for p in range(UP):
        load_copy(p).start()
    pmb[...] = jnp.zeros_like(pmb)
    dsrc[...] = jnp.zeros_like(dsrc)
    for m in range(nf // B):
        lam_ref[0:1, m * B:(m + 1) * B] = lam_in[m:m + 1, :]
        mu_ref[0:1, m * B:(m + 1) * B] = mu_in[m:m + 1, :]
    pl.semaphore_wait(barrier, 15)

    @pl.loop(0, NUM_STEPS)
    def _(step):
        @pl.when(step > 0)
        def _():
            row_sums()

        sacc[...] = jnp.zeros_like(sacc)

        def renew(g):
            gp = jnp.minimum(g, UP - 1)

            @pl.when(g < UP)
            def _():
                @pl.when(step == 0)
                def _():
                    load_copy(gp).wait()

                @pl.when(step > 0)
                def _():
                    update(gp)

                post(gp)

            @pl.when(g == UP - 1)
            def _():
                for e in range(8):
                    mine = me == (e // 4) * 12 + e % 4

                    @pl.when(mine)
                    def _():
                        dg_local().start()

                    @pl.when(jnp.logical_not(mine))
                    def _():
                        dg_copy(e).start()

                pm_copy().start()

            @pl.when((g >= 1) & (g <= UP))
            def _():
                th_copy(_clip(g - 1, UP)).wait()

        def sums(g, yf):
            if yf:
                @pl.when(g == START + PM)
                def _():
                    pm_copy().wait()

            v = g - YF0
            v_on = (v >= 0) & (v < 2 * rounds)
            v = _clip(v, 2 * rounds)
            vk = lax.div(v, 2)
            vd = v - 2 * vk

            if yf:
                @pl.when(v_on)
                def _():
                    gram(gy.at[vd, vk], _ref(vk, 1, vd, 1 - y, c))

            state = []
            for d in range(2):
                pos = z if d else 3 - z
                i = g - START - LAG * pos
                on = (i >= 0) & (i < chain)
                i = _clip(i, chain)
                w, k, e = place(i, c)
                state.append((pos, on, i, w, k, e))

            def send_sum(d):
                pos, on, i, w, k, e = state[d]

                @pl.when(on)
                def _():
                    rides = (i >= PM) & (i < PM + 2)

                    @pl.when(pos < 3)
                    def _():
                        @pl.when(rides)
                        def _():
                            pz_copy(d, e).start()

                        z_copy(d, i).start()

                    @pl.when((pos == 3) & (w == 0) & (e != y))
                    def _():
                        @pl.when(rides)
                        def _():
                            pye_copy(e).start()

                        ye_copy(k, i).start()

            for d in range(2):
                pos, on, i, w, k, e = state[d]

                @pl.when(on)
                def _():
                    gram(gsrc.at[d, i], _ref(k, w, d, e + w * (y - e), c))

                if d == 0 and yf:
                    @pl.when(v_on)
                    def _():
                        y_copy(vd, vk).start()

                if d == 1:
                    send_sum(0)

                @pl.when(on)
                def _():
                    @pl.when(w == 1)
                    def _():
                        y_copy(d, k).wait_recv()
                        gsrc[d, i] = gsrc[d, i] + yrecv[d, k]

                    @pl.when((i >= PM) & (i < PM + 2))
                    def _():
                        rows = pl.ds(pl.multiple_of((2 * d + e) * 32, 32), 32)
                        ps[d, e] = pmb[c, rows, :] + pmrecv[rows, :]

                        @pl.when(pos > 0)
                        def _():
                            pz_copy(d, e).wait_recv()
                            ps[d, e] = ps[d, e] + pzr[d, e]

                    @pl.when(pos > 0)
                    def _():
                        z_copy(d, i).wait_recv()
                        gsrc[d, i] = gsrc[d, i] + zrecv[d, i]

            if yf:
                send_sum(1)
                return

            i = g - FIN0
            on = corner & (i >= 0) & (i < chain)
            i = _clip(i, chain)
            w, k, e = place(i, c)

            @pl.when(on & (i == 0))
            def _():
                tot = jnp.zeros((16, B), f32)
                for o in range(16):
                    pltpu.make_async_copy(dsrc, dgather.at[o], dg_r.at[o]).wait()
                    tot = tot + dgather[o]
                dsum[...] = tot

            @pl.when(on & ((w == 1) | (e == y)))
            def _():
                @pl.when(w == 0)
                def _():
                    ye_copy(k, i).wait_recv()
                    gsrc[dc, i] = gsrc[dc, i] + yend[k]

                bi, bj, bp, be = _block(_ref(k, w, dc, y, c))

                def kern(gi, gj):
                    sq = jnp.maximum(gi + gj - 2.0 * gsrc[dc, i], 0.0)
                    return jnp.exp(sq * (-1.0 / bandwidth))

                def add_sums(q, blk):
                    sacc[pl.ds(q, 1), :] = sacc[pl.ds(q, 1), :] + jnp.sum(blk, axis=0, keepdims=True)

                @pl.when(be == 0)
                def _():
                    kk = kern(jnp.broadcast_to(dsum[pl.ds(bi, 1), :], (B, B)).T, dsum[pl.ds(bj, 1), :])
                    kc[c, dc, i] = kk.astype(bf16)
                    add_sums(bj, kk)
                    add_sums(bi, kk.T)

                @pl.when(be == 1)
                def _():
                    tri = low_tri() >= 0
                    ga = jnp.broadcast_to(dsum[pl.ds(2 * bp, 1), :], (B, B))
                    gb = jnp.broadcast_to(dsum[pl.ds(2 * bp + 1, 1), :], (B, B))
                    kk = kern(jnp.where(tri, ga.T, gb.T), jnp.where(tri, ga, gb))
                    kk = jnp.where(low_tri() == 0, 1.0, kk)
                    kc[c, dc, i] = kk.astype(bf16)
                    first, second = unpack(kk)
                    add_sums(2 * bp, first)
                    add_sums(2 * bp + 1, second)

                @pl.when((i >= PM) & (i < PM + 2))
                def _():
                    pye_copy(e).wait_recv()
                    pmf[c, 2 * dc + e] = (ps[dc, e] + pye[...]).astype(bf16)

            send_sum(1)

            @pl.when(on & ((w == 1) | (e == y)))
            def _():
                @pl.when((i >= PM) & (i < PM + 2))
                def _():
                    pky_copy(e).start()

                @pl.when(w == 0)
                def _():
                    kyz_copy(k, i).start()

                @pl.when(w == 1)
                def _():
                    ky_copy(dc, k, i).start()

            @pl.when(on & (i == chain - 1))
            def _():
                for o in range(16):
                    @pl.when(me == o)
                    def _():
                        sg_local().start()

                    @pl.when(me != o)
                    def _():
                        sg_copy(o).start()

        def spread(g):
            heard = []
            for d in range(2):
                dist = 3 - z if d else z
                h = g - AG0 - LAG2 * dist
                on = (h >= 0) & (h < chain)
                i = _clip(h, chain)
                heard.append((h, on, i))

                @pl.when(on)
                def _():
                    w, k, e = place(i, c)
                    turn = (dist == 0) & (w == 0) & (e != y)

                    @pl.when((i >= PM) & (i < PM + 2))
                    def _():
                        @pl.when(turn)
                        def _():
                            pky_copy(1 - y).wait_recv()

                        @pl.when(dist > 0)
                        def _():
                            pkz_copy(d, e).wait_recv()

                        @pl.when(dist < 3)
                        def _():
                            pkz_copy(d, e).start()

                        pkd_copy(d, e, c).start()

                    @pl.when(turn)
                    def _():
                        kyz_copy(k, i).wait_recv()

                    @pl.when(dist > 0)
                    def _():
                        kz_copy(d, i).wait_recv()

                        @pl.when(w == 1)
                        def _():
                            ky_copy(d, k, i).start()

                    @pl.when(dist < 3)
                    def _():
                        kz_copy(d, i).start()

                    kd_copy(d, i, c).start()

                k = h - OUT2 - 2 * rounds

                @pl.when((k >= 0) & (k < rounds))
                def _():
                    kk = _clip(k, rounds)
                    ky_copy(d, kk, 0).wait_recv()
                    ke_copy(d, kk, c).start()

            for d in range(2):
                h, on, i = heard[d]

                @pl.when(on)
                def _():
                    settle(kc.at[c, d, i], num_chain(i, d, c))

                k = h - OUT2 - 2 * rounds

                @pl.when((k >= 0) & (k < rounds))
                def _():
                    kk = _clip(k, rounds)
                    settle(ko.at[c, d, kk], _ref(kk, 1, d, 1 - y, c))

                j = h - DIE

                @pl.when((j >= 0) & (j < other_chain))
                def _():
                    jj = _clip(j, other_chain)

                    @pl.when((jj >= PM) & (jj < PM + 2))
                    def _():
                        pkd_copy(d, jj - 2 * lax.div(jj, 2), 1 - c).wait_recv()

                    kd_copy(d, jj, 1 - c).wait_recv()
                    settle(kc.at[1 - c, d, jj], num_chain(jj, d, 1 - c))

                m = h - OUT2 - DIE - 2 * (9 - rounds)

                @pl.when((m >= 0) & (m < 9 - rounds))
                def _():
                    mm = _clip(m, 9 - rounds)
                    ke_copy(d, mm, 1 - c).wait_recv()
                    settle(ko.at[1 - c, d, mm], _ref(mm, 1, d, 1 - y, 1 - c))

        def drive(g):
            p = g - DRV0
            on = (p >= 0) & (p < UP)
            p = _clip(p, UP)

            @pl.when(on)
            def _():
                q = lax.rem(p, 3) * 2
                half = lax.div(p, 3)
                pmt = jnp.concatenate(
                    [pmf[half, lax.div(q, 2), pl.ds(16 * h, 16), :] for h in range(2)], axis=1
                )
                low = lax.dot_general(
                    pmt.astype(f32).T.astype(bf16), ut_ref[...], (((1,), (0,)), ((), ())), preferred_element_type=f32
                )
                cur = theta[panel(p), :]
                grad = -((cur - mu_ref[0:1, 0:nf]) * lam_ref[0:1, 0:nf] + low)
                a_ref[panel(p), :] = (grad - rep * cur).astype(bf16)

        @pl.loop(0, UP + 1)
        def _(g):
            renew(g)
            sums(g, True)

        @pl.loop(UP + 1, FIN0)
        def _(g):
            sums(g, True)

        @pl.loop(FIN0, FIN0 + CH)
        def _(g):
            sums(g, False)
            spread(g)

        @pl.loop(FIN0 + CH, ITERS)
        def _(g):
            spread(g)
            drive(g)

        for e in range(8):
            @pl.when(me != (e // 4) * 12 + e % 4)
            def _():
                dg_copy(e).wait_send()

        for d in range(2):
            pos = z if d else 3 - z
            for e in range(2):
                @pl.when(pos < 3)
                def _():
                    pz_copy(d, e).wait_send()

                @pl.when(pos > 0)
                def _():
                    pkz_copy(d, e).wait_send()

                pkd_copy(d, e, c).wait_send()

        @pl.when(corner)
        def _():
            pye_copy(1 - y).wait_send()
            pky_copy(y).wait_send()

        @pl.loop(0, rounds)
        def _(k):
            for d in range(2):
                y_copy(d, k).wait_send()
                ke_copy(d, k, c).wait_send()
                ky_copy(d, k, 0).wait_send()

            @pl.when(corner)
            def _():
                ye_copy(k, 2 * k + 1 - y).wait_send()
                kyz_copy(k, 0).wait_send()

        @pl.loop(0, chain)
        def _(i):
            for d in range(2):
                pos = z if d else 3 - z

                @pl.when(pos < 3)
                def _():
                    z_copy(d, i).wait_send()

                @pl.when(pos > 0)
                def _():
                    kz_copy(d, i).wait_send()

                kd_copy(d, i, c).wait_send()

        @pl.when(corner)
        def _():
            for e in range(16):
                @pl.when(me != e)
                def _():
                    sg_copy(e).wait_send()

    row_sums()

    @pl.loop(0, UP)
    def _(p):
        update(p)
        out_copy(p).start()

    @pl.loop(0, UP)
    def _(p):
        out_copy(p).wait()


def solution(mesh):
    def run_steps(particles, prec_diag, mean_vec, low_rank):
        width = particles.shape[1]

        def local_steps(current, prec_loc, mean_loc, fac_loc):
            n_part, nf = current.shape
            dma = pltpu.SemaphoreType.DMA
            f32, bf16 = jnp.float32, jnp.bfloat16
            vmem = pltpu.VMEM
            return pl.pallas_call(
                functools.partial(kernel, width),
                out_shape=jax.ShapeDtypeStruct((n_part, nf), f32),
                in_specs=[pl.BlockSpec(memory_space=pl.ANY)] + [pl.BlockSpec(memory_space=pltpu.VMEM)] * 3,
                out_specs=pl.BlockSpec(memory_space=pl.ANY),
                scratch_shapes=[
                    vmem((n_part, nf), f32),
                    vmem((n_part, 2 * nf), bf16),
                    vmem((n_part, nf), bf16),
                    vmem((n_part, n_part), bf16),
                    vmem((2, 2, CH, B, B), bf16),
                    vmem((2, 2, 5, B, B), bf16),
                    vmem((2, CH, B, B), f32),
                    vmem((2, 5, B, B), f32),
                    vmem((2, CH, B, B), f32),
                    vmem((2, 5, B, B), f32),
                    vmem((5, B, B), f32),
                    vmem((2, B, B), f32),
                    vmem((B, B), f32),
                    vmem((2, 2, 32, B), f32),
                    vmem((2, 2, 32, B), f32),
                    vmem((32, B), f32),
                    vmem((2, 4, 32, B), bf16),
                    vmem((8, nf + B), f32),
                    vmem((8, nf + B), f32),
                    vmem((16, B), f32),
                    vmem((16, 16, B), f32),
                    vmem((16, B), f32),
                    vmem((16, B), f32),
                    vmem((8, 16, B), f32),
                    vmem((16, B), f32),
                    dma((UP,)), dma((UP,)), dma((UP,)), dma((UP,)), dma, dma, dma((8,)), dma((16,)), dma((16,)), dma((8,)),
                    dma((2, CH)), dma((2, CH)), dma((2, 5)), dma((2, 5)), dma((5,)), dma((5,)),
                    dma((2, CH)), dma((2, CH)), dma((5,)), dma((5,)), dma((2, 5)), dma((2, 5)),
                    dma((2, CH)), dma((2, CH)), dma((2, 5)), dma((2, 5)),
                    dma((2, 2)), dma((2, 2)), dma, dma, dma, dma, dma((2, 2)), dma((2, 2)), dma((2, 2)), dma((2, 2)),
                ],
                compiler_params=pltpu.CompilerParams(
                    collective_id=0, has_side_effects=True, vmem_limit_bytes=56 * 1024 * 1024
                ),
                name="svgd",
            )(current, prec_loc.reshape(nf // B, B), mean_loc.reshape(nf // B, B), fac_loc.T)

        sharded = jax.shard_map(
            local_steps,
            mesh=mesh,
            in_specs=(P("ens", FEAT_AXES), P(LEAD_AXES), P(LEAD_AXES), P(LEAD_AXES, None)),
            out_specs=P("ens", FEAT_AXES),
            check_vma=False,
        )
        return sharded(particles, prec_diag, mean_vec, low_rank)

    return run_steps
```

```python
import functools

import jax
import jax.numpy as jnp
from jax import lax
from jax.experimental import pallas as pl
from jax.experimental.pallas import tpu as pltpu
from jax.sharding import PartitionSpec as P

NUM_STEPS = 3
BAND_SCALE = 4.0
STEP_SCALE = 0.4
FEAT_AXES = ("slab", "feat")
LEAD_AXES = ("ens", "slab", "feat")
MESH = pl.DeviceIdType.MESH

B = 128
ROW = 256
UP = 6
START = 2
LAG = 3
END = 2
OUT1 = 2
LAG2 = 3
OUT2 = 2
DIE = 2
YF0 = 3
FIN0 = START + 3 * LAG + END
AG0 = FIN0 + OUT1
CH = 15
PM = 6
DRV0 = AG0 + 3 * LAG2 + PM + 1 + DIE + 1
ITERS = AG0 + 3 * LAG2 + CH + OUT2 + DIE
assert YF0 + 10 <= FIN0 and FIN0 + CH <= DRV0 and DRV0 + UP <= ITERS


def _ref(k, t, d, ey, c):
    f = lax.div(k, 4)
    return k * 16 + (1 - f) * (t * 8 + d * 4 + ey * 2 + c) + f * (t * 4 + d * 2 + ey)


def _block(n):
    p = lax.div(n + 126, B) + lax.div(n + 120, B) + lax.div(n + 110, B) + lax.div(n + 96, B) + lax.div(n + 78, B)
    r = n - 2 * p * p
    i = lax.div(r, 2)
    j = 2 * p + lax.rem(r, 2)
    return i, j, p, 1 - jnp.minimum(j - i, 1)


def _clip(i, n):
    return jnp.minimum(jnp.maximum(i, 0), n - 1)


def _span(i):
    return pl.ds(pl.multiple_of(i * B, B), B)


def kernel(width, x_hbm, lam_in, mu_in, ut_ref, o_hbm, theta, th, a_ref, kf, kc, ko, gsrc, gy, zrecv, yrecv, yend, pmb, pmrecv,
           ps, pzr, pye, pmf, lam_ref, mu_ref,
           dsrc, dgather, dsum, sacc, sgather, ssum, ld, od, thd_s, thd_r, pm_s, pm_r, dg_s, dg_r, sg_s, sg_r,
           zs, zr, ys, yr, ye_s, ye_r, kz_s, kz_r, kyz_s, kyz_r, ky_s, ky_r, kd_s, kd_r, ke_s, ke_r,
           pz_s, pz_r, pye_s, pye_r, pky_s, pky_r, pkz_s, pkz_r, pkd_s, pkd_r):
    nf = theta.shape[1]
    n_part = theta.shape[0]
    bandwidth = BAND_SCALE * width
    step_size = STEP_SCALE * width
    rep = 2.0 / bandwidth
    f32, bf16 = jnp.float32, jnp.bfloat16
    ens = lax.axis_index("ens")
    z = lax.axis_index("slab")
    feat = lax.axis_index("feat")
    y = lax.div(feat, 2)
    c = lax.rem(feat, 2)
    me = z * 4 + feat
    ypart = (ens, z, (1 - y) * 2 + c)
    dpart = (ens, z, y * 2 + 1 - c)
    dc = lax.div(z, 3)
    corner = lax.rem(z, 3) == 0
    own8 = (dc * 2 + y) * 2 + c
    rounds = 4 + c
    chain = 3 * rounds
    other_chain = 27 - chain

    def rcopy(src, dst, s, r, dev):
        return pltpu.make_async_remote_copy(src_ref=src, dst_ref=dst, send_sem=s, recv_sem=r, device_id=dev, device_id_type=MESH)

    def zdev(dz):
        return (ens, z + dz, feat)

    def place(i, cc):
        zf = 8 + 2 * cc
        w = _clip(i - zf + 1, 2)
        h = lax.div(i, 2)
        return w, h + w * (i - zf - h), i - 2 * h

    def num_chain(i, d, cc):
        w, k, e = place(i, cc)
        return _ref(k, w, d, (1 - w) * e + w * y, cc)

    def panel(p):
        return pl.ds(pl.multiple_of(p * ROW, ROW), ROW)

    def load_copy(p):
        return pltpu.make_async_copy(x_hbm.at[panel(p)], theta.at[panel(p)], ld.at[p])

    def out_copy(p):
        return pltpu.make_async_copy(theta.at[panel(p)], o_hbm.at[panel(p)], od.at[p])

    def th_copy(p):
        return rcopy(th.at[panel(p), pl.ds(0, nf)], th.at[panel(p), pl.ds(nf, nf)], thd_s.at[p], thd_r.at[p], dpart)

    def pm_copy():
        return rcopy(pmb.at[1 - c], pmrecv, pm_s, pm_r, dpart)

    def dg_copy(e):
        return rcopy(dsrc, dgather.at[me], dg_s.at[e], dg_r.at[me], (ens, (e // 4) * 3, e % 4))

    def dg_local():
        return pltpu.make_async_copy(dsrc, dgather.at[me], dg_r.at[me])

    def sg_copy(e):
        return rcopy(sacc, sgather.at[own8], sg_s.at[e], sg_r.at[own8], (ens, e // 4, e % 4))

    def sg_local():
        return pltpu.make_async_copy(sacc, sgather.at[own8], sg_r.at[own8])

    def z_copy(d, i):
        return rcopy(gsrc.at[d, i], zrecv.at[d, i], zs.at[d, i], zr.at[d, i], zdev(2 * d - 1))

    def y_copy(d, k):
        return rcopy(gy.at[d, k], yrecv.at[d, k], ys.at[d, k], yr.at[d, k], ypart)

    def ye_copy(k, i):
        return rcopy(gsrc.at[dc, i], yend.at[k], ye_s.at[k], ye_r.at[k], ypart)

    def kc_copy(d, i, cc, s, r, dev):
        return rcopy(kc.at[cc, d, i], kc.at[cc, d, i], s, r, dev)

    def ko_copy(d, k, cc, s, r, dev):
        return rcopy(ko.at[cc, d, k], ko.at[cc, d, k], s, r, dev)

    def kz_copy(d, i):
        return kc_copy(d, i, c, kz_s.at[d, i], kz_r.at[d, i], zdev(1 - 2 * d))

    def kyz_copy(k, i):
        return kc_copy(dc, i, c, kyz_s.at[k], kyz_r.at[k], ypart)

    def ky_copy(d, k, i):
        return rcopy(kc.at[c, d, i], ko.at[c, d, k], ky_s.at[d, k], ky_r.at[d, k], ypart)

    def kd_copy(d, i, cc):
        return kc_copy(d, i, cc, kd_s.at[d, i], kd_r.at[d, i], dpart)

    def ke_copy(d, k, cc):
        return ko_copy(d, k, cc, ke_s.at[d, k], ke_r.at[d, k], dpart)

    def pz_copy(d, e):
        return rcopy(ps.at[d, e], pzr.at[d, e], pz_s.at[d, e], pz_r.at[d, e], zdev(2 * d - 1))

    def pye_copy(e):
        return rcopy(ps.at[dc, e], pye, pye_s, pye_r, ypart)

    def pf_copy(d, e, cc, s, r, dev):
        return rcopy(pmf.at[cc, 2 * d + e], pmf.at[cc, 2 * d + e], s, r, dev)

    def pky_copy(e):
        return pf_copy(dc, e, c, pky_s, pky_r, ypart)

    def pkz_copy(d, e):
        return pf_copy(d, e, c, pkz_s.at[d, e], pkz_r.at[d, e], zdev(1 - 2 * d))

    def pkd_copy(d, e, cc):
        return pf_copy(d, e, cc, pkd_s.at[d, e], pkd_r.at[d, e], dpart)

    def low_tri():
        return lax.broadcasted_iota(jnp.int32, (B, B), 0) - lax.broadcasted_iota(jnp.int32, (B, B), 1)

    def unpack(kk):
        kt = kk.T
        tri = low_tri()
        return jnp.where(tri >= 0, kk, kt), jnp.where(tri < 0, kk, jnp.where(tri == 0, 1.0, kt))

    def settle(src, n):
        i, j, p, e = _block(n)

        @pl.when(e == 0)
        def _():
            blk = src[...]
            kf[_span(i), _span(j)] = blk
            kf[_span(j), _span(i)] = blk.T

        @pl.when(e == 1)
        def _():
            first, second = unpack(src[...].astype(f32))
            kf[_span(2 * p), _span(2 * p)] = first.astype(bf16)
            kf[_span(2 * p + 1), _span(2 * p + 1)] = second.astype(bf16)

    def dot_t(i, j):
        return lax.dot_general(th[_span(i), :], th[_span(j), :], (((1,), (1,)), ((), ())), preferred_element_type=f32)

    def gram(dst, n):
        i, j, p, e = _block(n)
        dst[...] = dot_t(i, j)

        @pl.when(e == 1)
        def _():
            dst[...] = jnp.where(low_tri() >= 0, dst[...], dot_t(2 * p + 1, 2 * p + 1))

    def post(p):
        new = theta[panel(p), :]
        tb = new.astype(bf16)
        th[panel(p), pl.ds(0, nf)] = tb
        xb = (new - mu_ref[0:1, 0:nf]).astype(bf16)
        pm = lax.dot_general(ut_ref[...], xb, (((1,), (1,)), ((), ())), preferred_element_type=f32)
        th_copy(p).start()
        half = lax.div(p, 3)
        for h in range(2):
            q = lax.rem(p, 3) * 2 + h
            pmb[half, pl.ds(pl.multiple_of(q * 16, 16), 16), :] = pm[:, h * B:(h + 1) * B]
            t = tb[h * B:(h + 1) * B, :].astype(f32)
            sq = t * t
            tot = sq[:, 0:B]
            for m in range(1, nf // B):
                tot = tot + sq[:, m * B:(m + 1) * B]
            dsrc[pl.ds(p * 2 + h, 1), :] = jnp.sum(tot.T, axis=0, keepdims=True)

    def row_sums():
        tot = jnp.zeros((16, B), f32)
        for e in range(8):
            pltpu.make_async_copy(sacc, sgather.at[e], sg_r.at[e]).wait()
            tot = tot + sgather[e]
        ssum[...] = tot

    def update(p):
        acc = jnp.dot(kf[panel(p), :], a_ref[...], preferred_element_type=f32)
        cur = theta[panel(p), :]
        col = jnp.concatenate(
            [jnp.broadcast_to(ssum[pl.ds(p * 2 + h, 1), :], (B, B)).T[:, 0:1] for h in range(2)], axis=0
        )
        phi = (acc + (rep * col) * cur) * (1.0 / n_part)
        theta[panel(p), :] = cur + step_size * phi

    barrier = pltpu.get_barrier_semaphore()
    for o in range(1, 16):
        e = lax.rem(me + o, 16)
        pl.semaphore_signal(barrier, inc=1, device_id=(ens, lax.div(e, 4), lax.rem(e, 4)), device_id_type=MESH)
    for p in range(UP):
        load_copy(p).start()
    pmb[...] = jnp.zeros_like(pmb)
    dsrc[...] = jnp.zeros_like(dsrc)
    for m in range(nf // B):
        lam_ref[0:1, m * B:(m + 1) * B] = lam_in[m:m + 1, :]
        mu_ref[0:1, m * B:(m + 1) * B] = mu_in[m:m + 1, :]
    pl.semaphore_wait(barrier, 15)

    @pl.loop(0, NUM_STEPS)
    def _(step):
        @pl.when(step > 0)
        def _():
            row_sums()

        sacc[...] = jnp.zeros_like(sacc)

        def renew(g):
            gp = jnp.minimum(g, UP - 1)

            @pl.when(g < UP)
            def _():
                @pl.when(step == 0)
                def _():
                    load_copy(gp).wait()

                @pl.when(step > 0)
                def _():
                    update(gp)

                post(gp)

            @pl.when(g == UP - 1)
            def _():
                for e in range(8):
                    mine = me == (e // 4) * 12 + e % 4

                    @pl.when(mine)
                    def _():
                        dg_local().start()

                    @pl.when(jnp.logical_not(mine))
                    def _():
                        dg_copy(e).start()

                pm_copy().start()

            @pl.when((g >= 1) & (g <= UP))
            def _():
                th_copy(_clip(g - 1, UP)).wait()

        def sums(g, yf):
            if yf:
                @pl.when(g == START + PM)
                def _():
                    pm_copy().wait()

            v = g - YF0
            v_on = (v >= 0) & (v < 2 * rounds)
            v = _clip(v, 2 * rounds)
            vk = lax.div(v, 2)
            vd = v - 2 * vk

            if yf:
                @pl.when(v_on)
                def _():
                    gram(gy.at[vd, vk], _ref(vk, 1, vd, 1 - y, c))

            state = []
            for d in range(2):
                pos = z if d else 3 - z
                i = g - START - LAG * pos
                on = (i >= 0) & (i < chain)
                i = _clip(i, chain)
                w, k, e = place(i, c)
                state.append((pos, on, i, w, k, e))

            def send_sum(d):
                pos, on, i, w, k, e = state[d]

                @pl.when(on)
                def _():
                    rides = (i >= PM) & (i < PM + 2)

                    @pl.when(pos < 3)
                    def _():
                        @pl.when(rides)
                        def _():
                            pz_copy(d, e).start()

                        z_copy(d, i).start()

                    @pl.when((pos == 3) & (w == 0) & (e != y))
                    def _():
                        @pl.when(rides)
                        def _():
                            pye_copy(e).start()

                        ye_copy(k, i).start()

            for d in range(2):
                pos, on, i, w, k, e = state[d]

                @pl.when(on)
                def _():
                    gram(gsrc.at[d, i], _ref(k, w, d, e + w * (y - e), c))

                if d == 0 and yf:
                    @pl.when(v_on)
                    def _():
                        y_copy(vd, vk).start()

                if d == 1:
                    send_sum(0)

                @pl.when(on)
                def _():
                    @pl.when(w == 1)
                    def _():
                        y_copy(d, k).wait_recv()
                        gsrc[d, i] = gsrc[d, i] + yrecv[d, k]

                    @pl.when((i >= PM) & (i < PM + 2))
                    def _():
                        rows = pl.ds(pl.multiple_of((2 * d + e) * 32, 32), 32)
                        ps[d, e] = pmb[c, rows, :] + pmrecv[rows, :]

                        @pl.when(pos > 0)
                        def _():
                            pz_copy(d, e).wait_recv()
                            ps[d, e] = ps[d, e] + pzr[d, e]

                    @pl.when(pos > 0)
                    def _():
                        z_copy(d, i).wait_recv()
                        gsrc[d, i] = gsrc[d, i] + zrecv[d, i]

            if yf:
                send_sum(1)
                return

            i = g - FIN0
            on = corner & (i >= 0) & (i < chain)
            i = _clip(i, chain)
            w, k, e = place(i, c)

            @pl.when(on & (i == 0))
            def _():
                tot = jnp.zeros((16, B), f32)
                for o in range(16):
                    pltpu.make_async_copy(dsrc, dgather.at[o], dg_r.at[o]).wait()
                    tot = tot + dgather[o]
                dsum[...] = tot

            @pl.when(on & ((w == 1) | (e == y)))
            def _():
                @pl.when(w == 0)
                def _():
                    ye_copy(k, i).wait_recv()
                    gsrc[dc, i] = gsrc[dc, i] + yend[k]

                bi, bj, bp, be = _block(_ref(k, w, dc, y, c))

                def kern(gi, gj):
                    sq = jnp.maximum(gi + gj - 2.0 * gsrc[dc, i], 0.0)
                    return jnp.exp(sq * (-1.0 / bandwidth))

                def add_sums(q, blk):
                    sacc[pl.ds(q, 1), :] = sacc[pl.ds(q, 1), :] + jnp.sum(blk, axis=0, keepdims=True)

                @pl.when(be == 0)
                def _():
                    kk = kern(jnp.broadcast_to(dsum[pl.ds(bi, 1), :], (B, B)).T, dsum[pl.ds(bj, 1), :])
                    kc[c, dc, i] = kk.astype(bf16)
                    add_sums(bj, kk)
                    add_sums(bi, kk.T)

                @pl.when(be == 1)
                def _():
                    tri = low_tri() >= 0
                    ga = jnp.broadcast_to(dsum[pl.ds(2 * bp, 1), :], (B, B))
                    gb = jnp.broadcast_to(dsum[pl.ds(2 * bp + 1, 1), :], (B, B))
                    kk = kern(jnp.where(tri, ga.T, gb.T), jnp.where(tri, ga, gb))
                    kk = jnp.where(low_tri() == 0, 1.0, kk)
                    kc[c, dc, i] = kk.astype(bf16)
                    first, second = unpack(kk)
                    add_sums(2 * bp, first)
                    add_sums(2 * bp + 1, second)

                @pl.when((i >= PM) & (i < PM + 2))
                def _():
                    pye_copy(e).wait_recv()
                    pmf[c, 2 * dc + e] = (ps[dc, e] + pye[...]).astype(bf16)

            send_sum(1)

            @pl.when(on & ((w == 1) | (e == y)))
            def _():
                @pl.when((i >= PM) & (i < PM + 2))
                def _():
                    pky_copy(e).start()

                @pl.when(w == 0)
                def _():
                    kyz_copy(k, i).start()

                @pl.when(w == 1)
                def _():
                    ky_copy(dc, k, i).start()

            @pl.when(on & (i == chain - 1))
            def _():
                for o in range(16):
                    @pl.when(me == o)
                    def _():
                        sg_local().start()

                    @pl.when(me != o)
                    def _():
                        sg_copy(o).start()

        def spread(g):
            heard = []
            for d in range(2):
                dist = 3 - z if d else z
                h = g - AG0 - LAG2 * dist
                on = (h >= 0) & (h < chain)
                i = _clip(h, chain)
                heard.append((h, on, i))

                @pl.when(on)
                def _():
                    w, k, e = place(i, c)
                    turn = (dist == 0) & (w == 0) & (e != y)

                    @pl.when((i >= PM) & (i < PM + 2))
                    def _():
                        @pl.when(turn)
                        def _():
                            pky_copy(1 - y).wait_recv()

                        @pl.when(dist > 0)
                        def _():
                            pkz_copy(d, e).wait_recv()

                        @pl.when(dist < 3)
                        def _():
                            pkz_copy(d, e).start()

                        pkd_copy(d, e, c).start()

                    @pl.when(turn)
                    def _():
                        kyz_copy(k, i).wait_recv()

                    @pl.when(dist > 0)
                    def _():
                        kz_copy(d, i).wait_recv()

                        @pl.when(w == 1)
                        def _():
                            ky_copy(d, k, i).start()

                    @pl.when(dist < 3)
                    def _():
                        kz_copy(d, i).start()

                    kd_copy(d, i, c).start()

                k = h - OUT2 - 2 * rounds

                @pl.when((k >= 0) & (k < rounds))
                def _():
                    kk = _clip(k, rounds)
                    ky_copy(d, kk, 0).wait_recv()
                    ke_copy(d, kk, c).start()

            for d in range(2):
                h, on, i = heard[d]

                @pl.when(on)
                def _():
                    settle(kc.at[c, d, i], num_chain(i, d, c))

                k = h - OUT2 - 2 * rounds

                @pl.when((k >= 0) & (k < rounds))
                def _():
                    kk = _clip(k, rounds)
                    settle(ko.at[c, d, kk], _ref(kk, 1, d, 1 - y, c))

                j = h - DIE

                @pl.when((j >= 0) & (j < other_chain))
                def _():
                    jj = _clip(j, other_chain)

                    @pl.when((jj >= PM) & (jj < PM + 2))
                    def _():
                        pkd_copy(d, jj - 2 * lax.div(jj, 2), 1 - c).wait_recv()

                    kd_copy(d, jj, 1 - c).wait_recv()
                    settle(kc.at[1 - c, d, jj], num_chain(jj, d, 1 - c))

                m = h - OUT2 - DIE - 2 * (9 - rounds)

                @pl.when((m >= 0) & (m < 9 - rounds))
                def _():
                    mm = _clip(m, 9 - rounds)
                    ke_copy(d, mm, 1 - c).wait_recv()
                    settle(ko.at[1 - c, d, mm], _ref(mm, 1, d, 1 - y, 1 - c))

        def drive(g):
            p = g - DRV0
            on = (p >= 0) & (p < UP)
            p = _clip(p, UP)

            @pl.when(on)
            def _():
                q = lax.rem(p, 3) * 2
                half = lax.div(p, 3)
                pmt = jnp.concatenate(
                    [pmf[half, lax.div(q, 2), pl.ds(16 * h, 16), :] for h in range(2)], axis=1
                )
                low = lax.dot_general(
                    pmt.astype(f32).T.astype(bf16), ut_ref[...], (((1,), (0,)), ((), ())), preferred_element_type=f32
                )
                cur = theta[panel(p), :]
                grad = -((cur - mu_ref[0:1, 0:nf]) * lam_ref[0:1, 0:nf] + low)
                a_ref[panel(p), :] = (grad - rep * cur).astype(bf16)

        @pl.loop(0, UP + 1)
        def _(g):
            renew(g)
            sums(g, True)

        @pl.loop(UP + 1, FIN0)
        def _(g):
            sums(g, True)

        @pl.loop(FIN0, FIN0 + CH)
        def _(g):
            sums(g, False)
            spread(g)

        @pl.loop(FIN0 + CH, ITERS)
        def _(g):
            spread(g)
            drive(g)

        for e in range(8):
            @pl.when(me != (e // 4) * 12 + e % 4)
            def _():
                dg_copy(e).wait_send()

        for d in range(2):
            pos = z if d else 3 - z
            for e in range(2):
                @pl.when(pos < 3)
                def _():
                    pz_copy(d, e).wait_send()

                @pl.when(pos > 0)
                def _():
                    pkz_copy(d, e).wait_send()

                pkd_copy(d, e, c).wait_send()

        @pl.when(corner)
        def _():
            pye_copy(1 - y).wait_send()
            pky_copy(y).wait_send()

        @pl.loop(0, rounds)
        def _(k):
            for d in range(2):
                y_copy(d, k).wait_send()
                ke_copy(d, k, c).wait_send()
                ky_copy(d, k, 0).wait_send()

            @pl.when(corner)
            def _():
                ye_copy(k, 2 * k + 1 - y).wait_send()
                kyz_copy(k, 0).wait_send()

        @pl.loop(0, chain)
        def _(i):
            for d in range(2):
                pos = z if d else 3 - z

                @pl.when(pos < 3)
                def _():
                    z_copy(d, i).wait_send()

                @pl.when(pos > 0)
                def _():
                    kz_copy(d, i).wait_send()

                kd_copy(d, i, c).wait_send()

        @pl.when(corner)
        def _():
            for e in range(16):
                @pl.when(me != e)
                def _():
                    sg_copy(e).wait_send()

    row_sums()

    @pl.loop(0, UP)
    def _(p):
        update(p)
        out_copy(p).start()

    @pl.loop(0, UP)
    def _(p):
        out_copy(p).wait()


def solution(mesh):
    def run_steps(particles, prec_diag, mean_vec, low_rank):
        width = particles.shape[1]

        def local_steps(current, prec_loc, mean_loc, fac_loc):
            n_part, nf = current.shape
            dma = pltpu.SemaphoreType.DMA
            f32, bf16 = jnp.float32, jnp.bfloat16
            vmem = pltpu.VMEM
            return pl.pallas_call(
                functools.partial(kernel, width),
                out_shape=jax.ShapeDtypeStruct((n_part, nf), f32),
                in_specs=[pl.BlockSpec(memory_space=pl.ANY)] + [pl.BlockSpec(memory_space=pltpu.VMEM)] * 3,
                out_specs=pl.BlockSpec(memory_space=pl.ANY),
                scratch_shapes=[
                    vmem((n_part, nf), f32),
                    vmem((n_part, 2 * nf), bf16),
                    vmem((n_part, nf), bf16),
                    vmem((n_part, n_part), bf16),
                    vmem((2, 2, CH, B, B), bf16),
                    vmem((2, 2, 5, B, B), bf16),
                    vmem((2, CH, B, B), f32),
                    vmem((2, 5, B, B), f32),
                    vmem((2, CH, B, B), f32),
                    vmem((2, 5, B, B), f32),
                    vmem((5, B, B), f32),
                    vmem((2, B, B), f32),
                    vmem((B, B), f32),
                    vmem((2, 2, 32, B), f32),
                    vmem((2, 2, 32, B), f32),
                    vmem((32, B), f32),
                    vmem((2, 4, 32, B), bf16),
                    vmem((8, nf + B), f32),
                    vmem((8, nf + B), f32),
                    vmem((16, B), f32),
                    vmem((16, 16, B), f32),
                    vmem((16, B), f32),
                    vmem((16, B), f32),
                    vmem((8, 16, B), f32),
                    vmem((16, B), f32),
                    dma((UP,)), dma((UP,)), dma((UP,)), dma((UP,)), dma, dma, dma((8,)), dma((16,)), dma((16,)), dma((8,)),
                    dma((2, CH)), dma((2, CH)), dma((2, 5)), dma((2, 5)), dma((5,)), dma((5,)),
                    dma((2, CH)), dma((2, CH)), dma((5,)), dma((5,)), dma((2, 5)), dma((2, 5)),
                    dma((2, CH)), dma((2, CH)), dma((2, 5)), dma((2, 5)),
                    dma((2, 2)), dma((2, 2)), dma, dma, dma, dma, dma((2, 2)), dma((2, 2)), dma((2, 2)), dma((2, 2)),
                ],
                compiler_params=pltpu.CompilerParams(
                    collective_id=0, has_side_effects=True, vmem_limit_bytes=56 * 1024 * 1024
                ),
                name="svgd",
            )(current, prec_loc.reshape(nf // B, B), mean_loc.reshape(nf // B, B), fac_loc.T)

        sharded = jax.shard_map(
            local_steps,
            mesh=mesh,
            in_specs=(P("ens", FEAT_AXES), P(LEAD_AXES), P(LEAD_AXES), P(LEAD_AXES, None)),
            out_specs=P("ens", FEAT_AXES),
            check_vma=False,
        )
        return sharded(particles, prec_diag, mean_vec, low_rank)

    return run_steps
```

```python
import functools

import jax
import jax.numpy as jnp
from jax import lax
from jax.experimental import pallas as pl
from jax.experimental.pallas import tpu as pltpu
from jax.sharding import PartitionSpec as P

NUM_STEPS = 3
BAND_SCALE = 4.0
STEP_SCALE = 0.4
FEAT_AXES = ("slab", "feat")
LEAD_AXES = ("ens", "slab", "feat")
MESH = pl.DeviceIdType.MESH

B = 128
ROW = 256
UP = 6
START = 2
LAG = 3
END = 2
OUT1 = 2
LAG2 = 3
OUT2 = 3
DIE = 3
YF0 = 3
FIN0 = START + 3 * LAG + END
AG0 = FIN0 + OUT1
CH = 15
PM = 6
DRV0 = AG0 + 3 * LAG2 + PM + 1 + DIE + 1
ITERS = AG0 + 3 * LAG2 + CH + OUT2 + DIE
assert YF0 + 10 <= FIN0 and FIN0 + CH <= DRV0 and DRV0 + UP <= ITERS


def _ref(k, t, d, ey, c):
    f = lax.div(k, 4)
    return k * 16 + (1 - f) * (t * 8 + d * 4 + ey * 2 + c) + f * (t * 4 + d * 2 + ey)


def _block(n):
    p = lax.div(n + 126, B) + lax.div(n + 120, B) + lax.div(n + 110, B) + lax.div(n + 96, B) + lax.div(n + 78, B)
    r = n - 2 * p * p
    i = lax.div(r, 2)
    j = 2 * p + lax.rem(r, 2)
    return i, j, p, 1 - jnp.minimum(j - i, 1)


def _clip(i, n):
    return jnp.minimum(jnp.maximum(i, 0), n - 1)


def _span(i):
    return pl.ds(pl.multiple_of(i * B, B), B)


def kernel(width, x_hbm, lam_in, mu_in, ut_ref, o_hbm, theta, th, a_ref, kf, kc, ko, gsrc, gy, zrecv, yrecv, yend, pmb, pmrecv,
           ps, pzr, pye, pmf, lam_ref, mu_ref,
           dsrc, dgather, dsum, sacc, sgather, ssum, ld, od, thd_s, thd_r, pm_s, pm_r, dg_s, dg_r, sg_s, sg_r,
           zs, zr, ys, yr, ye_s, ye_r, kz_s, kz_r, kyz_s, kyz_r, ky_s, ky_r, kd_s, kd_r, ke_s, ke_r,
           pz_s, pz_r, pye_s, pye_r, pky_s, pky_r, pkz_s, pkz_r, pkd_s, pkd_r):
    nf = theta.shape[1]
    n_part = theta.shape[0]
    bandwidth = BAND_SCALE * width
    step_size = STEP_SCALE * width
    rep = 2.0 / bandwidth
    f32, bf16 = jnp.float32, jnp.bfloat16
    ens = lax.axis_index("ens")
    z = lax.axis_index("slab")
    feat = lax.axis_index("feat")
    y = lax.div(feat, 2)
    c = lax.rem(feat, 2)
    me = z * 4 + feat
    ypart = (ens, z, (1 - y) * 2 + c)
    dpart = (ens, z, y * 2 + 1 - c)
    dc = lax.div(z, 3)
    corner = lax.rem(z, 3) == 0
    own8 = (dc * 2 + y) * 2 + c
    rounds = 4 + c
    chain = 3 * rounds
    other_chain = 27 - chain

    def rcopy(src, dst, s, r, dev):
        return pltpu.make_async_remote_copy(src_ref=src, dst_ref=dst, send_sem=s, recv_sem=r, device_id=dev, device_id_type=MESH)

    def zdev(dz):
        return (ens, z + dz, feat)

    def place(i, cc):
        zf = 8 + 2 * cc
        w = _clip(i - zf + 1, 2)
        h = lax.div(i, 2)
        return w, h + w * (i - zf - h), i - 2 * h

    def num_chain(i, d, cc):
        w, k, e = place(i, cc)
        return _ref(k, w, d, (1 - w) * e + w * y, cc)

    def panel(p):
        return pl.ds(pl.multiple_of(p * ROW, ROW), ROW)

    def load_copy(p):
        return pltpu.make_async_copy(x_hbm.at[panel(p)], theta.at[panel(p)], ld.at[p])

    def out_copy(p):
        return pltpu.make_async_copy(theta.at[panel(p)], o_hbm.at[panel(p)], od.at[p])

    def th_copy(p):
        return rcopy(th.at[panel(p), pl.ds(0, nf)], th.at[panel(p), pl.ds(nf, nf)], thd_s.at[p], thd_r.at[p], dpart)

    def pm_copy():
        return rcopy(pmb.at[1 - c], pmrecv, pm_s, pm_r, dpart)

    def dg_copy(e):
        return rcopy(dsrc, dgather.at[me], dg_s.at[e], dg_r.at[me], (ens, (e // 4) * 3, e % 4))

    def dg_local():
        return pltpu.make_async_copy(dsrc, dgather.at[me], dg_r.at[me])

    def sg_copy(e):
        return rcopy(sacc, sgather.at[own8], sg_s.at[e], sg_r.at[own8], (ens, e // 4, e % 4))

    def sg_local():
        return pltpu.make_async_copy(sacc, sgather.at[own8], sg_r.at[own8])

    def z_copy(d, i):
        return rcopy(gsrc.at[d, i], zrecv.at[d, i], zs.at[d, i], zr.at[d, i], zdev(2 * d - 1))

    def y_copy(d, k):
        return rcopy(gy.at[d, k], yrecv.at[d, k], ys.at[d, k], yr.at[d, k], ypart)

    def ye_copy(k, i):
        return rcopy(gsrc.at[dc, i], yend.at[k], ye_s.at[k], ye_r.at[k], ypart)

    def kc_copy(d, i, cc, s, r, dev):
        return rcopy(kc.at[cc, d, i], kc.at[cc, d, i], s, r, dev)

    def ko_copy(d, k, cc, s, r, dev):
        return rcopy(ko.at[cc, d, k], ko.at[cc, d, k], s, r, dev)

    def kz_copy(d, i):
        return kc_copy(d, i, c, kz_s.at[d, i], kz_r.at[d, i], zdev(1 - 2 * d))

    def kyz_copy(k, i):
        return kc_copy(dc, i, c, kyz_s.at[k], kyz_r.at[k], ypart)

    def ky_copy(d, k, i):
        return rcopy(kc.at[c, d, i], ko.at[c, d, k], ky_s.at[d, k], ky_r.at[d, k], ypart)

    def kd_copy(d, i, cc):
        return kc_copy(d, i, cc, kd_s.at[d, i], kd_r.at[d, i], dpart)

    def ke_copy(d, k, cc):
        return ko_copy(d, k, cc, ke_s.at[d, k], ke_r.at[d, k], dpart)

    def pz_copy(d, e):
        return rcopy(ps.at[d, e], pzr.at[d, e], pz_s.at[d, e], pz_r.at[d, e], zdev(2 * d - 1))

    def pye_copy(e):
        return rcopy(ps.at[dc, e], pye, pye_s, pye_r, ypart)

    def pf_copy(d, e, cc, s, r, dev):
        return rcopy(pmf.at[cc, 2 * d + e], pmf.at[cc, 2 * d + e], s, r, dev)

    def pky_copy(e):
        return pf_copy(dc, e, c, pky_s, pky_r, ypart)

    def pkz_copy(d, e):
        return pf_copy(d, e, c, pkz_s.at[d, e], pkz_r.at[d, e], zdev(1 - 2 * d))

    def pkd_copy(d, e, cc):
        return pf_copy(d, e, cc, pkd_s.at[d, e], pkd_r.at[d, e], dpart)

    def low_tri():
        return lax.broadcasted_iota(jnp.int32, (B, B), 0) - lax.broadcasted_iota(jnp.int32, (B, B), 1)

    def unpack(kk):
        kt = kk.T
        tri = low_tri()
        return jnp.where(tri >= 0, kk, kt), jnp.where(tri < 0, kk, jnp.where(tri == 0, 1.0, kt))

    def settle(src, n):
        i, j, p, e = _block(n)

        @pl.when(e == 0)
        def _():
            blk = src[...]
            kf[_span(i), _span(j)] = blk
            kf[_span(j), _span(i)] = blk.T

        @pl.when(e == 1)
        def _():
            first, second = unpack(src[...].astype(f32))
            kf[_span(2 * p), _span(2 * p)] = first.astype(bf16)
            kf[_span(2 * p + 1), _span(2 * p + 1)] = second.astype(bf16)

    def dot_t(i, j):
        return lax.dot_general(th[_span(i), :], th[_span(j), :], (((1,), (1,)), ((), ())), preferred_element_type=f32)

    def gram(dst, n):
        i, j, p, e = _block(n)
        dst[...] = dot_t(i, j)

        @pl.when(e == 1)
        def _():
            dst[...] = jnp.where(low_tri() >= 0, dst[...], dot_t(2 * p + 1, 2 * p + 1))

    def post(p):
        new = theta[panel(p), :]
        tb = new.astype(bf16)
        th[panel(p), pl.ds(0, nf)] = tb
        xb = (new - mu_ref[0:1, 0:nf]).astype(bf16)
        pm = lax.dot_general(ut_ref[...], xb, (((1,), (1,)), ((), ())), preferred_element_type=f32)
        th_copy(p).start()
        half = lax.div(p, 3)
        for h in range(2):
            q = lax.rem(p, 3) * 2 + h
            pmb[half, pl.ds(pl.multiple_of(q * 16, 16), 16), :] = pm[:, h * B:(h + 1) * B]
            t = tb[h * B:(h + 1) * B, :].astype(f32)
            sq = t * t
            tot = sq[:, 0:B]
            for m in range(1, nf // B):
                tot = tot + sq[:, m * B:(m + 1) * B]
            dsrc[pl.ds(p * 2 + h, 1), :] = jnp.sum(tot.T, axis=0, keepdims=True)

    def row_sums():
        tot = jnp.zeros((16, B), f32)
        for e in range(8):
            pltpu.make_async_copy(sacc, sgather.at[e], sg_r.at[e]).wait()
            tot = tot + sgather[e]
        ssum[...] = tot

    def update(p):
        acc = jnp.dot(kf[panel(p), :], a_ref[...], preferred_element_type=f32)
        cur = theta[panel(p), :]
        col = jnp.concatenate(
            [jnp.broadcast_to(ssum[pl.ds(p * 2 + h, 1), :], (B, B)).T[:, 0:1] for h in range(2)], axis=0
        )
        phi = (acc + (rep * col) * cur) * (1.0 / n_part)
        theta[panel(p), :] = cur + step_size * phi

    barrier = pltpu.get_barrier_semaphore()
    for o in range(1, 16):
        e = lax.rem(me + o, 16)
        pl.semaphore_signal(barrier, inc=1, device_id=(ens, lax.div(e, 4), lax.rem(e, 4)), device_id_type=MESH)
    for p in range(UP):
        load_copy(p).start()
    pmb[...] = jnp.zeros_like(pmb)
    dsrc[...] = jnp.zeros_like(dsrc)
    for m in range(nf // B):
        lam_ref[0:1, m * B:(m + 1) * B] = lam_in[m:m + 1, :]
        mu_ref[0:1, m * B:(m + 1) * B] = mu_in[m:m + 1, :]
    pl.semaphore_wait(barrier, 15)

    @pl.loop(0, NUM_STEPS)
    def _(step):
        @pl.when(step > 0)
        def _():
            row_sums()

        sacc[...] = jnp.zeros_like(sacc)

        def renew(g):
            gp = jnp.minimum(g, UP - 1)

            @pl.when(g < UP)
            def _():
                @pl.when(step == 0)
                def _():
                    load_copy(gp).wait()

                @pl.when(step > 0)
                def _():
                    update(gp)

                post(gp)

            @pl.when(g == UP - 1)
            def _():
                for e in range(8):
                    mine = me == (e // 4) * 12 + e % 4

                    @pl.when(mine)
                    def _():
                        dg_local().start()

                    @pl.when(jnp.logical_not(mine))
                    def _():
                        dg_copy(e).start()

                pm_copy().start()

            @pl.when((g >= 1) & (g <= UP))
            def _():
                th_copy(_clip(g - 1, UP)).wait()

        def sums(g, yf):
            if yf:
                @pl.when(g == START + PM)
                def _():
                    pm_copy().wait()

            v = g - YF0
            v_on = (v >= 0) & (v < 2 * rounds)
            v = _clip(v, 2 * rounds)
            vk = lax.div(v, 2)
            vd = v - 2 * vk

            if yf:
                @pl.when(v_on)
                def _():
                    gram(gy.at[vd, vk], _ref(vk, 1, vd, 1 - y, c))

            state = []
            for d in range(2):
                pos = z if d else 3 - z
                i = g - START - LAG * pos
                on = (i >= 0) & (i < chain)
                i = _clip(i, chain)
                w, k, e = place(i, c)
                state.append((pos, on, i, w, k, e))

            def send_sum(d):
                pos, on, i, w, k, e = state[d]

                @pl.when(on)
                def _():
                    rides = (i >= PM) & (i < PM + 2)

                    @pl.when(pos < 3)
                    def _():
                        @pl.when(rides)
                        def _():
                            pz_copy(d, e).start()

                        z_copy(d, i).start()

                    @pl.when((pos == 3) & (w == 0) & (e != y))
                    def _():
                        @pl.when(rides)
                        def _():
                            pye_copy(e).start()

                        ye_copy(k, i).start()

            for d in range(2):
                pos, on, i, w, k, e = state[d]

                @pl.when(on)
                def _():
                    gram(gsrc.at[d, i], _ref(k, w, d, e + w * (y - e), c))

                if d == 0 and yf:
                    @pl.when(v_on)
                    def _():
                        y_copy(vd, vk).start()

                if d == 1:
                    send_sum(0)

                @pl.when(on)
                def _():
                    @pl.when(w == 1)
                    def _():
                        y_copy(d, k).wait_recv()
                        gsrc[d, i] = gsrc[d, i] + yrecv[d, k]

                    @pl.when((i >= PM) & (i < PM + 2))
                    def _():
                        rows = pl.ds(pl.multiple_of((2 * d + e) * 32, 32), 32)
                        ps[d, e] = pmb[c, rows, :] + pmrecv[rows, :]

                        @pl.when(pos > 0)
                        def _():
                            pz_copy(d, e).wait_recv()
                            ps[d, e] = ps[d, e] + pzr[d, e]

                    @pl.when(pos > 0)
                    def _():
                        z_copy(d, i).wait_recv()
                        gsrc[d, i] = gsrc[d, i] + zrecv[d, i]

            if yf:
                send_sum(1)
                return

            i = g - FIN0
            on = corner & (i >= 0) & (i < chain)
            i = _clip(i, chain)
            w, k, e = place(i, c)

            @pl.when(on & (i == 0))
            def _():
                tot = jnp.zeros((16, B), f32)
                for o in range(16):
                    pltpu.make_async_copy(dsrc, dgather.at[o], dg_r.at[o]).wait()
                    tot = tot + dgather[o]
                dsum[...] = tot

            @pl.when(on & ((w == 1) | (e == y)))
            def _():
                @pl.when(w == 0)
                def _():
                    ye_copy(k, i).wait_recv()
                    gsrc[dc, i] = gsrc[dc, i] + yend[k]

                bi, bj, bp, be = _block(_ref(k, w, dc, y, c))

                def kern(gi, gj):
                    sq = jnp.maximum(gi + gj - 2.0 * gsrc[dc, i], 0.0)
                    return jnp.exp(sq * (-1.0 / bandwidth))

                def add_sums(q, blk):
                    sacc[pl.ds(q, 1), :] = sacc[pl.ds(q, 1), :] + jnp.sum(blk, axis=0, keepdims=True)

                @pl.when(be == 0)
                def _():
                    kk = kern(jnp.broadcast_to(dsum[pl.ds(bi, 1), :], (B, B)).T, dsum[pl.ds(bj, 1), :])
                    kc[c, dc, i] = kk.astype(bf16)
                    add_sums(bj, kk)
                    add_sums(bi, kk.T)

                @pl.when(be == 1)
                def _():
                    tri = low_tri() >= 0
                    ga = jnp.broadcast_to(dsum[pl.ds(2 * bp, 1), :], (B, B))
                    gb = jnp.broadcast_to(dsum[pl.ds(2 * bp + 1, 1), :], (B, B))
                    kk = kern(jnp.where(tri, ga.T, gb.T), jnp.where(tri, ga, gb))
                    kk = jnp.where(low_tri() == 0, 1.0, kk)
                    kc[c, dc, i] = kk.astype(bf16)
                    first, second = unpack(kk)
                    add_sums(2 * bp, first)
                    add_sums(2 * bp + 1, second)

                @pl.when((i >= PM) & (i < PM + 2))
                def _():
                    pye_copy(e).wait_recv()
                    pmf[c, 2 * dc + e] = (ps[dc, e] + pye[...]).astype(bf16)

            send_sum(1)

            @pl.when(on & ((w == 1) | (e == y)))
            def _():
                @pl.when((i >= PM) & (i < PM + 2))
                def _():
                    pky_copy(e).start()

                @pl.when(w == 0)
                def _():
                    kyz_copy(k, i).start()

                @pl.when(w == 1)
                def _():
                    ky_copy(dc, k, i).start()

            @pl.when(on & (i == chain - 1))
            def _():
                for o in range(16):
                    @pl.when(me == o)
                    def _():
                        sg_local().start()

                    @pl.when(me != o)
                    def _():
                        sg_copy(o).start()

        def spread(g):
            heard = []
            for d in range(2):
                dist = 3 - z if d else z
                h = g - AG0 - LAG2 * dist
                on = (h >= 0) & (h < chain)
                i = _clip(h, chain)
                heard.append((h, on, i))

                @pl.when(on)
                def _():
                    w, k, e = place(i, c)
                    turn = (dist == 0) & (w == 0) & (e != y)

                    @pl.when((i >= PM) & (i < PM + 2))
                    def _():
                        @pl.when(turn)
                        def _():
                            pky_copy(1 - y).wait_recv()

                        @pl.when(dist > 0)
                        def _():
                            pkz_copy(d, e).wait_recv()

                        @pl.when(dist < 3)
                        def _():
                            pkz_copy(d, e).start()

                        pkd_copy(d, e, c).start()

                    @pl.when(turn)
                    def _():
                        kyz_copy(k, i).wait_recv()

                    @pl.when(dist > 0)
                    def _():
                        kz_copy(d, i).wait_recv()

                        @pl.when(w == 1)
                        def _():
                            ky_copy(d, k, i).start()

                    @pl.when(dist < 3)
                    def _():
                        kz_copy(d, i).start()

                    kd_copy(d, i, c).start()

                k = h - OUT2 - 2 * rounds

                @pl.when((k >= 0) & (k < rounds))
                def _():
                    kk = _clip(k, rounds)
                    ky_copy(d, kk, 0).wait_recv()
                    ke_copy(d, kk, c).start()

            for d in range(2):
                h, on, i = heard[d]

                @pl.when(on)
                def _():
                    settle(kc.at[c, d, i], num_chain(i, d, c))

                k = h - OUT2 - 2 * rounds

                @pl.when((k >= 0) & (k < rounds))
                def _():
                    kk = _clip(k, rounds)
                    settle(ko.at[c, d, kk], _ref(kk, 1, d, 1 - y, c))

                j = h - DIE

                @pl.when((j >= 0) & (j < other_chain))
                def _():
                    jj = _clip(j, other_chain)

                    @pl.when((jj >= PM) & (jj < PM + 2))
                    def _():
                        pkd_copy(d, jj - 2 * lax.div(jj, 2), 1 - c).wait_recv()

                    kd_copy(d, jj, 1 - c).wait_recv()
                    settle(kc.at[1 - c, d, jj], num_chain(jj, d, 1 - c))

                m = h - OUT2 - DIE - 2 * (9 - rounds)

                @pl.when((m >= 0) & (m < 9 - rounds))
                def _():
                    mm = _clip(m, 9 - rounds)
                    ke_copy(d, mm, 1 - c).wait_recv()
                    settle(ko.at[1 - c, d, mm], _ref(mm, 1, d, 1 - y, 1 - c))

        def drive(g):
            p = g - DRV0
            on = (p >= 0) & (p < UP)
            p = _clip(p, UP)

            @pl.when(on)
            def _():
                q = lax.rem(p, 3) * 2
                half = lax.div(p, 3)
                pmt = jnp.concatenate(
                    [pmf[half, lax.div(q, 2), pl.ds(16 * h, 16), :] for h in range(2)], axis=1
                )
                low = lax.dot_general(
                    pmt.astype(f32).T.astype(bf16), ut_ref[...], (((1,), (0,)), ((), ())), preferred_element_type=f32
                )
                cur = theta[panel(p), :]
                grad = -((cur - mu_ref[0:1, 0:nf]) * lam_ref[0:1, 0:nf] + low)
                a_ref[panel(p), :] = (grad - rep * cur).astype(bf16)

        @pl.loop(0, UP + 1)
        def _(g):
            renew(g)
            sums(g, True)

        @pl.loop(UP + 1, FIN0)
        def _(g):
            sums(g, True)

        @pl.loop(FIN0, FIN0 + CH)
        def _(g):
            sums(g, False)
            spread(g)

        @pl.loop(FIN0 + CH, ITERS)
        def _(g):
            spread(g)
            drive(g)

        for e in range(8):
            @pl.when(me != (e // 4) * 12 + e % 4)
            def _():
                dg_copy(e).wait_send()

        for d in range(2):
            pos = z if d else 3 - z
            for e in range(2):
                @pl.when(pos < 3)
                def _():
                    pz_copy(d, e).wait_send()

                @pl.when(pos > 0)
                def _():
                    pkz_copy(d, e).wait_send()

                pkd_copy(d, e, c).wait_send()

        @pl.when(corner)
        def _():
            pye_copy(1 - y).wait_send()
            pky_copy(y).wait_send()

        @pl.loop(0, rounds)
        def _(k):
            for d in range(2):
                y_copy(d, k).wait_send()
                ke_copy(d, k, c).wait_send()
                ky_copy(d, k, 0).wait_send()

            @pl.when(corner)
            def _():
                ye_copy(k, 2 * k + 1 - y).wait_send()
                kyz_copy(k, 0).wait_send()

        @pl.loop(0, chain)
        def _(i):
            for d in range(2):
                pos = z if d else 3 - z

                @pl.when(pos < 3)
                def _():
                    z_copy(d, i).wait_send()

                @pl.when(pos > 0)
                def _():
                    kz_copy(d, i).wait_send()

                kd_copy(d, i, c).wait_send()

        @pl.when(corner)
        def _():
            for e in range(16):
                @pl.when(me != e)
                def _():
                    sg_copy(e).wait_send()

    row_sums()

    @pl.loop(0, UP)
    def _(p):
        update(p)
        out_copy(p).start()

    @pl.loop(0, UP)
    def _(p):
        out_copy(p).wait()


def hand_over(x_hbm, o_hbm, buf, s_in, s_out):
    n, rows = s_in.shape[0], buf.shape[0] // s_in.shape[0]

    def part(p):
        return pl.ds(p * rows, rows)

    for p in range(n):
        pltpu.make_async_copy(x_hbm.at[part(p)], buf.at[part(p)], s_in.at[p]).start()
    for p in range(n):
        pltpu.make_async_copy(x_hbm.at[part(p)], buf.at[part(p)], s_in.at[p]).wait()
        pltpu.make_async_copy(buf.at[part(p)], o_hbm.at[part(p)], s_out.at[p]).start()
    for p in range(n):
        pltpu.make_async_copy(buf.at[part(p)], o_hbm.at[part(p)], s_out.at[p]).wait()


def solution(mesh):
    def run_steps(particles, prec_diag, mean_vec, low_rank):
        width = particles.shape[1]

        def local_steps(current, prec_loc, mean_loc, fac_loc):
            n_part, nf = current.shape
            dma = pltpu.SemaphoreType.DMA
            f32, bf16 = jnp.float32, jnp.bfloat16
            vmem = pltpu.VMEM
            res = pl.pallas_call(
                functools.partial(kernel, width),
                out_shape=jax.ShapeDtypeStruct((n_part, nf), f32),
                in_specs=[pl.BlockSpec(memory_space=pl.ANY)] + [pl.BlockSpec(memory_space=pltpu.VMEM)] * 3,
                out_specs=pl.BlockSpec(memory_space=pl.ANY),
                scratch_shapes=[
                    vmem((n_part, nf), f32),
                    vmem((n_part, 2 * nf), bf16),
                    vmem((n_part, nf), bf16),
                    vmem((n_part, n_part), bf16),
                    vmem((2, 2, CH, B, B), bf16),
                    vmem((2, 2, 5, B, B), bf16),
                    vmem((2, CH, B, B), f32),
                    vmem((2, 5, B, B), f32),
                    vmem((2, CH, B, B), f32),
                    vmem((2, 5, B, B), f32),
                    vmem((5, B, B), f32),
                    vmem((2, B, B), f32),
                    vmem((B, B), f32),
                    vmem((2, 2, 32, B), f32),
                    vmem((2, 2, 32, B), f32),
                    vmem((32, B), f32),
                    vmem((2, 4, 32, B), bf16),
                    vmem((8, nf + B), f32),
                    vmem((8, nf + B), f32),
                    vmem((16, B), f32),
                    vmem((16, 16, B), f32),
                    vmem((16, B), f32),
                    vmem((16, B), f32),
                    vmem((8, 16, B), f32),
                    vmem((16, B), f32),
                    dma((UP,)), dma((UP,)), dma((UP,)), dma((UP,)), dma, dma, dma((8,)), dma((16,)), dma((16,)), dma((8,)),
                    dma((2, CH)), dma((2, CH)), dma((2, 5)), dma((2, 5)), dma((5,)), dma((5,)),
                    dma((2, CH)), dma((2, CH)), dma((5,)), dma((5,)), dma((2, 5)), dma((2, 5)),
                    dma((2, CH)), dma((2, CH)), dma((2, 5)), dma((2, 5)),
                    dma((2, 2)), dma((2, 2)), dma, dma, dma, dma, dma((2, 2)), dma((2, 2)), dma((2, 2)), dma((2, 2)),
                ],
                compiler_params=pltpu.CompilerParams(
                    collective_id=0, has_side_effects=True, vmem_limit_bytes=56 * 1024 * 1024
                ),
                name="svgd",
            )(current, prec_loc.reshape(nf // B, B), mean_loc.reshape(nf // B, B), fac_loc.T)
            return pl.pallas_call(
                hand_over,
                out_shape=jax.ShapeDtypeStruct((n_part, nf), f32),
                in_specs=[pl.BlockSpec(memory_space=pl.ANY)],
                out_specs=pl.BlockSpec(memory_space=pl.ANY),
                scratch_shapes=[vmem((n_part, nf), f32), dma((16,)), dma((16,))],
                name="hand_over",
            )(res)

        sharded = jax.shard_map(
            local_steps,
            mesh=mesh,
            in_specs=(P("ens", FEAT_AXES), P(LEAD_AXES), P(LEAD_AXES), P(LEAD_AXES, None)),
            out_specs=P("ens", FEAT_AXES),
            check_vma=False,
        )
        return sharded(particles, prec_diag, mean_vec, low_rank)

    return run_steps
```

```python
import functools

import jax
import jax.numpy as jnp
from jax import lax
from jax.experimental import pallas as pl
from jax.experimental.pallas import tpu as pltpu
from jax.sharding import PartitionSpec as P

NUM_STEPS = 3
BAND_SCALE = 4.0
STEP_SCALE = 0.4
FEAT_AXES = ("slab", "feat")
LEAD_AXES = ("ens", "slab", "feat")
MESH = pl.DeviceIdType.MESH

B = 128
ROW = 256
UP = 6
START = 2
LAG = 3
END = 2
OUT1 = 2
LAG2 = 3
OUT2 = 3
DIE = 3
YF0 = 3
FIN0 = START + 3 * LAG + END
AG0 = FIN0 + OUT1
CH = 15
PM = 6
DRV0 = AG0 + 3 * LAG2 + PM + 1 + DIE + 1
ITERS = AG0 + 3 * LAG2 + CH + OUT2 + DIE
assert YF0 + 10 <= FIN0 and FIN0 + CH <= DRV0 and DRV0 + UP <= ITERS


def _ref(k, t, d, ey, c):
    f = lax.div(k, 4)
    return k * 16 + (1 - f) * (t * 8 + d * 4 + ey * 2 + c) + f * (t * 4 + d * 2 + ey)


def _block(n):
    p = lax.div(n + 126, B) + lax.div(n + 120, B) + lax.div(n + 110, B) + lax.div(n + 96, B) + lax.div(n + 78, B)
    r = n - 2 * p * p
    i = lax.div(r, 2)
    j = 2 * p + lax.rem(r, 2)
    return i, j, p, 1 - jnp.minimum(j - i, 1)


def _clip(i, n):
    return jnp.minimum(jnp.maximum(i, 0), n - 1)


def _span(i):
    return pl.ds(pl.multiple_of(i * B, B), B)


def kernel(width, x_hbm, lam_in, mu_in, ut_ref, theta, th, a_ref, kf, kc, ko, gsrc, gy, zrecv, yrecv, yend, pmb, pmrecv,
           ps, pzr, pye, pmf, lam_ref, mu_ref,
           dsrc, dgather, dsum, sacc, sgather, ssum, ld, thd_s, thd_r, pm_s, pm_r, dg_s, dg_r, sg_s, sg_r,
           zs, zr, ys, yr, ye_s, ye_r, kz_s, kz_r, kyz_s, kyz_r, ky_s, ky_r, kd_s, kd_r, ke_s, ke_r,
           pz_s, pz_r, pye_s, pye_r, pky_s, pky_r, pkz_s, pkz_r, pkd_s, pkd_r):
    nf = theta.shape[1]
    n_part = theta.shape[0]
    bandwidth = BAND_SCALE * width
    step_size = STEP_SCALE * width
    rep = 2.0 / bandwidth
    f32, bf16 = jnp.float32, jnp.bfloat16
    ens = lax.axis_index("ens")
    z = lax.axis_index("slab")
    feat = lax.axis_index("feat")
    y = lax.div(feat, 2)
    c = lax.rem(feat, 2)
    me = z * 4 + feat
    ypart = (ens, z, (1 - y) * 2 + c)
    dpart = (ens, z, y * 2 + 1 - c)
    dc = lax.div(z, 3)
    corner = lax.rem(z, 3) == 0
    own8 = (dc * 2 + y) * 2 + c
    rounds = 4 + c
    chain = 3 * rounds
    other_chain = 27 - chain

    def rcopy(src, dst, s, r, dev):
        return pltpu.make_async_remote_copy(src_ref=src, dst_ref=dst, send_sem=s, recv_sem=r, device_id=dev, device_id_type=MESH)

    def zdev(dz):
        return (ens, z + dz, feat)

    def place(i, cc):
        zf = 8 + 2 * cc
        w = _clip(i - zf + 1, 2)
        h = lax.div(i, 2)
        return w, h + w * (i - zf - h), i - 2 * h

    def num_chain(i, d, cc):
        w, k, e = place(i, cc)
        return _ref(k, w, d, (1 - w) * e + w * y, cc)

    def panel(p):
        return pl.ds(pl.multiple_of(p * ROW, ROW), ROW)

    def load_copy(p):
        return pltpu.make_async_copy(x_hbm.at[panel(p)], theta.at[panel(p)], ld.at[p])

    def th_copy(p):
        return rcopy(th.at[panel(p), pl.ds(0, nf)], th.at[panel(p), pl.ds(nf, nf)], thd_s.at[p], thd_r.at[p], dpart)

    def pm_copy():
        return rcopy(pmb.at[1 - c], pmrecv, pm_s, pm_r, dpart)

    def dg_copy(e):
        return rcopy(dsrc, dgather.at[me], dg_s.at[e], dg_r.at[me], (ens, (e // 4) * 3, e % 4))

    def dg_local():
        return pltpu.make_async_copy(dsrc, dgather.at[me], dg_r.at[me])

    def sg_copy(e):
        return rcopy(sacc, sgather.at[own8], sg_s.at[e], sg_r.at[own8], (ens, e // 4, e % 4))

    def sg_local():
        return pltpu.make_async_copy(sacc, sgather.at[own8], sg_r.at[own8])

    def z_copy(d, i):
        return rcopy(gsrc.at[d, i], zrecv.at[d, i], zs.at[d, i], zr.at[d, i], zdev(2 * d - 1))

    def y_copy(d, k):
        return rcopy(gy.at[d, k], yrecv.at[d, k], ys.at[d, k], yr.at[d, k], ypart)

    def ye_copy(k, i):
        return rcopy(gsrc.at[dc, i], yend.at[k], ye_s.at[k], ye_r.at[k], ypart)

    def kc_copy(d, i, cc, s, r, dev):
        return rcopy(kc.at[cc, d, i], kc.at[cc, d, i], s, r, dev)

    def ko_copy(d, k, cc, s, r, dev):
        return rcopy(ko.at[cc, d, k], ko.at[cc, d, k], s, r, dev)

    def kz_copy(d, i):
        return kc_copy(d, i, c, kz_s.at[d, i], kz_r.at[d, i], zdev(1 - 2 * d))

    def kyz_copy(k, i):
        return kc_copy(dc, i, c, kyz_s.at[k], kyz_r.at[k], ypart)

    def ky_copy(d, k, i):
        return rcopy(kc.at[c, d, i], ko.at[c, d, k], ky_s.at[d, k], ky_r.at[d, k], ypart)

    def kd_copy(d, i, cc):
        return kc_copy(d, i, cc, kd_s.at[d, i], kd_r.at[d, i], dpart)

    def ke_copy(d, k, cc):
        return ko_copy(d, k, cc, ke_s.at[d, k], ke_r.at[d, k], dpart)

    def pz_copy(d, e):
        return rcopy(ps.at[d, e], pzr.at[d, e], pz_s.at[d, e], pz_r.at[d, e], zdev(2 * d - 1))

    def pye_copy(e):
        return rcopy(ps.at[dc, e], pye, pye_s, pye_r, ypart)

    def pf_copy(d, e, cc, s, r, dev):
        return rcopy(pmf.at[cc, 2 * d + e], pmf.at[cc, 2 * d + e], s, r, dev)

    def pky_copy(e):
        return pf_copy(dc, e, c, pky_s, pky_r, ypart)

    def pkz_copy(d, e):
        return pf_copy(d, e, c, pkz_s.at[d, e], pkz_r.at[d, e], zdev(1 - 2 * d))

    def pkd_copy(d, e, cc):
        return pf_copy(d, e, cc, pkd_s.at[d, e], pkd_r.at[d, e], dpart)

    def low_tri():
        return lax.broadcasted_iota(jnp.int32, (B, B), 0) - lax.broadcasted_iota(jnp.int32, (B, B), 1)

    def unpack(kk):
        kt = kk.T
        tri = low_tri()
        return jnp.where(tri >= 0, kk, kt), jnp.where(tri < 0, kk, jnp.where(tri == 0, 1.0, kt))

    def settle(src, n):
        i, j, p, e = _block(n)

        @pl.when(e == 0)
        def _():
            blk = src[...]
            kf[_span(i), _span(j)] = blk
            kf[_span(j), _span(i)] = blk.T

        @pl.when(e == 1)
        def _():
            first, second = unpack(src[...].astype(f32))
            kf[_span(2 * p), _span(2 * p)] = first.astype(bf16)
            kf[_span(2 * p + 1), _span(2 * p + 1)] = second.astype(bf16)

    def dot_t(i, j):
        return lax.dot_general(th[_span(i), :], th[_span(j), :], (((1,), (1,)), ((), ())), preferred_element_type=f32)

    def gram(dst, n):
        i, j, p, e = _block(n)
        dst[...] = dot_t(i, j)

        @pl.when(e == 1)
        def _():
            dst[...] = jnp.where(low_tri() >= 0, dst[...], dot_t(2 * p + 1, 2 * p + 1))

    def post(p):
        new = theta[panel(p), :]
        tb = new.astype(bf16)
        th[panel(p), pl.ds(0, nf)] = tb
        xb = (new - mu_ref[0:1, 0:nf]).astype(bf16)
        pm = lax.dot_general(ut_ref[...], xb, (((1,), (1,)), ((), ())), preferred_element_type=f32)
        th_copy(p).start()
        half = lax.div(p, 3)
        for h in range(2):
            q = lax.rem(p, 3) * 2 + h
            pmb[half, pl.ds(pl.multiple_of(q * 16, 16), 16), :] = pm[:, h * B:(h + 1) * B]
            t = tb[h * B:(h + 1) * B, :].astype(f32)
            sq = t * t
            tot = sq[:, 0:B]
            for m in range(1, nf // B):
                tot = tot + sq[:, m * B:(m + 1) * B]
            dsrc[pl.ds(p * 2 + h, 1), :] = jnp.sum(tot.T, axis=0, keepdims=True)

    def row_sums():
        tot = jnp.zeros((16, B), f32)
        for e in range(8):
            pltpu.make_async_copy(sacc, sgather.at[e], sg_r.at[e]).wait()
            tot = tot + sgather[e]
        ssum[...] = tot

    def update(p):
        acc = jnp.dot(kf[panel(p), :], a_ref[...], preferred_element_type=f32)
        cur = theta[panel(p), :]
        col = jnp.concatenate(
            [jnp.broadcast_to(ssum[pl.ds(p * 2 + h, 1), :], (B, B)).T[:, 0:1] for h in range(2)], axis=0
        )
        phi = (acc + (rep * col) * cur) * (1.0 / n_part)
        theta[panel(p), :] = cur + step_size * phi

    barrier = pltpu.get_barrier_semaphore()
    for o in range(1, 16):
        e = lax.rem(me + o, 16)
        pl.semaphore_signal(barrier, inc=1, device_id=(ens, lax.div(e, 4), lax.rem(e, 4)), device_id_type=MESH)
    for p in range(UP):
        load_copy(p).start()
    pmb[...] = jnp.zeros_like(pmb)
    dsrc[...] = jnp.zeros_like(dsrc)
    for m in range(nf // B):
        lam_ref[0:1, m * B:(m + 1) * B] = lam_in[m:m + 1, :]
        mu_ref[0:1, m * B:(m + 1) * B] = mu_in[m:m + 1, :]
    pl.semaphore_wait(barrier, 15)

    @pl.loop(0, NUM_STEPS)
    def _(step):
        @pl.when(step > 0)
        def _():
            row_sums()

        sacc[...] = jnp.zeros_like(sacc)

        def renew(g):
            gp = jnp.minimum(g, UP - 1)

            @pl.when(g < UP)
            def _():
                @pl.when(step == 0)
                def _():
                    load_copy(gp).wait()

                @pl.when(step > 0)
                def _():
                    update(gp)

                post(gp)

            @pl.when(g == UP - 1)
            def _():
                for e in range(8):
                    mine = me == (e // 4) * 12 + e % 4

                    @pl.when(mine)
                    def _():
                        dg_local().start()

                    @pl.when(jnp.logical_not(mine))
                    def _():
                        dg_copy(e).start()

                pm_copy().start()

            @pl.when((g >= 1) & (g <= UP))
            def _():
                th_copy(_clip(g - 1, UP)).wait()

        def sums(g, yf):
            if yf:
                @pl.when(g == START + PM)
                def _():
                    pm_copy().wait()

            v = g - YF0
            v_on = (v >= 0) & (v < 2 * rounds)
            v = _clip(v, 2 * rounds)
            vk = lax.div(v, 2)
            vd = v - 2 * vk

            if yf:
                @pl.when(v_on)
                def _():
                    gram(gy.at[vd, vk], _ref(vk, 1, vd, 1 - y, c))

            state = []
            for d in range(2):
                pos = z if d else 3 - z
                i = g - START - LAG * pos
                on = (i >= 0) & (i < chain)
                i = _clip(i, chain)
                w, k, e = place(i, c)
                state.append((pos, on, i, w, k, e))

            def send_sum(d):
                pos, on, i, w, k, e = state[d]

                @pl.when(on)
                def _():
                    rides = (i >= PM) & (i < PM + 2)

                    @pl.when(pos < 3)
                    def _():
                        @pl.when(rides)
                        def _():
                            pz_copy(d, e).start()

                        z_copy(d, i).start()

                    @pl.when((pos == 3) & (w == 0) & (e != y))
                    def _():
                        @pl.when(rides)
                        def _():
                            pye_copy(e).start()

                        ye_copy(k, i).start()

            for d in range(2):
                pos, on, i, w, k, e = state[d]

                @pl.when(on)
                def _():
                    gram(gsrc.at[d, i], _ref(k, w, d, e + w * (y - e), c))

                if d == 0 and yf:
                    @pl.when(v_on)
                    def _():
                        y_copy(vd, vk).start()

                if d == 1:
                    send_sum(0)

                @pl.when(on)
                def _():
                    @pl.when(w == 1)
                    def _():
                        y_copy(d, k).wait_recv()
                        gsrc[d, i] = gsrc[d, i] + yrecv[d, k]

                    @pl.when((i >= PM) & (i < PM + 2))
                    def _():
                        rows = pl.ds(pl.multiple_of((2 * d + e) * 32, 32), 32)
                        ps[d, e] = pmb[c, rows, :] + pmrecv[rows, :]

                        @pl.when(pos > 0)
                        def _():
                            pz_copy(d, e).wait_recv()
                            ps[d, e] = ps[d, e] + pzr[d, e]

                    @pl.when(pos > 0)
                    def _():
                        z_copy(d, i).wait_recv()
                        gsrc[d, i] = gsrc[d, i] + zrecv[d, i]

            if yf:
                send_sum(1)
                return

            i = g - FIN0
            on = corner & (i >= 0) & (i < chain)
            i = _clip(i, chain)
            w, k, e = place(i, c)

            @pl.when(on & (i == 0))
            def _():
                tot = jnp.zeros((16, B), f32)
                for o in range(16):
                    pltpu.make_async_copy(dsrc, dgather.at[o], dg_r.at[o]).wait()
                    tot = tot + dgather[o]
                dsum[...] = tot

            @pl.when(on & ((w == 1) | (e == y)))
            def _():
                @pl.when(w == 0)
                def _():
                    ye_copy(k, i).wait_recv()
                    gsrc[dc, i] = gsrc[dc, i] + yend[k]

                bi, bj, bp, be = _block(_ref(k, w, dc, y, c))

                def kern(gi, gj):
                    sq = jnp.maximum(gi + gj - 2.0 * gsrc[dc, i], 0.0)
                    return jnp.exp(sq * (-1.0 / bandwidth))

                def add_sums(q, blk):
                    sacc[pl.ds(q, 1), :] = sacc[pl.ds(q, 1), :] + jnp.sum(blk, axis=0, keepdims=True)

                @pl.when(be == 0)
                def _():
                    kk = kern(jnp.broadcast_to(dsum[pl.ds(bi, 1), :], (B, B)).T, dsum[pl.ds(bj, 1), :])
                    kc[c, dc, i] = kk.astype(bf16)
                    add_sums(bj, kk)
                    add_sums(bi, kk.T)

                @pl.when(be == 1)
                def _():
                    tri = low_tri() >= 0
                    ga = jnp.broadcast_to(dsum[pl.ds(2 * bp, 1), :], (B, B))
                    gb = jnp.broadcast_to(dsum[pl.ds(2 * bp + 1, 1), :], (B, B))
                    kk = kern(jnp.where(tri, ga.T, gb.T), jnp.where(tri, ga, gb))
                    kk = jnp.where(low_tri() == 0, 1.0, kk)
                    kc[c, dc, i] = kk.astype(bf16)
                    first, second = unpack(kk)
                    add_sums(2 * bp, first)
                    add_sums(2 * bp + 1, second)

                @pl.when((i >= PM) & (i < PM + 2))
                def _():
                    pye_copy(e).wait_recv()
                    pmf[c, 2 * dc + e] = (ps[dc, e] + pye[...]).astype(bf16)

            send_sum(1)

            @pl.when(on & ((w == 1) | (e == y)))
            def _():
                @pl.when((i >= PM) & (i < PM + 2))
                def _():
                    pky_copy(e).start()

                @pl.when(w == 0)
                def _():
                    kyz_copy(k, i).start()

                @pl.when(w == 1)
                def _():
                    ky_copy(dc, k, i).start()

            @pl.when(on & (i == chain - 1))
            def _():
                for o in range(16):
                    @pl.when(me == o)
                    def _():
                        sg_local().start()

                    @pl.when(me != o)
                    def _():
                        sg_copy(o).start()

        def spread(g):
            heard = []
            for d in range(2):
                dist = 3 - z if d else z
                h = g - AG0 - LAG2 * dist
                on = (h >= 0) & (h < chain)
                i = _clip(h, chain)
                heard.append((h, on, i))

                @pl.when(on)
                def _():
                    w, k, e = place(i, c)
                    turn = (dist == 0) & (w == 0) & (e != y)

                    @pl.when((i >= PM) & (i < PM + 2))
                    def _():
                        @pl.when(turn)
                        def _():
                            pky_copy(1 - y).wait_recv()

                        @pl.when(dist > 0)
                        def _():
                            pkz_copy(d, e).wait_recv()

                        @pl.when(dist < 3)
                        def _():
                            pkz_copy(d, e).start()

                        pkd_copy(d, e, c).start()

                    @pl.when(turn)
                    def _():
                        kyz_copy(k, i).wait_recv()

                    @pl.when(dist > 0)
                    def _():
                        kz_copy(d, i).wait_recv()

                        @pl.when(w == 1)
                        def _():
                            ky_copy(d, k, i).start()

                    @pl.when(dist < 3)
                    def _():
                        kz_copy(d, i).start()

                    kd_copy(d, i, c).start()

                k = h - OUT2 - 2 * rounds

                @pl.when((k >= 0) & (k < rounds))
                def _():
                    kk = _clip(k, rounds)
                    ky_copy(d, kk, 0).wait_recv()
                    ke_copy(d, kk, c).start()

            for d in range(2):
                h, on, i = heard[d]

                @pl.when(on)
                def _():
                    settle(kc.at[c, d, i], num_chain(i, d, c))

                k = h - OUT2 - 2 * rounds

                @pl.when((k >= 0) & (k < rounds))
                def _():
                    kk = _clip(k, rounds)
                    settle(ko.at[c, d, kk], _ref(kk, 1, d, 1 - y, c))

                j = h - DIE

                @pl.when((j >= 0) & (j < other_chain))
                def _():
                    jj = _clip(j, other_chain)

                    @pl.when((jj >= PM) & (jj < PM + 2))
                    def _():
                        pkd_copy(d, jj - 2 * lax.div(jj, 2), 1 - c).wait_recv()

                    kd_copy(d, jj, 1 - c).wait_recv()
                    settle(kc.at[1 - c, d, jj], num_chain(jj, d, 1 - c))

                m = h - OUT2 - DIE - 2 * (9 - rounds)

                @pl.when((m >= 0) & (m < 9 - rounds))
                def _():
                    mm = _clip(m, 9 - rounds)
                    ke_copy(d, mm, 1 - c).wait_recv()
                    settle(ko.at[1 - c, d, mm], _ref(mm, 1, d, 1 - y, 1 - c))

        def drive(g):
            p = g - DRV0
            on = (p >= 0) & (p < UP)
            p = _clip(p, UP)

            @pl.when(on)
            def _():
                q = lax.rem(p, 3) * 2
                half = lax.div(p, 3)
                pmt = jnp.concatenate(
                    [pmf[half, lax.div(q, 2), pl.ds(16 * h, 16), :] for h in range(2)], axis=1
                )
                low = lax.dot_general(
                    pmt.astype(f32).T.astype(bf16), ut_ref[...], (((1,), (0,)), ((), ())), preferred_element_type=f32
                )
                cur = theta[panel(p), :]
                grad = -((cur - mu_ref[0:1, 0:nf]) * lam_ref[0:1, 0:nf] + low)
                a_ref[panel(p), :] = (grad - rep * cur).astype(bf16)

        @pl.loop(0, UP + 1)
        def _(g):
            renew(g)
            sums(g, True)

        @pl.loop(UP + 1, FIN0)
        def _(g):
            sums(g, True)

        @pl.loop(FIN0, FIN0 + CH)
        def _(g):
            sums(g, False)
            spread(g)

        @pl.loop(FIN0 + CH, ITERS)
        def _(g):
            spread(g)
            drive(g)

        for e in range(8):
            @pl.when(me != (e // 4) * 12 + e % 4)
            def _():
                dg_copy(e).wait_send()

        for d in range(2):
            pos = z if d else 3 - z
            for e in range(2):
                @pl.when(pos < 3)
                def _():
                    pz_copy(d, e).wait_send()

                @pl.when(pos > 0)
                def _():
                    pkz_copy(d, e).wait_send()

                pkd_copy(d, e, c).wait_send()

        @pl.when(corner)
        def _():
            pye_copy(1 - y).wait_send()
            pky_copy(y).wait_send()

        @pl.loop(0, rounds)
        def _(k):
            for d in range(2):
                y_copy(d, k).wait_send()
                ke_copy(d, k, c).wait_send()
                ky_copy(d, k, 0).wait_send()

            @pl.when(corner)
            def _():
                ye_copy(k, 2 * k + 1 - y).wait_send()
                kyz_copy(k, 0).wait_send()

        @pl.loop(0, chain)
        def _(i):
            for d in range(2):
                pos = z if d else 3 - z

                @pl.when(pos < 3)
                def _():
                    z_copy(d, i).wait_send()

                @pl.when(pos > 0)
                def _():
                    kz_copy(d, i).wait_send()

                kd_copy(d, i, c).wait_send()

        @pl.when(corner)
        def _():
            for e in range(16):
                @pl.when(me != e)
                def _():
                    sg_copy(e).wait_send()

    row_sums()

    @pl.loop(0, UP)
    def _(p):
        update(p)


def solution(mesh):
    def run_steps(particles, prec_diag, mean_vec, low_rank):
        width = particles.shape[1]

        def local_steps(current, prec_loc, mean_loc, fac_loc):
            n_part, nf = current.shape
            dma = pltpu.SemaphoreType.DMA
            f32, bf16 = jnp.float32, jnp.bfloat16
            vmem = pltpu.VMEM
            res = pl.pallas_call(
                functools.partial(kernel, width),
                out_shape=pltpu.VMEM((n_part, nf), f32),
                in_specs=[pl.BlockSpec(memory_space=pl.ANY)] + [pl.BlockSpec(memory_space=pltpu.VMEM)] * 3,
                out_specs=pl.BlockSpec(memory_space=pltpu.VMEM),
                scratch_shapes=[
                    vmem((n_part, 2 * nf), bf16),
                    vmem((n_part, nf), bf16),
                    vmem((n_part, n_part), bf16),
                    vmem((2, 2, CH, B, B), bf16),
                    vmem((2, 2, 5, B, B), bf16),
                    vmem((2, CH, B, B), f32),
                    vmem((2, 5, B, B), f32),
                    vmem((2, CH, B, B), f32),
                    vmem((2, 5, B, B), f32),
                    vmem((5, B, B), f32),
                    vmem((2, B, B), f32),
                    vmem((B, B), f32),
                    vmem((2, 2, 32, B), f32),
                    vmem((2, 2, 32, B), f32),
                    vmem((32, B), f32),
                    vmem((2, 4, 32, B), bf16),
                    vmem((8, nf + B), f32),
                    vmem((8, nf + B), f32),
                    vmem((16, B), f32),
                    vmem((16, 16, B), f32),
                    vmem((16, B), f32),
                    vmem((16, B), f32),
                    vmem((8, 16, B), f32),
                    vmem((16, B), f32),
                    dma((UP,)), dma((UP,)), dma((UP,)), dma, dma, dma((8,)), dma((16,)), dma((16,)), dma((8,)),
                    dma((2, CH)), dma((2, CH)), dma((2, 5)), dma((2, 5)), dma((5,)), dma((5,)),
                    dma((2, CH)), dma((2, CH)), dma((5,)), dma((5,)), dma((2, 5)), dma((2, 5)),
                    dma((2, CH)), dma((2, CH)), dma((2, 5)), dma((2, 5)),
                    dma((2, 2)), dma((2, 2)), dma, dma, dma, dma, dma((2, 2)), dma((2, 2)), dma((2, 2)), dma((2, 2)),
                ],
                compiler_params=pltpu.CompilerParams(
                    collective_id=0, has_side_effects=True, vmem_limit_bytes=56 * 1024 * 1024
                ),
                name="svgd",
            )(current, prec_loc.reshape(nf // B, B), mean_loc.reshape(nf // B, B), fac_loc.T)
            return res

        sharded = jax.shard_map(
            local_steps,
            mesh=mesh,
            in_specs=(P("ens", FEAT_AXES), P(LEAD_AXES), P(LEAD_AXES), P(LEAD_AXES, None)),
            out_specs=P("ens", FEAT_AXES),
            check_vma=False,
        )
        return sharded(particles, prec_diag, mean_vec, low_rank)

    return run_steps
```
